32 devices in a mesh: batch: 16 (over z, x, core), seq: 2 (over y).
Axes of the slice: x: 2, y: 2, z: 4, core: 2. Of those that a mesh axis runs over, the one named last changes fastest.
Arguments:
- tokens: bfloat16 [16, 1024, 2560], P('batch', 'seq'), may hold values from -6 to 6
- attn_in: bfloat16 [16, 1024, 2560], P('batch', 'seq'), may hold values from -6 to 6
- lengths: int32 [16], P('batch'), may hold values from 256 to 1024
- norm_gain: float32 [2560], replicated, may hold values from 0.5 to 1.5
- attn_gain: float32 [2560], replicated, may hold values from 0.5 to 1.5
- w_x: bfloat16 [2560, 2560], P(('batch', 'seq')), may hold values from -0.125 to 0.125
- conv_w: float32 [4, 2560], replicated, may hold values from -3 to 3
- w_a: bfloat16 [10, 256, 256], replicated, may hold values from -0.375 to 0.375
- w_i: bfloat16 [10, 256, 256], replicated, may hold values from -0.375 to 0.375
- lru_decay: float32 [2560], replicated, may hold values from 4 to 20
- w_kv: bfloat16 [2560, 512], replicated, may hold values from -0.125 to 0.125
Outputs:
- lru_state: float32 [16, 2560], P('batch', 'seq')
- conv_state: bfloat16 [16, 3, 2560], P('batch', None, 'seq')
- kv_cache: bfloat16 [16, 2048, 512], P('batch', None, 'seq')
The draws below stay inside these ranges and needn't reach their ends.
Inputs may be any that keep to these rules, and one draw needn't show every extreme that they name: `lengths`: positions from a prompt's length on are padding.
All inputs are finite; a program needn't handle non-finite values.
Results may differ from the reference program's by a relative error of at most 0.0051.
Values may be sent and summed in bfloat16 or wider, within the bound.
A program may use at most 128 MiB of HBM per device.

```python
import jax
import jax.numpy as jnp
from jax import lax

D = 2560
H = 10
HD = 256
W = 2048
SEQ = 1024
PROMPTS = 16


def draw_lru_decay(key, part):
    pick_key = jax.random.fold_in(key, 11)
    slow_key = jax.random.fold_in(key, 12)
    fast_key = jax.random.fold_in(key, 13)
    share = 50
    fast_mask = jax.random.randint(pick_key, (D,), 0, 100) < share
    slow_value = jnp.log(8.0 * SEQ / jax.random.uniform(slow_key, (D,), jnp.float32, 0.2, 1.0))
    fast_value = jnp.log(jax.random.uniform(fast_key, (D,), jnp.float32, 120.0, 200.0))
    return jnp.where(fast_mask, fast_value, slow_value).astype(jnp.float32)


def place_ends(array, own_key, smallest, largest):
    index_at = [jax.random.randint(jax.random.fold_in(own_key, axis), (), 0, length) for axis, length in enumerate(array.shape)]
    widest = array.shape.index(max(array.shape))
    beside = index_at[:widest] + [(index_at[widest] + 1) % array.shape[widest]] + index_at[widest + 1:]
    return array.at[tuple(index_at)].set(smallest).at[tuple(beside)].set(largest)


def shard_levels(stream_key, shape, pieces, smallest, largest):
    def one(axis_at, blocks):
        heights = jax.random.uniform(jax.random.fold_in(jax.random.fold_in(stream_key, 6), axis_at), (blocks,), jnp.float32, smallest / len(pieces), largest / len(pieces))
        return jnp.repeat(jnp.exp(heights), shape[axis_at] // blocks).reshape((-1,) + (1,) * (len(shape) - axis_at - 1))

    loudness = one(*pieces[0])
    for cut in pieces[1:]:
        loudness = loudness * one(*cut)
    return loudness


def noise(rng, dims, spread, reach, pieces=(), kind=jnp.bfloat16):
    result = jax.random.normal(rng, dims, jnp.float32) * spread
    if len(pieces) > 0:
        result = shard_levels(rng, dims, pieces, -0.22, 0.18) * result
    return jnp.clip(result, min=-reach, max=reach).astype(kind)


def setup_inputs(seed: int = 0) -> dict:
    key_list = jax.random.split(jax.random.key(seed), 12)
    return {
        "tokens": noise(key_list[0], (PROMPTS, SEQ, D), 1.0, 6.0, ((0, 16), (1, 2))),
        "attn_in": noise(key_list[1], (PROMPTS, SEQ, D), 1.0, 6.0, ((0, 16), (1, 2))),
        "lengths": place_ends(jax.random.randint(key_list[2], (PROMPTS,), SEQ // 4, SEQ + 1), jax.random.fold_in(key_list[2], 1), SEQ // 4, SEQ).astype(jnp.int32),
        "norm_gain": jnp.clip(1.0 + 0.1 * jax.random.normal(key_list[3], (D,), jnp.float32), 0.5, 1.5),
        "attn_gain": jnp.clip(1.0 + 0.1 * jax.random.normal(key_list[4], (D,), jnp.float32), 0.5, 1.5),
        "w_x": noise(key_list[5], (D, D), D ** -0.5, 0.125, ((0, 32),)),
        "conv_w": noise(key_list[6], (4, D), 0.5, 3.0, (), jnp.float32),
        "w_a": noise(key_list[7], (H, HD, HD), HD ** -0.5, 0.375),
        "w_i": noise(key_list[8], (H, HD, HD), HD ** -0.5, 0.375),
        "lru_decay": draw_lru_decay(jax.random.fold_in(key_list[11], 71), 0),
        "w_kv": noise(key_list[10], (D, 2 * HD), D ** -0.5, 0.125),
    }


def rms_norm(values, gain_vec):
    widened = values.astype(jnp.float32)
    inverse = lax.rsqrt(lax.optimization_barrier(jnp.mean(widened * widened, axis=-1, keepdims=True)) + 1e-06)
    return (widened * inverse * gain_vec).astype(jnp.bfloat16)

def rotate_keys(key_rows, positions):
    quarter = key_rows.shape[-1] // 4
    spacing = jnp.exp(-jnp.log(10000.0) * jnp.arange(quarter, dtype=jnp.float32) / quarter)
    angles = positions.astype(jnp.float32)[:, None] * spacing[None, :]
    cosine_rows = jnp.cos(angles)
    sine_rows = jnp.sin(angles)
    first_part = key_rows[:, :quarter]
    second_part = key_rows[:, quarter:2 * quarter]
    return jnp.concatenate([first_part * cosine_rows - second_part * sine_rows, second_part * cosine_rows + first_part * sine_rows, key_rows[:, 2 * quarter:]], axis=1)

def one_prompt(norm_gain, attn_gain, w_x, conv_w, w_a, w_i, lru_decay, w_kv, tokens, attn_in, length):
    seq_len = tokens.shape[0]
    normed = rms_norm(tokens, norm_gain)
    x_proj = jnp.dot(normed, w_x, preferred_element_type=jnp.float32).astype(jnp.bfloat16)
    padded = jnp.concatenate([jnp.zeros((3, D), jnp.bfloat16), x_proj], axis=0)
    conv_sum = conv_w[0] * padded[0:seq_len].astype(jnp.float32)
    for offset in range(1, 4):
        conv_sum = conv_sum + conv_w[offset] * padded[offset:offset + seq_len].astype(jnp.float32)
    x_conv = conv_sum.astype(jnp.bfloat16)
    head_rows = x_conv.astype(jnp.float32).reshape(seq_len, H, HD)
    gate_a = jnp.einsum('lhk,hkj->lhj', head_rows, w_a.astype(jnp.float32)).reshape(seq_len, D)
    gate_i = jnp.einsum('lhk,hkj->lhj', head_rows, w_i.astype(jnp.float32)).reshape(seq_len, D)
    positions = jnp.arange(seq_len, dtype=jnp.int32)
    valid_row = (positions < length).astype(jnp.float32)[:, None]
    log_rate = -8.0 * jax.nn.softplus(-lru_decay) * jax.nn.sigmoid(gate_a)
    keep_rate = jnp.exp(log_rate * valid_row)
    push_term = jnp.sqrt(-jnp.expm1(2.0 * log_rate)) * jax.nn.sigmoid(gate_i) * x_conv.astype(jnp.float32) * valid_row

    def advance(carried, step_pair):
        return (step_pair[0] * carried + step_pair[1], None)
    lru_state = lax.scan(advance, jnp.zeros((D,), jnp.float32), (keep_rate, push_term))[0]
    conv_state = lax.dynamic_slice_in_dim(padded, length.astype(jnp.int32), 3, 0)
    attn_normed = rms_norm(attn_in, attn_gain)
    kv_full = jnp.dot(attn_normed, w_kv, preferred_element_type=jnp.float32)
    kv_rows = jnp.concatenate([rotate_keys(kv_full[:, :HD], positions), kv_full[:, HD:]], axis=1).astype(jnp.bfloat16)
    in_window = ((positions >= length - W) & (positions < length)).astype(jnp.float32)[:, None]
    masked = kv_rows.astype(jnp.float32) * in_window
    lap_count = -(-seq_len // W)
    masked = jnp.concatenate([masked, jnp.zeros((lap_count * W - seq_len, 2 * HD), jnp.float32)], axis=0)
    kv_cache = lax.optimization_barrier(jnp.sum(masked.reshape(lap_count, W, 2 * HD), axis=0)).astype(jnp.bfloat16)
    return (lru_state, conv_state, kv_cache)

def reference(tokens, attn_in, lengths, norm_gain, attn_gain, w_x, conv_w, w_a, w_i, lru_decay, w_kv):

    def per_prompt(inputs):
        return one_prompt(norm_gain, attn_gain, w_x, conv_w, w_a, w_i, lru_decay, w_kv, inputs[0], inputs[1], inputs[2])
    lru_state, conv_state, kv_cache = lax.map(per_prompt, (tokens, attn_in, lengths))
    return (lru_state, conv_state, kv_cache)
```

```python
import functools

import jax
import jax.numpy as jnp
from jax import lax
from jax.experimental import pallas as pl
from jax.experimental.pallas import tpu as pltpu
from jax.sharding import PartitionSpec as P

H = 10
HD = 256
W = 2048
LANES_OF_TIME = 8
TAPS = 4
HALO = 16
STEP_ROWS = 32


def passed_along(block, axis, distance):
    devices = range(lax.axis_size(axis))
    route = [(i - distance, i) for i in devices if i - distance in devices]
    return lax.ppermute(block, axis, route)


def rms_norm(values, gain_vec):
    widened = values.astype(jnp.float32)
    inverse = lax.rsqrt(jnp.mean(widened * widened, axis=-1, keepdims=True) + 1e-06)
    return (widened * inverse * gain_vec).astype(jnp.bfloat16)


def rotate_keys(key_rows, positions):
    quarter = key_rows.shape[-1] // 4
    spacing = jnp.exp(-jnp.log(10000.0) * jnp.arange(quarter, dtype=jnp.float32) / quarter)
    angles = positions.astype(jnp.float32)[:, None] * spacing[None, :]
    cosine_rows = jnp.cos(angles)
    sine_rows = jnp.sin(angles)
    first_part = key_rows[:, :quarter]
    second_part = key_rows[:, quarter : 2 * quarter]
    return jnp.concatenate(
        [
            first_part * cosine_rows - second_part * sine_rows,
            second_part * cosine_rows + first_part * sine_rows,
            key_rows[:, 2 * quarter :],
        ],
        axis=1,
    )


def ordered_rows(tokens_ref, halo_ref, gain_ref, normed_ref):
    local_len = tokens_ref.shape[0]
    steps = local_len // LANES_OF_TIME
    row = lax.broadcasted_iota(jnp.int32, (normed_ref.shape[0], local_len + HALO), 0)
    col = lax.broadcasted_iota(jnp.int32, (normed_ref.shape[0], local_len + HALO), 1)
    at = lax.rem(row, LANES_OF_TIME) * steps + lax.div(row, LANES_OF_TIME) - (TAPS - 1)
    pick = (jnp.where(at < 0, at + local_len + HALO, at) == col).astype(jnp.bfloat16)
    rows = jnp.concatenate(
        [rms_norm(tokens_ref[...], gain_ref[...]), rms_norm(halo_ref[...], gain_ref[...])], axis=0
    )
    normed_ref[...] = jnp.dot(pick, rows, preferred_element_type=jnp.float32).astype(jnp.bfloat16)


def one_head(
    normed_ref, w_block, conv_w, w_a, w_i, rate, length, start, out_ref, xp_ref, xc_ref, ga_ref, gi_ref
):
    rows_ext = normed_ref.shape[0]
    local_len = xc_ref.shape[0]
    steps = local_len // LANES_OF_TIME
    projected = jnp.dot(normed_ref[...], w_block, preferred_element_type=jnp.float32).astype(
        jnp.bfloat16
    )
    xp_ref[...] = projected.astype(jnp.float32)
    row = lax.broadcasted_iota(jnp.int32, (HALO, rows_ext), 1)
    wanted = length - (TAPS - 1) + lax.broadcasted_iota(jnp.int32, (HALO, rows_ext), 0) - 2
    step = lax.div(row, LANES_OF_TIME) - (TAPS - 1)
    at = start + lax.rem(row, LANES_OF_TIME) * steps + step
    real = (step >= 0) & (step < steps) & (wanted < length) & (wanted >= length - (TAPS - 1))
    picker = (real & (at == wanted)).astype(jnp.bfloat16)
    picked = jnp.dot(picker, projected, preferred_element_type=jnp.float32)
    conv_sum = conv_w[0:1] * xp_ref[0:local_len]
    for offset in range(1, TAPS):
        shift = offset * LANES_OF_TIME
        conv_sum = conv_sum + conv_w[offset : offset + 1] * xp_ref[shift : shift + local_len]
    x_conv = conv_sum.astype(jnp.bfloat16)
    xc_ref[...] = x_conv.astype(jnp.float32)
    ga_ref[...] = jnp.dot(x_conv, w_a, preferred_element_type=jnp.float32)
    gi_ref[...] = jnp.dot(x_conv, w_i, preferred_element_type=jnp.float32)
    inner = lax.broadcasted_iota(jnp.int32, (STEP_ROWS, HD), 0)
    first_at = start + lax.rem(inner, LANES_OF_TIME) * steps + lax.div(inner, LANES_OF_TIME)

    def block(i, carry):
        state, rate_sum = carry
        rows = pl.ds(pl.multiple_of(i * STEP_ROWS, STEP_ROWS), STEP_ROWS)
        valid = first_at + i * (STEP_ROWS // LANES_OF_TIME) < length
        log_rate = rate * jax.nn.sigmoid(ga_ref[rows])
        fall = -2.0 * log_rate
        lost = 1.0 - fall * (1.0 / 6.0)
        for order in (5.0, 4.0, 3.0, 2.0):
            lost = 1.0 - fall * (1.0 / order) * lost
        lost = fall * lost
        root = lost * lax.rsqrt(jnp.maximum(lost, 1e-37))
        push = jnp.where(valid, root * jax.nn.sigmoid(gi_ref[rows]) * xc_ref[rows], 0.0)
        held = jnp.where(valid, log_rate, 0.0)
        keep = jnp.exp(held)
        for k in range(STEP_ROWS // LANES_OF_TIME):
            tile = slice(k * LANES_OF_TIME, (k + 1) * LANES_OF_TIME)
            state = keep[tile] * state + push[tile]
            rate_sum = rate_sum + held[tile]
        return state, rate_sum

    zeros = jnp.zeros((LANES_OF_TIME, HD), jnp.float32)
    state, rate_sum = lax.fori_loop(0, local_len // STEP_ROWS, block, (zeros, zeros))
    keep_all = jnp.exp(rate_sum)
    total = state[0:1]
    for s in range(1, LANES_OF_TIME):
        total = keep_all[s : s + 1] * total + state[s : s + 1]
    keep_total = jnp.exp(jnp.sum(rate_sum, axis=0, keepdims=True))
    place = lax.broadcasted_iota(jnp.int32, (LANES_OF_TIME, HD), 0)
    out_ref[...] = jnp.where(
        place == 0, keep_total, jnp.where(place == 1, total, picked[0:LANES_OF_TIME])
    )


def recurrent_kernel(
    length_ref,
    tokens_ref,
    halo_ref,
    gain_ref,
    w_ref,
    conv_ref,
    wa_ref,
    wi_ref,
    rate_ref,
    out_ref,
    normed_ref,
    *work
):
    @pl.when(pl.program_id(0) == 0)
    def _():
        ordered_rows(tokens_ref, halo_ref, gain_ref, normed_ref)

    start = lax.axis_index("seq") * tokens_ref.shape[0]
    one_head(
        normed_ref,
        w_ref[...],
        conv_ref[...],
        wa_ref[0],
        wi_ref[0],
        rate_ref[...],
        length_ref[0],
        start,
        out_ref,
        *work
    )


def recurrent(first, tokens, halo, lengths, norm_gain, w_part, conv_w, w_a, w_i, rate):
    local_len, width = tokens.shape
    part_width = w_part.shape[1]
    rows_ext = -(-(local_len + (TAPS - 1) * LANES_OF_TIME) // HALO) * HALO
    whole = lambda *shape: pl.BlockSpec(shape, lambda h: (0,) * len(shape))
    return pl.pallas_call(
        recurrent_kernel,
        grid=(part_width // HD,),
        in_specs=[
            pl.BlockSpec(memory_space=pltpu.SMEM),
            whole(local_len, width),
            whole(HALO, width),
            whole(1, width),
            pl.BlockSpec((width, HD), lambda h: (0, h)),
            pl.BlockSpec((TAPS, HD), lambda h: (0, h + first)),
            pl.BlockSpec((1, HD, HD), lambda h: (h + first, 0, 0)),
            pl.BlockSpec((1, HD, HD), lambda h: (h + first, 0, 0)),
            pl.BlockSpec((1, HD), lambda h: (0, h + first)),
        ],
        out_specs=pl.BlockSpec((LANES_OF_TIME, HD), lambda h: (0, h)),
        out_shape=jax.ShapeDtypeStruct((LANES_OF_TIME, part_width), jnp.float32),
        scratch_shapes=[
            pltpu.VMEM((rows_ext, width), jnp.bfloat16),
            pltpu.VMEM((rows_ext, HD), jnp.float32),
            pltpu.VMEM((local_len, HD), jnp.float32),
            pltpu.VMEM((local_len, HD), jnp.float32),
            pltpu.VMEM((local_len, HD), jnp.float32),
        ],
        compiler_params=pltpu.CompilerParams(vmem_limit_bytes=60 * 1024 * 1024),
        cost_estimate=pl.CostEstimate(
            flops=2 * local_len * part_width * (width + 2 * HD),
            bytes_accessed=2 * width * (local_len + part_width),
            transcendentals=6 * local_len * part_width,
        ),
    )(lengths, tokens, halo, norm_gain[None], w_part, conv_w, w_a, w_i, rate[None])


def on_device(
    tokens, attn_in, lengths, norm_gain, attn_gain, w_x, conv_w, w_a, w_i, lru_decay, w_kv
):
    local_len = tokens.shape[1]
    feature_dim = tokens.shape[2]
    seq_parts = lax.axis_size("seq")
    seq_place = lax.axis_index("seq")
    length = lengths[0]
    halo = passed_along(tokens[0, local_len - HALO :], "seq", 1)
    heads = feature_dim // HD
    early = (4 * heads) // 5
    positions = seq_place * local_len + jnp.arange(local_len, dtype=jnp.int32)
    attn_normed = rms_norm(attn_in[0], attn_gain)
    kv_full = jnp.dot(attn_normed, w_kv, preferred_element_type=jnp.float32)
    kv_rows = jnp.concatenate(
        [rotate_keys(kv_full[:, :HD], positions), kv_full[:, HD:]], axis=1
    ).astype(jnp.bfloat16)
    in_window = ((positions >= length - W) & (positions < length))[:, None]
    masked = jnp.where(in_window, kv_rows, jnp.zeros_like(kv_rows))
    by_column = lax.all_to_all(masked, "seq", split_axis=1, concat_axis=0, tiled=True)
    laps = -(-seq_parts * local_len // W)
    by_column = jnp.pad(by_column, ((0, laps * W - seq_parts * local_len), (0, 0)))
    kv_cache = by_column[:W]
    for lap in range(1, laps):
        kv_cache = kv_cache + by_column[lap * W : (lap + 1) * W]
    w_early = lax.all_gather(w_x[:, : early * HD], ("batch", "seq"), axis=0, tiled=True)
    w_early, w_local, kv_cache, halo = lax.optimization_barrier((w_early, w_x, kv_cache, halo))
    w_late = lax.all_gather(w_local[:, early * HD :], ("batch", "seq"), axis=0, tiled=True)
    w_parts = ((0, w_early), (early, w_late))
    rate = -8.0 * jax.nn.softplus(-lru_decay)
    summary = jnp.concatenate(
        [
            recurrent(first, tokens[0], halo, lengths, norm_gain, w_part, conv_w, w_a, w_i, rate)
            for first, w_part in w_parts
        ],
        axis=1,
    )
    owned_width = feature_dim // seq_parts
    gathered = lax.all_gather(summary, "seq", axis=0, tiled=True)
    owned = lax.dynamic_slice_in_dim(gathered, seq_place * owned_width, owned_width, 1)
    state = owned[1:2]
    picked = owned[2:5]
    for part in range(1, seq_parts):
        at = part * LANES_OF_TIME
        state = owned[at : at + 1] * state + owned[at + 1 : at + 2]
        picked = picked + owned[at + 2 : at + 5]
    conv_state = picked.astype(jnp.bfloat16)
    return (state, conv_state[None], kv_cache[None])


MESH_ID = pl.DeviceIdType.MESH
PLANE_ROWS = 16
CROSS_ROWS = 16
NEAR, PLANE = 0, 1


def physical_grid(mesh):
    grid = mesh.devices
    try:
        spots = [
            [(*device.coords, device.core_on_chip) for device in line] for line in grid.tolist()
        ]
    except AttributeError:
        return None
    sizes = [len({spot[k] for line in spots for spot in line}) for k in range(4)]
    low = [min(spot[k] for line in spots for spot in line) for k in range(4)]
    x_size, y_size, z_size, cores = sizes
    if (x_size, y_size, z_size, cores) != (2, 2, 4, 2) or grid.shape != (z_size * x_size * cores, y_size):
        return None
    for b, line in enumerate(spots):
        for y, spot in enumerate(line):
            want = ((b // cores) % x_size, y, b // (cores * x_size), b % cores)
            if tuple(v - l for v, l in zip(spot, low)) != want:
                return None
    return z_size, x_size, cores, y_size


class Exchange:
    def __init__(self, sizes, heads, w_buf, send_sem, recv_sem, core_send, core_recv):
        self.sizes, self.heads = sizes, heads
        self.w_buf, self.send_sem, self.recv_sem = w_buf, send_sem, recv_sem
        self.core_send, self.core_recv = core_send, core_recv
        z_size, x_size, cores, _ = sizes
        at = lax.axis_index("batch")
        self.core = lax.rem(at, cores)
        self.x = lax.rem(lax.div(at, cores), x_size)
        self.z = lax.div(at, cores * x_size)
        self.y = lax.axis_index("seq")
        self.shard_rows = w_buf.shape[5]
        self.near_rows = self.shard_rows - PLANE_ROWS
        self.is_end = (self.z == 0) | (self.z == z_size - 1)

    def device(self, z=None, x=None, core=None, y=None):
        z = self.z if z is None else z
        x = self.x if x is None else x
        core = self.core if core is None else core
        y = self.y if y is None else y
        _, x_size, cores, _ = self.sizes
        return ((z * x_size + x) * cores + core, y)

    def peers(self):
        z_size = self.sizes[0]
        along = [self.device(z=lax.rem(self.z + d, z_size)) for d in range(1, z_size)]
        return along + [
            self.device(x=1 - self.x),
            self.device(y=1 - self.y),
            self.device(x=1 - self.x, y=1 - self.y),
            self.device(core=1 - self.core),
        ]

    def blocks(self, head, z, x, y, first, rows, core=None):
        core = self.core if core is None else core
        return self.w_buf.at[head, z, x, core, y, pl.ds(first, rows)]

    def copy(self, head, stage, group, part, to):
        return pltpu.make_async_remote_copy(
            src_ref=part,
            dst_ref=part,
            send_sem=self.send_sem.at[head, stage, group],
            recv_sem=self.recv_sem.at[head, stage, group],
            device_id=to,
            device_id_type=MESH_ID,
        )

    def hand_over(self, head, part):
        pltpu.make_async_remote_copy(
            src_ref=part,
            dst_ref=part,
            send_sem=self.core_send.at[head],
            recv_sem=self.core_recv.at[head],
            device_id=self.device(core=1 - self.core),
            device_id_type=MESH_ID,
        ).start()

    def some(self, head, count, rows):
        every = slice(None)
        if count == 3:
            return self.w_buf.at[head, pl.ds(0, 3), 0, 0, 0, pl.ds(0, rows)]
        if count == 4:
            return self.w_buf.at[head, every, 0, 0, 0, pl.ds(0, rows)]
        if count == 8:
            return self.w_buf.at[head, every, every, 0, 0, pl.ds(0, rows)]
        return self.w_buf.at[head, pl.ds(0, 3), every, 0, every, pl.ds(0, rows)]

    def arrived(self, head, stage, group, count, rows):
        self.copy(head, stage, group, self.some(head, count, rows), self.device(core=1 - self.core)).wait_recv()

    def left(self, head, stage, group, count, rows):
        self.copy(head, stage, group, self.some(head, count, rows), self.device(core=1 - self.core)).wait_send()

    def routes(self, act):
        near = (PLANE_ROWS, self.near_rows)

        @pl.when(self.core == 0)
        def _():
            act("yx", PLANE_ROWS, CROSS_ROWS)
            act("xy", PLANE_ROWS + CROSS_ROWS, self.near_rows - CROSS_ROWS)

        @pl.when(self.core != 0)
        def _():
            act("yx", *near)

    def first(self, head):
        z_size = self.sizes[0]
        near = self.blocks(head, self.z, self.x, self.y, PLANE_ROWS, self.near_rows)
        for d in range(1, z_size):
            self.copy(head, 0, NEAR, near, self.device(z=lax.rem(self.z + d, z_size))).start()
        plane = self.blocks(head, self.z, self.x, self.y, 0, PLANE_ROWS)
        self.copy(head, 0, PLANE, plane, self.device(x=1 - self.x)).start()
        self.copy(head, 0, PLANE, plane, self.device(y=1 - self.y)).start()
        self.copy(head, 0, PLANE, plane, self.device(x=1 - self.x, y=1 - self.y)).start()

    def second(self, head):
        every = slice(None)
        last = self.sizes[0] - 1
        self.arrived(head, 0, NEAR, 3, self.near_rows)

        def near(order, first, rows):
            part = self.blocks(head, every, self.x, self.y, first, rows)
            to = self.device(x=1 - self.x) if order == "xy" else self.device(y=1 - self.y)
            self.copy(head, 1, NEAR, part, to).start()

        self.routes(near)
        self.arrived(head, 0, PLANE, 3, PLANE_ROWS)
        plane = self.blocks(head, self.z, every, every, 0, PLANE_ROWS)
        up = jnp.where(self.z == last, 1, self.z + 1)
        down = jnp.where(self.z == 0, last - 1, self.z - 1)
        self.copy(head, 1, PLANE, plane, self.device(z=up)).start()
        self.copy(head, 1, PLANE, plane, self.device(z=down)).start()
        self.hand_over(head, plane)

    def third(self, head):
        every = slice(None)
        last = self.sizes[0] - 1
        self.arrived(head, 1, NEAR, 4, self.near_rows)

        def near(order, first, rows):
            if order == "xy":
                part = self.blocks(head, every, every, self.y, first, rows)
                to = self.device(y=1 - self.y)
            else:
                part = self.blocks(head, every, self.x, every, first, rows)
                to = self.device(x=1 - self.x)
            self.copy(head, 2, NEAR, part, to).start()
            self.hand_over(head, part)

        self.routes(near)

        @pl.when(self.is_end)
        def _():
            self.arrived(head, 1, PLANE, 4, PLANE_ROWS)

        @pl.when(jnp.logical_not(self.is_end))
        def _():
            self.arrived(head, 1, PLANE, 12, PLANE_ROWS)
            half = (last + 1) // 2
            start = jnp.where(self.z >= half, 0, half)
            part = self.blocks(head, pl.ds(start, half), every, every, 0, PLANE_ROWS)
            self.copy(head, 2, PLANE, part, self.device(z=jnp.where(self.z >= half, last, 0))).start()

    def fourth(self, head):
        every = slice(None)
        z_size = self.sizes[0]
        self.arrived(head, 2, NEAR, 8, self.near_rows)

        def near(order, first, rows):
            if order == "xy":
                part = self.blocks(head, every, every, 1 - self.y, first, rows)
            else:
                part = self.blocks(head, every, 1 - self.x, every, first, rows)
            self.hand_over(head, part)

        self.routes(near)

        @pl.when(self.is_end)
        def _():
            self.arrived(head, 2, PLANE, 8, PLANE_ROWS)

        for d in range(1, z_size):
            self.hand_over(head, self.blocks(head, lax.rem(self.z + d, z_size), every, every, 0, PLANE_ROWS))

    def handed(self, head, core):
        every = slice(None)
        part = self.w_buf.at[head, every, every, core]
        return pltpu.make_async_remote_copy(
            src_ref=part,
            dst_ref=part,
            send_sem=self.core_send.at[head],
            recv_sem=self.core_recv.at[head],
            device_id=self.device(core=1 - self.core),
            device_id_type=MESH_ID,
        )

    def ready(self, head):
        self.handed(head, 1 - self.core).wait_recv()

    def settled(self, head):
        self.left(head, 0, NEAR, 3, self.near_rows)
        self.left(head, 0, PLANE, 3, PLANE_ROWS)
        self.left(head, 1, NEAR, 4, self.near_rows)
        self.left(head, 1, PLANE, 8, PLANE_ROWS)
        self.left(head, 2, NEAR, 8, self.near_rows)

        @pl.when(jnp.logical_not(self.is_end))
        def _():
            self.left(head, 2, PLANE, 8, PLANE_ROWS)

        self.handed(head, self.core).wait_send()


def prefill_kernel(
    sizes,
    length_ref,
    tokens_hbm,
    attn_hbm,
    norm_gain_ref,
    attn_gain_ref,
    w_hbm,
    conv_ref,
    wa_hbm,
    wi_hbm,
    decay_ref,
    wkv_hbm,
    state_ref,
    cache_ref,
    w_buf,
    tokens_v,
    attn_v,
    wkv_v,
    wa_v,
    wi_v,
    halo_v,
    rows_v,
    normed_v,
    kv_v,
    zeros_v,
    xp_v,
    xc_v,
    ga_v,
    gi_v,
    summary_v,
    theirs_v,
    turn_v,
    send_sem,
    recv_sem,
    core_send,
    core_recv,
    load_sem,
    side_send,
    side_recv,
):
    heads = w_buf.shape[0]
    local_len = tokens_v.shape[0]
    seq_parts = sizes[3]
    ex = Exchange(sizes, heads, w_buf, send_sem, recv_sem, core_send, core_recv)
    y = ex.y
    start = y * local_len
    beside = ex.device(y=1 - y)

    shard = [
        pltpu.make_async_copy(
            w_hbm.at[:, pl.ds(h * HD, HD)], w_buf.at[h, ex.z, ex.x, ex.core, y], load_sem.at[h]
        )
        for h in range(heads)
    ]
    loads = [
        pltpu.make_async_copy(source, target, load_sem.at[heads + i])
        for i, (source, target) in enumerate(
            (
                (tokens_hbm, tokens_v),
                (attn_hbm, attn_v),
                (wkv_hbm, wkv_v),
                (wa_hbm, wa_v),
                (wi_hbm, wi_v),
            )
        )
    ]
    for copy in shard + [loads[1], loads[2], loads[0], loads[3], loads[4]]:
        copy.start()

    barrier = pltpu.get_barrier_semaphore()
    peers = ex.peers()
    for peer in peers:
        pl.semaphore_signal(barrier, inc=1, device_id=peer, device_id_type=MESH_ID)

    zeros_v[...] = jnp.zeros_like(zeros_v)
    quarter = HD // 4
    lane = lax.broadcasted_iota(jnp.int32, (1, 2 * quarter), 1)
    spacing = jnp.exp(
        (-jnp.log(10000.0) / quarter) * lax.rem(lane, quarter).astype(jnp.float32)
    )
    half_len = local_len // 2
    fine = lax.broadcasted_iota(jnp.int32, (half_len, 2 * quarter), 0).astype(jnp.float32) * spacing
    turn_v[0] = jnp.cos(fine)
    turn_v[1] = jnp.sin(fine)

    for copy in shard:
        copy.wait()
    pl.semaphore_wait(barrier, len(peers))
    for h in range(4):
        ex.first(h)

    length = length_ref[0]

    def kv_half(k):
        rows = slice(k * half_len, (k + 1) * half_len)
        normed = rms_norm(attn_v[rows], attn_gain_ref[...])
        full = jnp.dot(normed, wkv_v[...], preferred_element_type=jnp.float32)
        place = start + k * half_len
        coarse = place.astype(jnp.float32) * spacing
        cos_c, sin_c = jnp.cos(coarse), jnp.sin(coarse)
        cosine = cos_c * turn_v[0] - sin_c * turn_v[1]
        sine = sin_c * turn_v[0] + cos_c * turn_v[1]
        sine = jnp.where(lane < quarter, -sine, sine)
        at = place + lax.broadcasted_iota(jnp.int32, (half_len, 1), 0)
        window = (at >= length - W) & (at < length)
        turned = full[:, : 2 * quarter]
        other = pltpu.roll(turned, quarter, axis=1)
        turned = turned * cosine + other * sine

        def put(half, columns, values):
            kv_v[half, rows, columns] = jnp.where(window, values, 0.0).astype(jnp.bfloat16)

        put(0, slice(0, 2 * quarter), turned)
        put(0, slice(2 * quarter, HD), full[:, 2 * quarter : HD])
        put(1, slice(0, HD), full[:, HD:])

    halo_copy = pltpu.make_async_remote_copy(
        src_ref=tokens_v.at[pl.ds(local_len - HALO, HALO)],
        dst_ref=halo_v,
        send_sem=side_send.at[0],
        recv_sem=side_recv.at[0],
        device_id=beside,
        device_id_type=MESH_ID,
    )
    loads[1].wait()
    loads[2].wait()
    kv_half(0)
    ex.second(0)
    loads[0].wait()

    @pl.when(y == 0)
    def _():
        halo_copy.start()
        halo_v[...] = jnp.zeros_like(halo_v)

    kv_half(1)
    ex.third(0)
    ex.second(1)
    kv_copy = pltpu.make_async_remote_copy(
        src_ref=kv_v.at[1 - y],
        dst_ref=cache_ref.at[pl.ds(start, local_len)],
        send_sem=side_send.at[1],
        recv_sem=side_recv.at[1],
        device_id=beside,
        device_id_type=MESH_ID,
    )
    kv_copy.start()
    kept = pltpu.make_async_copy(kv_v.at[y], cache_ref.at[pl.ds(start, local_len)], load_sem.at[heads + 5])
    kept.start()
    rest = seq_parts * local_len
    blank = pltpu.make_async_copy(
        zeros_v, cache_ref.at[pl.ds(rest, cache_ref.shape[0] - rest)], load_sem.at[heads + 6]
    )
    blank.start()

    norm_step = 64

    def norm_rows(i, carry):
        rows = pl.ds(pl.multiple_of(i * norm_step, norm_step), norm_step)
        rows_v[rows] = rms_norm(tokens_v[rows], norm_gain_ref[...])
        return carry

    lax.fori_loop(0, local_len // norm_step, norm_rows, 0)
    ex.second(2)
    ex.third(1)

    @pl.when(y != 0)
    def _():
        halo_copy.wait_recv()

    steps = local_len // LANES_OF_TIME
    rows_ext = normed_v.shape[0]
    row = lax.broadcasted_iota(jnp.int32, (rows_ext, local_len), 0)
    col = lax.broadcasted_iota(jnp.int32, (rows_ext, local_len), 1)
    at = lax.rem(row, LANES_OF_TIME) * steps + lax.div(row, LANES_OF_TIME) - (TAPS - 1)
    pick = (at == col).astype(jnp.bfloat16)

    def reorder(i, carry):
        columns = pl.ds(pl.multiple_of(i * HD, HD), HD)
        normed_v[:, columns] = jnp.dot(
            pick, rows_v[:, columns], preferred_element_type=jnp.float32
        ).astype(jnp.bfloat16)
        return carry

    lax.fori_loop(0, heads, reorder, 0)
    edge = 2 * HALO
    row = lax.broadcasted_iota(jnp.int32, (edge, HALO), 0)
    col = lax.broadcasted_iota(jnp.int32, (edge, HALO), 1)
    at = lax.div(row, LANES_OF_TIME) - (TAPS - 1)
    early = ((lax.rem(row, LANES_OF_TIME) == 0) & (at < 0) & (at + HALO == col)).astype(jnp.bfloat16)
    halo_rows = rms_norm(halo_v[...], norm_gain_ref[...])
    before = jnp.dot(early, halo_rows, preferred_element_type=jnp.float32)
    normed_v[0:edge] = (normed_v[0:edge].astype(jnp.float32) + before).astype(jnp.bfloat16)
    ex.fourth(0)
    loads[3].wait()
    loads[4].wait()

    per_owner = heads // seq_parts

    def summary_copy(head, slot):
        return pltpu.make_async_remote_copy(
            src_ref=summary_v.at[head],
            dst_ref=theirs_v.at[slot],
            send_sem=side_send.at[2],
            recv_sem=side_recv.at[2],
            device_id=beside,
            device_id_type=MESH_ID,
        )

    inner = lax.broadcasted_iota(jnp.int32, (STEP_ROWS, HD), 0)
    first_at = start + lax.rem(inner, LANES_OF_TIME) * steps + lax.div(inner, LANES_OF_TIME)

    def head_step(head, carry):
        ex.ready(head)

        @pl.when(head + 3 < heads)
        def _():
            ex.second(head + 3)

        @pl.when(head + 2 < heads)
        def _():
            ex.third(head + 2)

        @pl.when(head + 4 < heads)
        def _():
            ex.first(head + 4)

        columns = pl.ds(pl.multiple_of(head * HD, HD), HD)
        w_block = w_buf[head].reshape(normed_v.shape[1], HD)
        projected = jnp.dot(
            normed_v[...], w_block, preferred_element_type=jnp.float32
        ).astype(jnp.bfloat16)
        xp_v[...] = projected.astype(jnp.float32)
        row = lax.broadcasted_iota(jnp.int32, (HALO, rows_ext), 1)
        wanted = length - (TAPS - 1) + lax.broadcasted_iota(jnp.int32, (HALO, rows_ext), 0) - 2
        step = lax.div(row, LANES_OF_TIME) - (TAPS - 1)
        at = start + lax.rem(row, LANES_OF_TIME) * steps + step
        real = (step >= 0) & (step < steps) & (wanted < length) & (wanted >= length - (TAPS - 1))
        picker = (real & (at == wanted)).astype(jnp.bfloat16)
        picked = jnp.dot(picker, projected, preferred_element_type=jnp.float32)
        conv_w = conv_ref[:, columns]
        conv_sum = conv_w[0:1] * xp_v[0:local_len]
        for offset in range(1, TAPS):
            shift = offset * LANES_OF_TIME
            conv_sum = conv_sum + conv_w[offset : offset + 1] * xp_v[shift : shift + local_len]
        x_conv = conv_sum.astype(jnp.bfloat16)
        xc_v[...] = x_conv.astype(jnp.float32)
        ga_v[...] = jnp.dot(x_conv, wa_v[head], preferred_element_type=jnp.float32)
        gi_v[...] = jnp.dot(x_conv, wi_v[head], preferred_element_type=jnp.float32)

        @pl.when(head + 1 < heads)
        def _():
            ex.fourth(head + 1)

        rate = -8.0 * jax.nn.softplus(-decay_ref[:, columns])

        def block(i, carry):
            state, rate_sum = carry
            rows = pl.ds(pl.multiple_of(i * STEP_ROWS, STEP_ROWS), STEP_ROWS)
            valid = first_at + i * (STEP_ROWS // LANES_OF_TIME) < length
            log_rate = rate * jax.nn.sigmoid(ga_v[rows])
            fall = -2.0 * log_rate
            lost = 1.0 - fall * (1.0 / 6.0)
            for order in (5.0, 4.0, 3.0, 2.0):
                lost = 1.0 - fall * (1.0 / order) * lost
            lost = fall * lost
            root = lost * lax.rsqrt(jnp.maximum(lost, 1e-37))
            push = jnp.where(valid, root * jax.nn.sigmoid(gi_v[rows]) * xc_v[rows], 0.0)
            held = jnp.where(valid, log_rate, 0.0)
            keep = jnp.exp(held)
            for k in range(STEP_ROWS // LANES_OF_TIME):
                tile = slice(k * LANES_OF_TIME, (k + 1) * LANES_OF_TIME)
                state = keep[tile] * state + push[tile]
                rate_sum = rate_sum + held[tile]
            return state, rate_sum

        zeros = jnp.zeros((LANES_OF_TIME, HD), jnp.float32)
        state, rate_sum = lax.fori_loop(0, local_len // STEP_ROWS, block, (zeros, zeros))
        keep_all = jnp.exp(rate_sum)
        total = state[0:1]
        for s in range(1, LANES_OF_TIME):
            total = keep_all[s : s + 1] * total + state[s : s + 1]
        keep_total = jnp.exp(jnp.sum(rate_sum, axis=0, keepdims=True))
        place = lax.broadcasted_iota(jnp.int32, (LANES_OF_TIME, HD), 0)
        summary_v[head] = jnp.where(
            place == 0, keep_total, jnp.where(place == 1, total, picked[0:LANES_OF_TIME])
        )

        @pl.when(lax.div(head, per_owner) != y)
        def _():
            summary_copy(head, lax.rem(head, per_owner)).start()

        ex.settled(head)
        return carry

    lax.fori_loop(0, heads, head_step, 0)

    every = summary_v.at[pl.ds(0, per_owner)]
    exchanged = pltpu.make_async_remote_copy(
        src_ref=every,
        dst_ref=theirs_v,
        send_sem=side_send.at[2],
        recv_sem=side_recv.at[2],
        device_id=beside,
        device_id_type=MESH_ID,
    )
    exchanged.wait_recv()
    place = lax.broadcasted_iota(jnp.int32, (LANES_OF_TIME, HD), 0)
    for k in range(per_owner):
        own = summary_v[y * per_owner + k]
        got = theirs_v[k]
        head_part = jnp.where(y == 0, own, got)
        tail_part = jnp.where(y == 0, got, own)
        state = tail_part[0:1] * head_part[1:2] + tail_part[1:2]
        state_ref[:, k * HD : (k + 1) * HD] = jnp.where(place == 0, state, head_part + tail_part)
    exchanged.wait_send()

    @pl.when(y == 0)
    def _():
        halo_copy.wait_send()

    kv_copy.wait()
    kept.wait()
    blank.wait()


def gathered_on_device(
    sizes, tokens, attn_in, lengths, norm_gain, attn_gain, w_x, conv_w, w_a, w_i, lru_decay, w_kv
):
    local_len, width = tokens.shape[1:]
    z_size, x_size, cores, seq_parts = sizes
    heads = width // HD
    rows_ext = -(-(local_len + (TAPS - 1) * LANES_OF_TIME) // HALO) * HALO
    anywhere = pl.BlockSpec(memory_space=pl.ANY)
    vmem = pl.BlockSpec(memory_space=pltpu.VMEM)
    owned = width // seq_parts
    per_owner = heads // seq_parts
    half = w_kv.shape[1] // seq_parts
    summary, cache = pl.pallas_call(
        functools.partial(prefill_kernel, sizes),
        in_specs=[
            pl.BlockSpec(memory_space=pltpu.SMEM),
            anywhere,
            anywhere,
            vmem,
            vmem,
            anywhere,
            vmem,
            anywhere,
            anywhere,
            vmem,
            anywhere,
        ],
        out_specs=(vmem, anywhere),
        out_shape=(
            jax.ShapeDtypeStruct((LANES_OF_TIME, owned), jnp.float32),
            jax.ShapeDtypeStruct((W, half), jnp.bfloat16),
        ),
        scratch_shapes=[
            pltpu.VMEM((heads, z_size, x_size, cores, seq_parts, w_x.shape[0], HD), jnp.bfloat16),
            pltpu.VMEM((local_len, width), jnp.bfloat16),
            pltpu.VMEM((local_len, width), jnp.bfloat16),
            pltpu.VMEM(w_kv.shape, jnp.bfloat16),
            pltpu.VMEM(w_a.shape, jnp.bfloat16),
            pltpu.VMEM(w_i.shape, jnp.bfloat16),
            pltpu.VMEM((HALO, width), jnp.bfloat16),
            pltpu.VMEM((local_len, width), jnp.bfloat16),
            pltpu.VMEM((rows_ext, width), jnp.bfloat16),
            pltpu.VMEM((2, local_len, half), jnp.bfloat16),
            pltpu.VMEM((W - seq_parts * local_len, half), jnp.bfloat16),
            pltpu.VMEM((rows_ext, HD), jnp.float32),
            pltpu.VMEM((local_len, HD), jnp.float32),
            pltpu.VMEM((local_len, HD), jnp.float32),
            pltpu.VMEM((local_len, HD), jnp.float32),
            pltpu.VMEM((heads, LANES_OF_TIME, HD), jnp.float32),
            pltpu.VMEM((per_owner, LANES_OF_TIME, HD), jnp.float32),
            pltpu.VMEM((2, local_len // 2, HD // 2), jnp.float32),
            pltpu.SemaphoreType.DMA((heads, 3, 2)),
            pltpu.SemaphoreType.DMA((heads, 3, 2)),
            pltpu.SemaphoreType.DMA((heads,)),
            pltpu.SemaphoreType.DMA((heads,)),
            pltpu.SemaphoreType.DMA((heads + 7,)),
            pltpu.SemaphoreType.DMA((3,)),
            pltpu.SemaphoreType.DMA((3,)),
        ],
        compiler_params=pltpu.CompilerParams(
            collective_id=0, has_side_effects=True, vmem_limit_bytes=60 * 1024 * 1024
        ),
    )(
        lengths,
        tokens[0],
        attn_in[0],
        norm_gain[None],
        attn_gain[None],
        w_x,
        conv_w,
        w_a,
        w_i,
        lru_decay[None],
        w_kv,
    )
    return summary[0:1], summary[2 : 2 + TAPS - 1].astype(jnp.bfloat16)[None], cache[None]


def fits(mesh, sizes, tokens, w_x, w_kv):
    if sizes is None:
        return False
    _, length, width = tokens.shape
    devices = mesh.size
    seq_parts = mesh.shape["seq"]
    return (
        length < W
        and width % (HD * seq_parts) == 0
        and w_x.shape[0] % (devices * HALO) == 0
        and w_x.shape[0] // devices > PLANE_ROWS + CROSS_ROWS
        and w_kv.shape[1] == seq_parts * HD
        and tokens.shape[0] == mesh.shape["batch"]
    )


def solution(mesh):
    in_specs = (
        P("batch", "seq", None),
        P("batch", "seq", None),
        P("batch"),
        P(),
        P(),
        P(("batch", "seq"), None),
        P(),
        P(),
        P(),
        P(),
        P(),
    )
    out_specs = (P("batch", "seq"), P("batch", None, "seq"), P("batch", None, "seq"))
    sizes = physical_grid(mesh)

    def run(*arrays):
        tokens, w_x, w_kv = arrays[0], arrays[5], arrays[10]
        body = on_device
        if fits(mesh, sizes, tokens, w_x, w_kv):
            body = functools.partial(gathered_on_device, sizes)
        return jax.shard_map(
            body, mesh=mesh, in_specs=in_specs, out_specs=out_specs, check_vma=False
        )(*arrays)

    return run
```

```python
import functools

import jax
import jax.numpy as jnp
from jax import lax
from jax.experimental import pallas as pl
from jax.experimental.pallas import tpu as pltpu
from jax.sharding import PartitionSpec as P

H = 10
HD = 256
W = 2048
LANES_OF_TIME = 8
TAPS = 4
HALO = 16
STEP_ROWS = 32


def passed_along(block, axis, distance):
    devices = range(lax.axis_size(axis))
    route = [(i - distance, i) for i in devices if i - distance in devices]
    return lax.ppermute(block, axis, route)


def rms_norm(values, gain_vec):
    widened = values.astype(jnp.float32)
    inverse = lax.rsqrt(jnp.mean(widened * widened, axis=-1, keepdims=True) + 1e-06)
    return (widened * inverse * gain_vec).astype(jnp.bfloat16)


def rotate_keys(key_rows, positions):
    quarter = key_rows.shape[-1] // 4
    spacing = jnp.exp(-jnp.log(10000.0) * jnp.arange(quarter, dtype=jnp.float32) / quarter)
    angles = positions.astype(jnp.float32)[:, None] * spacing[None, :]
    cosine_rows = jnp.cos(angles)
    sine_rows = jnp.sin(angles)
    first_part = key_rows[:, :quarter]
    second_part = key_rows[:, quarter : 2 * quarter]
    return jnp.concatenate(
        [
            first_part * cosine_rows - second_part * sine_rows,
            second_part * cosine_rows + first_part * sine_rows,
            key_rows[:, 2 * quarter :],
        ],
        axis=1,
    )


def ordered_rows(tokens_ref, halo_ref, gain_ref, normed_ref):
    local_len = tokens_ref.shape[0]
    steps = local_len // LANES_OF_TIME
    row = lax.broadcasted_iota(jnp.int32, (normed_ref.shape[0], local_len + HALO), 0)
    col = lax.broadcasted_iota(jnp.int32, (normed_ref.shape[0], local_len + HALO), 1)
    at = lax.rem(row, LANES_OF_TIME) * steps + lax.div(row, LANES_OF_TIME) - (TAPS - 1)
    pick = (jnp.where(at < 0, at + local_len + HALO, at) == col).astype(jnp.bfloat16)
    rows = jnp.concatenate(
        [rms_norm(tokens_ref[...], gain_ref[...]), rms_norm(halo_ref[...], gain_ref[...])], axis=0
    )
    normed_ref[...] = jnp.dot(pick, rows, preferred_element_type=jnp.float32).astype(jnp.bfloat16)


def one_head(
    normed_ref, w_block, conv_w, w_a, w_i, rate, length, start, out_ref, xp_ref, xc_ref, ga_ref, gi_ref
):
    rows_ext = normed_ref.shape[0]
    local_len = xc_ref.shape[0]
    steps = local_len // LANES_OF_TIME
    projected = jnp.dot(normed_ref[...], w_block, preferred_element_type=jnp.float32).astype(
        jnp.bfloat16
    )
    xp_ref[...] = projected.astype(jnp.float32)
    row = lax.broadcasted_iota(jnp.int32, (HALO, rows_ext), 1)
    wanted = length - (TAPS - 1) + lax.broadcasted_iota(jnp.int32, (HALO, rows_ext), 0) - 2
    step = lax.div(row, LANES_OF_TIME) - (TAPS - 1)
    at = start + lax.rem(row, LANES_OF_TIME) * steps + step
    real = (step >= 0) & (step < steps) & (wanted < length) & (wanted >= length - (TAPS - 1))
    picker = (real & (at == wanted)).astype(jnp.bfloat16)
    picked = jnp.dot(picker, projected, preferred_element_type=jnp.float32)
    conv_sum = conv_w[0:1] * xp_ref[0:local_len]
    for offset in range(1, TAPS):
        shift = offset * LANES_OF_TIME
        conv_sum = conv_sum + conv_w[offset : offset + 1] * xp_ref[shift : shift + local_len]
    x_conv = conv_sum.astype(jnp.bfloat16)
    xc_ref[...] = x_conv.astype(jnp.float32)
    ga_ref[...] = jnp.dot(x_conv, w_a, preferred_element_type=jnp.float32)
    gi_ref[...] = jnp.dot(x_conv, w_i, preferred_element_type=jnp.float32)
    inner = lax.broadcasted_iota(jnp.int32, (STEP_ROWS, HD), 0)
    first_at = start + lax.rem(inner, LANES_OF_TIME) * steps + lax.div(inner, LANES_OF_TIME)

    def block(i, carry):
        state, rate_sum = carry
        rows = pl.ds(pl.multiple_of(i * STEP_ROWS, STEP_ROWS), STEP_ROWS)
        valid = first_at + i * (STEP_ROWS // LANES_OF_TIME) < length
        log_rate = rate * jax.nn.sigmoid(ga_ref[rows])
        fall = -2.0 * log_rate
        lost = 1.0 - fall * (1.0 / 6.0)
        for order in (5.0, 4.0, 3.0, 2.0):
            lost = 1.0 - fall * (1.0 / order) * lost
        lost = fall * lost
        root = lost * lax.rsqrt(jnp.maximum(lost, 1e-37))
        push = jnp.where(valid, root * jax.nn.sigmoid(gi_ref[rows]) * xc_ref[rows], 0.0)
        held = jnp.where(valid, log_rate, 0.0)
        keep = jnp.exp(held)
        for k in range(STEP_ROWS // LANES_OF_TIME):
            tile = slice(k * LANES_OF_TIME, (k + 1) * LANES_OF_TIME)
            state = keep[tile] * state + push[tile]
            rate_sum = rate_sum + held[tile]
        return state, rate_sum

    zeros = jnp.zeros((LANES_OF_TIME, HD), jnp.float32)
    state, rate_sum = lax.fori_loop(0, local_len // STEP_ROWS, block, (zeros, zeros))
    keep_all = jnp.exp(rate_sum)
    total = state[0:1]
    for s in range(1, LANES_OF_TIME):
        total = keep_all[s : s + 1] * total + state[s : s + 1]
    keep_total = jnp.exp(jnp.sum(rate_sum, axis=0, keepdims=True))
    place = lax.broadcasted_iota(jnp.int32, (LANES_OF_TIME, HD), 0)
    out_ref[...] = jnp.where(
        place == 0, keep_total, jnp.where(place == 1, total, picked[0:LANES_OF_TIME])
    )


def recurrent_kernel(
    length_ref,
    tokens_ref,
    halo_ref,
    gain_ref,
    w_ref,
    conv_ref,
    wa_ref,
    wi_ref,
    rate_ref,
    out_ref,
    normed_ref,
    *work
):
    @pl.when(pl.program_id(0) == 0)
    def _():
        ordered_rows(tokens_ref, halo_ref, gain_ref, normed_ref)

    start = lax.axis_index("seq") * tokens_ref.shape[0]
    one_head(
        normed_ref,
        w_ref[...],
        conv_ref[...],
        wa_ref[0],
        wi_ref[0],
        rate_ref[...],
        length_ref[0],
        start,
        out_ref,
        *work
    )


def recurrent(first, tokens, halo, lengths, norm_gain, w_part, conv_w, w_a, w_i, rate):
    local_len, width = tokens.shape
    part_width = w_part.shape[1]
    rows_ext = -(-(local_len + (TAPS - 1) * LANES_OF_TIME) // HALO) * HALO
    whole = lambda *shape: pl.BlockSpec(shape, lambda h: (0,) * len(shape))
    return pl.pallas_call(
        recurrent_kernel,
        grid=(part_width // HD,),
        in_specs=[
            pl.BlockSpec(memory_space=pltpu.SMEM),
            whole(local_len, width),
            whole(HALO, width),
            whole(1, width),
            pl.BlockSpec((width, HD), lambda h: (0, h)),
            pl.BlockSpec((TAPS, HD), lambda h: (0, h + first)),
            pl.BlockSpec((1, HD, HD), lambda h: (h + first, 0, 0)),
            pl.BlockSpec((1, HD, HD), lambda h: (h + first, 0, 0)),
            pl.BlockSpec((1, HD), lambda h: (0, h + first)),
        ],
        out_specs=pl.BlockSpec((LANES_OF_TIME, HD), lambda h: (0, h)),
        out_shape=jax.ShapeDtypeStruct((LANES_OF_TIME, part_width), jnp.float32),
        scratch_shapes=[
            pltpu.VMEM((rows_ext, width), jnp.bfloat16),
            pltpu.VMEM((rows_ext, HD), jnp.float32),
            pltpu.VMEM((local_len, HD), jnp.float32),
            pltpu.VMEM((local_len, HD), jnp.float32),
            pltpu.VMEM((local_len, HD), jnp.float32),
        ],
        compiler_params=pltpu.CompilerParams(vmem_limit_bytes=60 * 1024 * 1024),
        cost_estimate=pl.CostEstimate(
            flops=2 * local_len * part_width * (width + 2 * HD),
            bytes_accessed=2 * width * (local_len + part_width),
            transcendentals=6 * local_len * part_width,
        ),
    )(lengths, tokens, halo, norm_gain[None], w_part, conv_w, w_a, w_i, rate[None])


def on_device(
    tokens, attn_in, lengths, norm_gain, attn_gain, w_x, conv_w, w_a, w_i, lru_decay, w_kv
):
    local_len = tokens.shape[1]
    feature_dim = tokens.shape[2]
    seq_parts = lax.axis_size("seq")
    seq_place = lax.axis_index("seq")
    length = lengths[0]
    halo = passed_along(tokens[0, local_len - HALO :], "seq", 1)
    heads = feature_dim // HD
    early = (4 * heads) // 5
    positions = seq_place * local_len + jnp.arange(local_len, dtype=jnp.int32)
    attn_normed = rms_norm(attn_in[0], attn_gain)
    kv_full = jnp.dot(attn_normed, w_kv, preferred_element_type=jnp.float32)
    kv_rows = jnp.concatenate(
        [rotate_keys(kv_full[:, :HD], positions), kv_full[:, HD:]], axis=1
    ).astype(jnp.bfloat16)
    in_window = ((positions >= length - W) & (positions < length))[:, None]
    masked = jnp.where(in_window, kv_rows, jnp.zeros_like(kv_rows))
    by_column = lax.all_to_all(masked, "seq", split_axis=1, concat_axis=0, tiled=True)
    laps = -(-seq_parts * local_len // W)
    by_column = jnp.pad(by_column, ((0, laps * W - seq_parts * local_len), (0, 0)))
    kv_cache = by_column[:W]
    for lap in range(1, laps):
        kv_cache = kv_cache + by_column[lap * W : (lap + 1) * W]
    w_early = lax.all_gather(w_x[:, : early * HD], ("batch", "seq"), axis=0, tiled=True)
    w_early, w_local, kv_cache, halo = lax.optimization_barrier((w_early, w_x, kv_cache, halo))
    w_late = lax.all_gather(w_local[:, early * HD :], ("batch", "seq"), axis=0, tiled=True)
    w_parts = ((0, w_early), (early, w_late))
    rate = -8.0 * jax.nn.softplus(-lru_decay)
    summary = jnp.concatenate(
        [
            recurrent(first, tokens[0], halo, lengths, norm_gain, w_part, conv_w, w_a, w_i, rate)
            for first, w_part in w_parts
        ],
        axis=1,
    )
    owned_width = feature_dim // seq_parts
    gathered = lax.all_gather(summary, "seq", axis=0, tiled=True)
    owned = lax.dynamic_slice_in_dim(gathered, seq_place * owned_width, owned_width, 1)
    state = owned[1:2]
    picked = owned[2:5]
    for part in range(1, seq_parts):
        at = part * LANES_OF_TIME
        state = owned[at : at + 1] * state + owned[at + 1 : at + 2]
        picked = picked + owned[at + 2 : at + 5]
    conv_state = picked.astype(jnp.bfloat16)
    return (state, conv_state[None], kv_cache[None])


MESH_ID = pl.DeviceIdType.MESH
PLANE_ROWS = 16
WIDE_PLANE_ROWS = 32
WIDE_HEADS = 2
NEAR, PLANE = 0, 1


def physical_grid(mesh):
    grid = mesh.devices
    try:
        spots = [
            [(*device.coords, device.core_on_chip) for device in line] for line in grid.tolist()
        ]
    except AttributeError:
        return None
    sizes = [len({spot[k] for line in spots for spot in line}) for k in range(4)]
    low = [min(spot[k] for line in spots for spot in line) for k in range(4)]
    x_size, y_size, z_size, cores = sizes
    if (x_size, y_size, z_size, cores) != (2, 2, 4, 2) or grid.shape != (z_size * x_size * cores, y_size):
        return None
    for b, line in enumerate(spots):
        for y, spot in enumerate(line):
            want = ((b // cores) % x_size, y, b // (cores * x_size), b % cores)
            if tuple(v - l for v, l in zip(spot, low)) != want:
                return None
    return z_size, x_size, cores, y_size


def scoped(method):
    @functools.wraps(method)
    def inside(*args):
        with jax.named_scope(method.__name__):
            return method(*args)

    return inside


def by_width(method):
    @functools.wraps(method)
    def inside(exchange, head):
        border = exchange.heads - WIDE_HEADS
        with jax.named_scope(method.__name__):
            if isinstance(head, int):
                method(exchange, head, PLANE_ROWS if head < border else WIDE_PLANE_ROWS)
                return
            for wide in (False, True):

                @pl.when((head >= border) == wide)
                def _():
                    method(exchange, head, WIDE_PLANE_ROWS if wide else PLANE_ROWS)

    return inside


class Exchange:
    def __init__(self, sizes, heads, w_buf, send_sem, recv_sem, core_send, core_recv):
        self.sizes, self.heads = sizes, heads
        self.w_buf, self.send_sem, self.recv_sem = w_buf, send_sem, recv_sem
        self.core_send, self.core_recv = core_send, core_recv
        z_size, x_size, cores, _ = sizes
        at = lax.axis_index("batch")
        self.core = lax.rem(at, cores)
        self.x = lax.rem(lax.div(at, cores), x_size)
        self.z = lax.div(at, cores * x_size)
        self.y = lax.axis_index("seq")
        self.shard_rows = w_buf.shape[5]
        self.is_end = (self.z == 0) | (self.z == z_size - 1)

    def device(self, z=None, x=None, core=None, y=None):
        z = self.z if z is None else z
        x = self.x if x is None else x
        core = self.core if core is None else core
        y = self.y if y is None else y
        _, x_size, cores, _ = self.sizes
        return ((z * x_size + x) * cores + core, y)

    def peers(self):
        z_size = self.sizes[0]
        along = [self.device(z=lax.rem(self.z + d, z_size)) for d in range(1, z_size)]
        return along + [
            self.device(x=1 - self.x),
            self.device(y=1 - self.y),
            self.device(x=1 - self.x, y=1 - self.y),
            self.device(core=1 - self.core),
        ]

    def blocks(self, head, z, x, y, first, rows, core=None):
        core = self.core if core is None else core
        return self.w_buf.at[head, z, x, core, y, pl.ds(first, rows)]

    def copy(self, head, stage, group, plane_rows, part, to):
        wide = 0 if plane_rows == PLANE_ROWS else 1
        return pltpu.make_async_remote_copy(
            src_ref=part,
            dst_ref=part,
            send_sem=self.send_sem.at[stage, group, wide],
            recv_sem=self.recv_sem.at[head, stage if group == NEAR or stage != 1 else 3],
            device_id=to,
            device_id_type=MESH_ID,
        )

    def hand_over(self, head, part):
        pltpu.make_async_remote_copy(
            src_ref=part,
            dst_ref=part,
            send_sem=self.core_send.at[0],
            recv_sem=self.core_recv.at[head],
            device_id=self.device(core=1 - self.core),
            device_id_type=MESH_ID,
        ).start()

    def some(self, head, count, rows):
        every = slice(None)
        if count == 2:
            return self.w_buf.at[head, pl.ds(0, 2), 0, 0, 0, pl.ds(0, rows)]
        if count == 3:
            return self.w_buf.at[head, pl.ds(0, 3), 0, 0, 0, pl.ds(0, rows)]
        if count == 4:
            return self.w_buf.at[head, every, 0, 0, 0, pl.ds(0, rows)]
        if count == 8:
            return self.w_buf.at[head, every, every, 0, 0, pl.ds(0, rows)]
        return self.w_buf.at[head, pl.ds(0, 3), every, 0, every, pl.ds(0, rows)]

    def arrived(self, head, stage, group, count, rows):
        part = self.some(head, count, rows)
        self.copy(head, stage, group, PLANE_ROWS, part, self.device(core=1 - self.core)).wait_recv()

    def left(self, stage, group, plane_rows, count, rows):
        border = self.heads - WIDE_HEADS
        span = pl.ds(0, border) if plane_rows == PLANE_ROWS else pl.ds(border, WIDE_HEADS)
        part = self.some(span, count, rows)
        self.copy(0, stage, group, plane_rows, part, self.device(core=1 - self.core)).wait_send()

    def routes(self, plane_rows, act):
        wide = WIDE_PLANE_ROWS

        @pl.when(self.core == 0)
        def _():
            if plane_rows < wide:
                act("yx", plane_rows, wide - plane_rows)
            act("xy", wide, self.shard_rows - wide)

        @pl.when(self.core != 0)
        def _():
            act("yx", plane_rows, self.shard_rows - plane_rows)

    @by_width
    def first_near(self, head, plane_rows):
        near = self.blocks(head, self.z, self.x, self.y, plane_rows, self.shard_rows - plane_rows)
        for d in range(1, self.sizes[0]):
            to = self.device(z=lax.rem(self.z + d, self.sizes[0]))
            self.copy(head, 0, NEAR, plane_rows, near, to).start()

    @by_width
    def first_plane(self, head, plane_rows):
        plane = self.blocks(head, self.z, self.x, self.y, 0, plane_rows)
        self.copy(head, 0, PLANE, plane_rows, plane, self.device(x=1 - self.x)).start()
        self.copy(head, 0, PLANE, plane_rows, plane, self.device(y=1 - self.y)).start()
        self.copy(head, 0, PLANE, plane_rows, plane, self.device(x=1 - self.x, y=1 - self.y)).start()

    @by_width
    def second(self, head, plane_rows):
        every = slice(None)
        last = self.sizes[0] - 1
        self.arrived(head, 0, NEAR, 3, self.shard_rows)

        def near(order, first, rows):
            part = self.blocks(head, every, self.x, self.y, first, rows)
            to = self.device(x=1 - self.x) if order == "xy" else self.device(y=1 - self.y)
            self.copy(head, 1, NEAR, plane_rows, part, to).start()

        self.routes(plane_rows, near)
        plane = self.blocks(head, self.z, every, every, 0, plane_rows)
        up = jnp.where(self.z == last, 1, self.z + 1)
        down = jnp.where(self.z == 0, last - 1, self.z - 1)
        self.copy(head, 1, PLANE, plane_rows, plane, self.device(z=up)).start()
        self.copy(head, 1, PLANE, plane_rows, plane, self.device(z=down)).start()
        self.hand_over(head, plane)

    @by_width
    def third(self, head, plane_rows):
        every = slice(None)
        last = self.sizes[0] - 1
        self.arrived(head, 1, NEAR, 4, self.shard_rows - plane_rows)

        def near(order, first, rows):
            if order == "xy":
                part = self.blocks(head, every, every, self.y, first, rows)
                to = self.device(y=1 - self.y)
            else:
                part = self.blocks(head, every, self.x, every, first, rows)
                to = self.device(x=1 - self.x)
            self.copy(head, 2, NEAR, plane_rows, part, to).start()
            self.hand_over(head, part)

        self.routes(plane_rows, near)

        @pl.when(self.is_end)
        def _():
            self.arrived(head, 1, PLANE, 4, plane_rows)

        @pl.when(jnp.logical_not(self.is_end))
        def _():
            self.arrived(head, 1, PLANE, 12, plane_rows)
            half = (last + 1) // 2
            start = jnp.where(self.z >= half, 0, half)
            part = self.blocks(head, pl.ds(start, half), every, every, 0, plane_rows)
            self.copy(head, 2, PLANE, plane_rows, part, self.device(z=jnp.where(self.z >= half, last, 0))).start()

    @by_width
    def fourth(self, head, plane_rows):
        every = slice(None)
        z_size = self.sizes[0]

        @pl.when(self.is_end)
        def _():
            self.arrived(head, 2, NEAR, 8, self.shard_rows)

        @pl.when(jnp.logical_not(self.is_end))
        def _():
            self.arrived(head, 2, NEAR, 8, self.shard_rows - plane_rows)

        def near(order, first, rows):
            if order == "xy":
                part = self.blocks(head, every, every, 1 - self.y, first, rows)
            else:
                part = self.blocks(head, every, 1 - self.x, every, first, rows)
            self.hand_over(head, part)

        self.routes(plane_rows, near)

        for d in range(1, z_size):
            self.hand_over(head, self.blocks(head, lax.rem(self.z + d, z_size), every, every, 0, plane_rows))

    def handed(self, head, core):
        part = self.w_buf.at[head, slice(None), slice(None), core]
        return pltpu.make_async_remote_copy(
            src_ref=part,
            dst_ref=part,
            send_sem=self.core_send.at[0],
            recv_sem=self.core_recv.at[0 if isinstance(head, slice) else head],
            device_id=self.device(core=1 - self.core),
            device_id_type=MESH_ID,
        )

    @scoped
    def ready(self, head):
        self.handed(head, 1 - self.core).wait_recv()

    @scoped
    def settled(self):
        for plane_rows in (PLANE_ROWS, WIDE_PLANE_ROWS):
            near_rows = self.shard_rows - plane_rows
            self.left(0, NEAR, plane_rows, 3, near_rows)
            self.left(0, PLANE, plane_rows, 3, plane_rows)
            self.left(1, NEAR, plane_rows, 4, near_rows)
            self.left(1, PLANE, plane_rows, 8, plane_rows)
            self.left(2, NEAR, plane_rows, 8, near_rows)

            @pl.when(jnp.logical_not(self.is_end))
            def _():
                self.left(2, PLANE, plane_rows, 8, plane_rows)

        self.handed(slice(None), self.core).wait_send()


def prefill_kernel(
    sizes,
    length_hbm,
    tokens_hbm,
    attn_hbm,
    norm_gain_hbm,
    attn_gain_hbm,
    w_hbm,
    conv_hbm,
    wa_hbm,
    wi_hbm,
    decay_hbm,
    wkv_hbm,
    own_ref,
    theirs_ref,
    cache_ref,
    w_buf,
    tokens_v,
    attn_v,
    wkv_v,
    wa_v,
    wi_v,
    halo_v,
    rows_v,
    normed_v,
    kv_v,
    xp_v,
    xc_v,
    ga_v,
    gi_v,
    summary_v,
    turn_v,
    norm_gain_ref,
    attn_gain_ref,
    decay_ref,
    conv_ref,
    length_ref,
    send_sem,
    recv_sem,
    core_send,
    core_recv,
    load_sem,
    side_send,
    side_recv,
):
    heads = w_buf.shape[0]
    local_len = tokens_v.shape[0]
    seq_parts = sizes[3]
    ex = Exchange(sizes, heads, w_buf, send_sem, recv_sem, core_send, core_recv)
    y = ex.y
    start = y * local_len
    beside = ex.device(y=1 - y)

    shard = [
        pltpu.make_async_copy(
            w_hbm.at[:, pl.ds(h * HD, HD)], w_buf.at[h, ex.z, ex.x, ex.core, y], load_sem.at[12]
        )
        for h in range(heads)
    ]
    loads = [
        pltpu.make_async_copy(source, target, load_sem.at[i])
        for i, (source, target) in enumerate(
            (
                (tokens_hbm, tokens_v),
                (attn_hbm, attn_v),
                (wkv_hbm, wkv_v),
                (wa_hbm, wa_v),
                (wi_hbm, wi_v),
                (norm_gain_hbm, norm_gain_ref.at[0]),
                (attn_gain_hbm, attn_gain_ref.at[0]),
                (decay_hbm, decay_ref.at[0]),
                (conv_hbm, conv_ref),
                (length_hbm, length_ref),
            )
        )
    ]
    for copy in shard + [loads[1], loads[2], loads[6], loads[9], loads[0], *loads[3:6], loads[7], loads[8]]:
        copy.start()

    barrier = pltpu.get_barrier_semaphore()
    peers = ex.peers()
    for peer in peers:
        pl.semaphore_signal(barrier, inc=1, device_id=peer, device_id_type=MESH_ID)

    own_shard = w_buf.at[:, ex.z, ex.x, ex.core, y]
    pltpu.make_async_copy(own_shard, own_shard, load_sem.at[12]).wait()
    pl.semaphore_wait(barrier, len(peers))
    ex.first_near(0)
    for h in range(heads):
        ex.first_plane(h)
    ex.first_near(1)
    ex.first_near(2)

    quarter = HD // 4
    lane = lax.broadcasted_iota(jnp.int32, (1, 2 * quarter), 1)
    spacing = jnp.exp(
        (-jnp.log(10000.0) / quarter) * lax.rem(lane, quarter).astype(jnp.float32)
    )
    half_len = local_len // 2
    fine = lax.broadcasted_iota(jnp.int32, (half_len, 2 * quarter), 0).astype(jnp.float32) * spacing
    turn_v[0] = jnp.cos(fine)
    turn_v[1] = jnp.sin(fine)

    loads[6].wait()
    loads[9].wait()
    length = length_ref[0]

    def kv_half(k):
        rows = slice(k * half_len, (k + 1) * half_len)
        normed = rms_norm(attn_v[rows], attn_gain_ref[...])
        full = jnp.dot(normed, wkv_v[...], preferred_element_type=jnp.float32)
        place = start + k * half_len
        coarse = place.astype(jnp.float32) * spacing
        cos_c, sin_c = jnp.cos(coarse), jnp.sin(coarse)
        cosine = cos_c * turn_v[0] - sin_c * turn_v[1]
        sine = sin_c * turn_v[0] + cos_c * turn_v[1]
        sine = jnp.where(lane < quarter, -sine, sine)
        at = place + lax.broadcasted_iota(jnp.int32, (half_len, 1), 0)
        window = (at >= length - W) & (at < length)
        turned = full[:, : 2 * quarter]
        other = pltpu.roll(turned, quarter, axis=1)
        turned = turned * cosine + other * sine

        def put(half, columns, values):
            kv_v[half, rows, columns] = jnp.where(window, values, 0.0).astype(jnp.bfloat16)

        put(0, slice(0, 2 * quarter), turned)
        put(0, slice(2 * quarter, HD), full[:, 2 * quarter : HD])
        put(1, slice(0, HD), full[:, HD:])

    halo_copy = pltpu.make_async_remote_copy(
        src_ref=tokens_v.at[pl.ds(local_len - HALO, HALO)],
        dst_ref=halo_v,
        send_sem=side_send.at[0],
        recv_sem=side_recv.at[0],
        device_id=beside,
        device_id_type=MESH_ID,
    )
    kv_copies = [
        pltpu.make_async_remote_copy(
            src_ref=kv_v.at[1 - y, pl.ds(k * half_len, half_len)],
            dst_ref=cache_ref.at[pl.ds(start + k * half_len, half_len)],
            send_sem=side_send.at[1 + k],
            recv_sem=side_recv.at[1 + k],
            device_id=beside,
            device_id_type=MESH_ID,
        )
        for k in range(2)
    ]
    kept = pltpu.make_async_copy(kv_v.at[y], cache_ref.at[pl.ds(start, local_len)], load_sem.at[10])
    loads[1].wait()
    loads[2].wait()
    with jax.named_scope("kv"):
        kv_half(0)
    loads[0].wait()
    loads[5].wait()

    @pl.when(y == 0)
    def _():
        halo_copy.start()
        halo_v[...] = jnp.zeros_like(halo_v)

    ex.second(0)
    kv_copies[0].start()
    with jax.named_scope("kv"):
        kv_half(1)
    ex.second(1)
    ex.third(0)
    ex.first_near(3)
    kv_copies[1].start()
    kept.start()

    norm_step = 64

    def norm_rows(i, carry):
        rows = pl.ds(pl.multiple_of(i * norm_step, norm_step), norm_step)
        rows_v[rows] = rms_norm(tokens_v[rows], norm_gain_ref[...])
        return carry

    with jax.named_scope("norm"):
        lax.fori_loop(0, local_len // norm_step, norm_rows, 0)
    ex.second(2)
    ex.third(1)
    ex.first_near(4)

    @pl.when(y != 0)
    def _():
        halo_copy.wait_recv()

    steps = local_len // LANES_OF_TIME
    rows_ext = normed_v.shape[0]
    row = lax.broadcasted_iota(jnp.int32, (rows_ext, local_len), 0)
    col = lax.broadcasted_iota(jnp.int32, (rows_ext, local_len), 1)
    at = lax.rem(row, LANES_OF_TIME) * steps + lax.div(row, LANES_OF_TIME) - (TAPS - 1)
    pick = (at == col).astype(jnp.bfloat16)

    def reorder(i, carry):
        columns = pl.ds(pl.multiple_of(i * HD, HD), HD)
        normed_v[:, columns] = jnp.dot(
            pick, rows_v[:, columns], preferred_element_type=jnp.float32
        ).astype(jnp.bfloat16)
        return carry

    lax.fori_loop(0, heads, reorder, 0)
    edge = 2 * HALO
    row = lax.broadcasted_iota(jnp.int32, (edge, HALO), 0)
    col = lax.broadcasted_iota(jnp.int32, (edge, HALO), 1)
    at = lax.div(row, LANES_OF_TIME) - (TAPS - 1)
    early = ((lax.rem(row, LANES_OF_TIME) == 0) & (at < 0) & (at + HALO == col)).astype(jnp.bfloat16)
    halo_rows = rms_norm(halo_v[...], norm_gain_ref[...])
    before = jnp.dot(early, halo_rows, preferred_element_type=jnp.float32)
    normed_v[0:edge] = (normed_v[0:edge].astype(jnp.float32) + before).astype(jnp.bfloat16)
    ex.second(3)
    ex.fourth(0)
    for copy in (loads[3], loads[4], loads[7], loads[8]):
        copy.wait()

    per_owner = heads // seq_parts

    def summary_copy(head, slot):
        return pltpu.make_async_remote_copy(
            src_ref=summary_v.at[head],
            dst_ref=theirs_ref.at[slot],
            send_sem=side_send.at[3],
            recv_sem=side_recv.at[3],
            device_id=beside,
            device_id_type=MESH_ID,
        )

    inner = lax.broadcasted_iota(jnp.int32, (STEP_ROWS, HD), 0)
    first_at = start + lax.rem(inner, LANES_OF_TIME) * steps + lax.div(inner, LANES_OF_TIME)

    def head_step(head, carry):
        ex.ready(head)

        for lag, stage in ((5, ex.first_near), (4, ex.second), (2, ex.third)):

            @pl.when(head + lag < heads)
            def _():
                stage(head + lag)

        columns = pl.ds(pl.multiple_of(head * HD, HD), HD)
        w_block = w_buf[head].reshape(normed_v.shape[1], HD)
        projected = jnp.dot(
            normed_v[...], w_block, preferred_element_type=jnp.float32
        ).astype(jnp.bfloat16)
        xp_v[...] = projected.astype(jnp.float32)
        row = lax.broadcasted_iota(jnp.int32, (HALO, rows_ext), 1)
        wanted = length - (TAPS - 1) + lax.broadcasted_iota(jnp.int32, (HALO, rows_ext), 0) - 2
        step = lax.div(row, LANES_OF_TIME) - (TAPS - 1)
        at = start + lax.rem(row, LANES_OF_TIME) * steps + step
        real = (step >= 0) & (step < steps) & (wanted < length) & (wanted >= length - (TAPS - 1))
        picker = (real & (at == wanted)).astype(jnp.bfloat16)
        picked = jnp.dot(picker, projected, preferred_element_type=jnp.float32)
        conv_w = conv_ref[:, columns]
        conv_sum = conv_w[0:1] * xp_v[0:local_len]
        for offset in range(1, TAPS):
            shift = offset * LANES_OF_TIME
            conv_sum = conv_sum + conv_w[offset : offset + 1] * xp_v[shift : shift + local_len]
        x_conv = conv_sum.astype(jnp.bfloat16)
        xc_v[...] = x_conv.astype(jnp.float32)
        ga_v[...] = jnp.dot(x_conv, wa_v[head], preferred_element_type=jnp.float32)
        gi_v[...] = jnp.dot(x_conv, wi_v[head], preferred_element_type=jnp.float32)

        @pl.when(head + 1 < heads)
        def _():
            ex.fourth(head + 1)

        rate = -8.0 * jax.nn.softplus(-decay_ref[:, columns])

        def block(i, carry):
            state, rate_sum = carry
            rows = pl.ds(pl.multiple_of(i * STEP_ROWS, STEP_ROWS), STEP_ROWS)
            valid = first_at + i * (STEP_ROWS // LANES_OF_TIME) < length
            log_rate = rate * jax.nn.sigmoid(ga_v[rows])
            fall = -2.0 * log_rate
            lost = 1.0 - fall * (1.0 / 6.0)
            for order in (5.0, 4.0, 3.0, 2.0):
                lost = 1.0 - fall * (1.0 / order) * lost
            lost = fall * lost
            root = lost * lax.rsqrt(jnp.maximum(lost, 1e-37))
            push = jnp.where(valid, root * jax.nn.sigmoid(gi_v[rows]) * xc_v[rows], 0.0)
            held = jnp.where(valid, log_rate, 0.0)
            keep = jnp.exp(held)
            for k in range(STEP_ROWS // LANES_OF_TIME):
                tile = slice(k * LANES_OF_TIME, (k + 1) * LANES_OF_TIME)
                state = keep[tile] * state + push[tile]
                rate_sum = rate_sum + held[tile]
            return state, rate_sum

        zeros = jnp.zeros((LANES_OF_TIME, HD), jnp.float32)
        state, rate_sum = lax.fori_loop(0, local_len // STEP_ROWS, block, (zeros, zeros))
        keep_all = jnp.exp(rate_sum)
        total = state[0:1]
        for s in range(1, LANES_OF_TIME):
            total = keep_all[s : s + 1] * total + state[s : s + 1]
        keep_total = jnp.exp(jnp.sum(rate_sum, axis=0, keepdims=True))
        place = lax.broadcasted_iota(jnp.int32, (LANES_OF_TIME, HD), 0)
        summary_v[head] = jnp.where(
            place == 0, keep_total, jnp.where(place == 1, total, picked[0:LANES_OF_TIME])
        )

        @pl.when(lax.div(head, per_owner) != y)
        def _():
            summary_copy(head, lax.rem(head, per_owner)).start()

        return carry

    lax.fori_loop(0, heads, head_step, 0)

    own = pltpu.make_async_copy(
        summary_v.at[pl.ds(y * per_owner, per_owner)], own_ref, load_sem.at[11]
    )
    own.start()
    every = summary_v.at[pl.ds(0, per_owner)]
    exchanged = pltpu.make_async_remote_copy(
        src_ref=every,
        dst_ref=theirs_ref,
        send_sem=side_send.at[3],
        recv_sem=side_recv.at[3],
        device_id=beside,
        device_id_type=MESH_ID,
    )
    for copy in kv_copies:
        copy.wait()
    kept.wait()

    @pl.when(y == 0)
    def _():
        halo_copy.wait_send()

    ex.settled()
    with jax.named_scope("exchanged"):
        own.wait()
        exchanged.wait()


def finish_kernel(
    own_hbm,
    theirs_hbm,
    kv_hbm,
    state_hbm,
    conv_hbm,
    cache_hbm,
    zeros_v,
    kv_v,
    own_v,
    theirs_v,
    state_v,
    conv_v,
    in_sem,
    out_sem,
):
    rest = kv_v.shape[0]
    load_own = pltpu.make_async_copy(own_hbm, own_v, in_sem.at[0])
    load_theirs = pltpu.make_async_copy(theirs_hbm, theirs_v, in_sem.at[1])
    load_kv = pltpu.make_async_copy(kv_hbm, kv_v, in_sem.at[2])
    for copy in (load_own, load_theirs, load_kv):
        copy.start()
    zeros_v[...] = jnp.zeros_like(zeros_v)
    store = [
        pltpu.make_async_copy(zeros_v, cache_hbm.at[pl.ds(rest, zeros_v.shape[0])], out_sem.at[0]),
        pltpu.make_async_copy(kv_v, cache_hbm.at[pl.ds(0, rest)], out_sem.at[1]),
        pltpu.make_async_copy(state_v, state_hbm, out_sem.at[2]),
        pltpu.make_async_copy(conv_v, conv_hbm, out_sem.at[3]),
    ]
    store[0].start()
    load_own.wait()
    load_theirs.wait()
    first_half = lax.axis_index("seq") == 0
    for k in range(own_v.shape[0]):
        own, got = own_v[k], theirs_v[k]
        head_part = jnp.where(first_half, own, got)
        tail_part = jnp.where(first_half, got, own)
        columns = slice(k * HD, (k + 1) * HD)
        state_v[:, columns] = tail_part[0:1] * head_part[1:2] + tail_part[1:2]
        picked = head_part[2 : 1 + TAPS] + tail_part[2 : 1 + TAPS]
        conv_v[0, :, columns] = picked.astype(jnp.bfloat16)
    store[2].start()
    store[3].start()
    load_kv.wait()
    store[1].start()
    for copy in store:
        copy.wait()


def gathered_on_device(
    sizes, tokens, attn_in, lengths, norm_gain, attn_gain, w_x, conv_w, w_a, w_i, lru_decay, w_kv
):
    local_len, width = tokens.shape[1:]
    z_size, x_size, cores, seq_parts = sizes
    heads = width // HD
    rows_ext = -(-(local_len + (TAPS - 1) * LANES_OF_TIME) // HALO) * HALO
    anywhere = pl.BlockSpec(memory_space=pl.ANY)
    owned = width // seq_parts
    per_owner = heads // seq_parts
    half = w_kv.shape[1] // seq_parts
    own, theirs, kv = pl.pallas_call(
        functools.partial(prefill_kernel, sizes),
        in_specs=[anywhere] * 11,
        out_specs=(anywhere, anywhere, anywhere),
        out_shape=(
            jax.ShapeDtypeStruct((per_owner, LANES_OF_TIME, HD), jnp.float32),
            jax.ShapeDtypeStruct((per_owner, LANES_OF_TIME, HD), jnp.float32),
            jax.ShapeDtypeStruct((seq_parts * local_len, half), jnp.bfloat16),
        ),
        scratch_shapes=[
            pltpu.VMEM((heads, z_size, x_size, cores, seq_parts, w_x.shape[0], HD), jnp.bfloat16),
            pltpu.VMEM((local_len, width), jnp.bfloat16),
            pltpu.VMEM((local_len, width), jnp.bfloat16),
            pltpu.VMEM(w_kv.shape, jnp.bfloat16),
            pltpu.VMEM(w_a.shape, jnp.bfloat16),
            pltpu.VMEM(w_i.shape, jnp.bfloat16),
            pltpu.VMEM((HALO, width), jnp.bfloat16),
            pltpu.VMEM((local_len, width), jnp.bfloat16),
            pltpu.VMEM((rows_ext, width), jnp.bfloat16),
            pltpu.VMEM((2, local_len, half), jnp.bfloat16),
            pltpu.VMEM((rows_ext, HD), jnp.float32),
            pltpu.VMEM((local_len, HD), jnp.float32),
            pltpu.VMEM((local_len, HD), jnp.float32),
            pltpu.VMEM((local_len, HD), jnp.float32),
            pltpu.VMEM((heads, LANES_OF_TIME, HD), jnp.float32),
            pltpu.VMEM((2, local_len // 2, HD // 2), jnp.float32),
            pltpu.VMEM((1, width), jnp.float32),
            pltpu.VMEM((1, width), jnp.float32),
            pltpu.VMEM((1, width), jnp.float32),
            pltpu.VMEM(conv_w.shape, jnp.float32),
            pltpu.SMEM((1,), jnp.int32),
            pltpu.SemaphoreType.DMA((3, 2, 2)),
            pltpu.SemaphoreType.DMA((heads, 4)),
            pltpu.SemaphoreType.DMA((1,)),
            pltpu.SemaphoreType.DMA((heads,)),
            pltpu.SemaphoreType.DMA((13,)),
            pltpu.SemaphoreType.DMA((4,)),
            pltpu.SemaphoreType.DMA((4,)),
        ],
        compiler_params=pltpu.CompilerParams(
            collective_id=0, has_side_effects=True, vmem_limit_bytes=60 * 1024 * 1024
        ),
    )(
        lengths,
        tokens[0],
        attn_in[0],
        norm_gain,
        attn_gain,
        w_x,
        conv_w,
        w_a,
        w_i,
        lru_decay,
        w_kv,
    )
    state_shape, conv_shape = (1, owned), (1, TAPS - 1, owned)
    state, conv_state, cache = pl.pallas_call(
        finish_kernel,
        in_specs=[anywhere] * 3,
        out_specs=(anywhere, anywhere, anywhere),
        out_shape=(
            jax.ShapeDtypeStruct(state_shape, jnp.float32),
            jax.ShapeDtypeStruct(conv_shape, jnp.bfloat16),
            jax.ShapeDtypeStruct((W, half), jnp.bfloat16),
        ),
        scratch_shapes=[
            pltpu.VMEM((W - kv.shape[0], half), jnp.bfloat16),
            pltpu.VMEM(kv.shape, jnp.bfloat16),
            pltpu.VMEM(own.shape, jnp.float32),
            pltpu.VMEM(own.shape, jnp.float32),
            pltpu.VMEM(state_shape, jnp.float32),
            pltpu.VMEM(conv_shape, jnp.bfloat16),
            pltpu.SemaphoreType.DMA((3,)),
            pltpu.SemaphoreType.DMA((4,)),
        ],
    )(own, theirs, kv)
    return state, conv_state, cache[None]


def fits(mesh, sizes, tokens, w_x, w_kv):
    if sizes is None:
        return False
    _, length, width = tokens.shape
    devices = mesh.size
    seq_parts = mesh.shape["seq"]
    return (
        length < W
        and width % (HD * seq_parts) == 0
        and w_x.shape[0] % (devices * HALO) == 0
        and w_x.shape[0] // devices > WIDE_PLANE_ROWS
        and w_kv.shape[1] == seq_parts * HD
        and tokens.shape[0] == mesh.shape["batch"]
    )


def solution(mesh):
    in_specs = (
        P("batch", "seq", None),
        P("batch", "seq", None),
        P("batch"),
        P(),
        P(),
        P(("batch", "seq"), None),
        P(),
        P(),
        P(),
        P(),
        P(),
    )
    out_specs = (P("batch", "seq"), P("batch", None, "seq"), P("batch", None, "seq"))
    sizes = physical_grid(mesh)

    def run(*arrays):
        tokens, w_x, w_kv = arrays[0], arrays[5], arrays[10]
        body = on_device
        if fits(mesh, sizes, tokens, w_x, w_kv):
            body = functools.partial(gathered_on_device, sizes)
        return jax.shard_map(
            body, mesh=mesh, in_specs=in_specs, out_specs=out_specs, check_vma=False
        )(*arrays)

    return run
```

```python
import functools

import jax
import jax.numpy as jnp
from jax import lax
from jax.experimental import pallas as pl
from jax.experimental.pallas import tpu as pltpu
from jax.sharding import PartitionSpec as P

H = 10
HD = 256
W = 2048
LANES_OF_TIME = 8
TAPS = 4
HALO = 16
STEP_ROWS = 32


def passed_along(block, axis, distance):
    devices = range(lax.axis_size(axis))
    route = [(i - distance, i) for i in devices if i - distance in devices]
    return lax.ppermute(block, axis, route)


def rms_norm(values, gain_vec):
    widened = values.astype(jnp.float32)
    inverse = lax.rsqrt(jnp.mean(widened * widened, axis=-1, keepdims=True) + 1e-06)
    return (widened * inverse * gain_vec).astype(jnp.bfloat16)


def rotate_keys(key_rows, positions):
    quarter = key_rows.shape[-1] // 4
    spacing = jnp.exp(-jnp.log(10000.0) * jnp.arange(quarter, dtype=jnp.float32) / quarter)
    angles = positions.astype(jnp.float32)[:, None] * spacing[None, :]
    cosine_rows = jnp.cos(angles)
    sine_rows = jnp.sin(angles)
    first_part = key_rows[:, :quarter]
    second_part = key_rows[:, quarter : 2 * quarter]
    return jnp.concatenate(
        [
            first_part * cosine_rows - second_part * sine_rows,
            second_part * cosine_rows + first_part * sine_rows,
            key_rows[:, 2 * quarter :],
        ],
        axis=1,
    )


def ordered_rows(tokens_ref, halo_ref, gain_ref, normed_ref):
    local_len = tokens_ref.shape[0]
    steps = local_len // LANES_OF_TIME
    row = lax.broadcasted_iota(jnp.int32, (normed_ref.shape[0], local_len + HALO), 0)
    col = lax.broadcasted_iota(jnp.int32, (normed_ref.shape[0], local_len + HALO), 1)
    at = lax.rem(row, LANES_OF_TIME) * steps + lax.div(row, LANES_OF_TIME) - (TAPS - 1)
    pick = (jnp.where(at < 0, at + local_len + HALO, at) == col).astype(jnp.bfloat16)
    rows = jnp.concatenate(
        [rms_norm(tokens_ref[...], gain_ref[...]), rms_norm(halo_ref[...], gain_ref[...])], axis=0
    )
    normed_ref[...] = jnp.dot(pick, rows, preferred_element_type=jnp.float32).astype(jnp.bfloat16)


def one_head(
    normed_ref, w_block, conv_w, w_a, w_i, rate, length, start, out_ref, xp_ref, xc_ref, ga_ref, gi_ref
):
    rows_ext = normed_ref.shape[0]
    local_len = xc_ref.shape[0]
    steps = local_len // LANES_OF_TIME
    projected = jnp.dot(normed_ref[...], w_block, preferred_element_type=jnp.float32).astype(
        jnp.bfloat16
    )
    xp_ref[...] = projected.astype(jnp.float32)
    row = lax.broadcasted_iota(jnp.int32, (HALO, rows_ext), 1)
    wanted = length - (TAPS - 1) + lax.broadcasted_iota(jnp.int32, (HALO, rows_ext), 0) - 2
    step = lax.div(row, LANES_OF_TIME) - (TAPS - 1)
    at = start + lax.rem(row, LANES_OF_TIME) * steps + step
    real = (step >= 0) & (step < steps) & (wanted < length) & (wanted >= length - (TAPS - 1))
    picker = (real & (at == wanted)).astype(jnp.bfloat16)
    picked = jnp.dot(picker, projected, preferred_element_type=jnp.float32)
    conv_sum = conv_w[0:1] * xp_ref[0:local_len]
    for offset in range(1, TAPS):
        shift = offset * LANES_OF_TIME
        conv_sum = conv_sum + conv_w[offset : offset + 1] * xp_ref[shift : shift + local_len]
    x_conv = conv_sum.astype(jnp.bfloat16)
    xc_ref[...] = x_conv.astype(jnp.float32)
    ga_ref[...] = jnp.dot(x_conv, w_a, preferred_element_type=jnp.float32)
    gi_ref[...] = jnp.dot(x_conv, w_i, preferred_element_type=jnp.float32)
    inner = lax.broadcasted_iota(jnp.int32, (STEP_ROWS, HD), 0)
    first_at = start + lax.rem(inner, LANES_OF_TIME) * steps + lax.div(inner, LANES_OF_TIME)

    def block(i, carry):
        state, rate_sum = carry
        rows = pl.ds(pl.multiple_of(i * STEP_ROWS, STEP_ROWS), STEP_ROWS)
        valid = first_at + i * (STEP_ROWS // LANES_OF_TIME) < length
        log_rate = rate * jax.nn.sigmoid(ga_ref[rows])
        fall = -2.0 * log_rate
        lost = 1.0 - fall * (1.0 / 6.0)
        for order in (5.0, 4.0, 3.0, 2.0):
            lost = 1.0 - fall * (1.0 / order) * lost
        lost = fall * lost
        root = lost * lax.rsqrt(jnp.maximum(lost, 1e-37))
        push = jnp.where(valid, root * jax.nn.sigmoid(gi_ref[rows]) * xc_ref[rows], 0.0)
        held = jnp.where(valid, log_rate, 0.0)
        keep = jnp.exp(held)
        for k in range(STEP_ROWS // LANES_OF_TIME):
            tile = slice(k * LANES_OF_TIME, (k + 1) * LANES_OF_TIME)
            state = keep[tile] * state + push[tile]
            rate_sum = rate_sum + held[tile]
        return state, rate_sum

    zeros = jnp.zeros((LANES_OF_TIME, HD), jnp.float32)
    state, rate_sum = lax.fori_loop(0, local_len // STEP_ROWS, block, (zeros, zeros))
    keep_all = jnp.exp(rate_sum)
    total = state[0:1]
    for s in range(1, LANES_OF_TIME):
        total = keep_all[s : s + 1] * total + state[s : s + 1]
    keep_total = jnp.exp(jnp.sum(rate_sum, axis=0, keepdims=True))
    place = lax.broadcasted_iota(jnp.int32, (LANES_OF_TIME, HD), 0)
    out_ref[...] = jnp.where(
        place == 0, keep_total, jnp.where(place == 1, total, picked[0:LANES_OF_TIME])
    )


def recurrent_kernel(
    length_ref,
    tokens_ref,
    halo_ref,
    gain_ref,
    w_ref,
    conv_ref,
    wa_ref,
    wi_ref,
    rate_ref,
    out_ref,
    normed_ref,
    *work
):
    @pl.when(pl.program_id(0) == 0)
    def _():
        ordered_rows(tokens_ref, halo_ref, gain_ref, normed_ref)

    start = lax.axis_index("seq") * tokens_ref.shape[0]
    one_head(
        normed_ref,
        w_ref[...],
        conv_ref[...],
        wa_ref[0],
        wi_ref[0],
        rate_ref[...],
        length_ref[0],
        start,
        out_ref,
        *work
    )


def recurrent(first, tokens, halo, lengths, norm_gain, w_part, conv_w, w_a, w_i, rate):
    local_len, width = tokens.shape
    part_width = w_part.shape[1]
    rows_ext = -(-(local_len + (TAPS - 1) * LANES_OF_TIME) // HALO) * HALO
    whole = lambda *shape: pl.BlockSpec(shape, lambda h: (0,) * len(shape))
    return pl.pallas_call(
        recurrent_kernel,
        grid=(part_width // HD,),
        in_specs=[
            pl.BlockSpec(memory_space=pltpu.SMEM),
            whole(local_len, width),
            whole(HALO, width),
            whole(1, width),
            pl.BlockSpec((width, HD), lambda h: (0, h)),
            pl.BlockSpec((TAPS, HD), lambda h: (0, h + first)),
            pl.BlockSpec((1, HD, HD), lambda h: (h + first, 0, 0)),
            pl.BlockSpec((1, HD, HD), lambda h: (h + first, 0, 0)),
            pl.BlockSpec((1, HD), lambda h: (0, h + first)),
        ],
        out_specs=pl.BlockSpec((LANES_OF_TIME, HD), lambda h: (0, h)),
        out_shape=jax.ShapeDtypeStruct((LANES_OF_TIME, part_width), jnp.float32),
        scratch_shapes=[
            pltpu.VMEM((rows_ext, width), jnp.bfloat16),
            pltpu.VMEM((rows_ext, HD), jnp.float32),
            pltpu.VMEM((local_len, HD), jnp.float32),
            pltpu.VMEM((local_len, HD), jnp.float32),
            pltpu.VMEM((local_len, HD), jnp.float32),
        ],
        compiler_params=pltpu.CompilerParams(vmem_limit_bytes=60 * 1024 * 1024),
        cost_estimate=pl.CostEstimate(
            flops=2 * local_len * part_width * (width + 2 * HD),
            bytes_accessed=2 * width * (local_len + part_width),
            transcendentals=6 * local_len * part_width,
        ),
    )(lengths, tokens, halo, norm_gain[None], w_part, conv_w, w_a, w_i, rate[None])


def on_device(
    tokens, attn_in, lengths, norm_gain, attn_gain, w_x, conv_w, w_a, w_i, lru_decay, w_kv
):
    local_len = tokens.shape[1]
    feature_dim = tokens.shape[2]
    seq_parts = lax.axis_size("seq")
    seq_place = lax.axis_index("seq")
    length = lengths[0]
    halo = passed_along(tokens[0, local_len - HALO :], "seq", 1)
    heads = feature_dim // HD
    early = (4 * heads) // 5
    positions = seq_place * local_len + jnp.arange(local_len, dtype=jnp.int32)
    attn_normed = rms_norm(attn_in[0], attn_gain)
    kv_full = jnp.dot(attn_normed, w_kv, preferred_element_type=jnp.float32)
    kv_rows = jnp.concatenate(
        [rotate_keys(kv_full[:, :HD], positions), kv_full[:, HD:]], axis=1
    ).astype(jnp.bfloat16)
    in_window = ((positions >= length - W) & (positions < length))[:, None]
    masked = jnp.where(in_window, kv_rows, jnp.zeros_like(kv_rows))
    by_column = lax.all_to_all(masked, "seq", split_axis=1, concat_axis=0, tiled=True)
    laps = -(-seq_parts * local_len // W)
    by_column = jnp.pad(by_column, ((0, laps * W - seq_parts * local_len), (0, 0)))
    kv_cache = by_column[:W]
    for lap in range(1, laps):
        kv_cache = kv_cache + by_column[lap * W : (lap + 1) * W]
    w_early = lax.all_gather(w_x[:, : early * HD], ("batch", "seq"), axis=0, tiled=True)
    w_early, w_local, kv_cache, halo = lax.optimization_barrier((w_early, w_x, kv_cache, halo))
    w_late = lax.all_gather(w_local[:, early * HD :], ("batch", "seq"), axis=0, tiled=True)
    w_parts = ((0, w_early), (early, w_late))
    rate = -8.0 * jax.nn.softplus(-lru_decay)
    summary = jnp.concatenate(
        [
            recurrent(first, tokens[0], halo, lengths, norm_gain, w_part, conv_w, w_a, w_i, rate)
            for first, w_part in w_parts
        ],
        axis=1,
    )
    owned_width = feature_dim // seq_parts
    gathered = lax.all_gather(summary, "seq", axis=0, tiled=True)
    owned = lax.dynamic_slice_in_dim(gathered, seq_place * owned_width, owned_width, 1)
    state = owned[1:2]
    picked = owned[2:5]
    for part in range(1, seq_parts):
        at = part * LANES_OF_TIME
        state = owned[at : at + 1] * state + owned[at + 1 : at + 2]
        picked = picked + owned[at + 2 : at + 5]
    conv_state = picked.astype(jnp.bfloat16)
    return (state, conv_state[None], kv_cache[None])


MESH_ID = pl.DeviceIdType.MESH
SPLITS = ((6, (16, 16)), (4, (16, 0)),)
NEAR, PLANE = 0, 1
START = (
    ("plane", 0), ("near", 1), ("own", 0), ("own", 4), ("own", 1), ("plane", 1), ("near", 0), ("plane", 2),
    ("own", 3), ("kv", 0), ("halo", 0), ("send_kv", 0), ("own", 2), ("plane", 3), ("near", 2), ("kv", 1),
    ("second", 0), ("near", 3), ("norm", 0), ("second", 1), ("plane", 4), ("third_plane", 0), ("second", 2),
    ("reorder", 0), ("near", 4), ("third", 0), ("second", 3), ("send_kv", 1), ("third", 1), ("third_plane", 1),
    ("plane", 6), ("reorder", 1),
)
SLOTS = (
    (
        (
            ("plane", 5), ("plane", 7), ("fourth", 0), ("third", 2), ("third", 3), ("third_plane", 2), ("near", 5),
            ("own", 7), ("own", 5), ("second", 4), ("fourth", 1), ("ready", 0),
        ),
        (),
    ),
    (
        (
            ("own", 6), ("plane", 8), ("third_plane", 3), ("near", 6), ("second", 5), ("fourth", 2), ("ready", 1),
        ),
        (
            ("plane", 9), ("third", 4),
        ),
    ),
    (
        (
            ("near", 7), ("third_plane", 4), ("second", 6), ("third", 5), ("ready", 2), ("fourth", 3),
        ),
        (),
    ),
    (
        (
            ("own", 8), ("near", 8), ("third_plane", 5), ("third_plane", 6), ("second", 7), ("ready", 3),
            ("third", 6),
        ),
        (
            ("fourth", 4), ("own", 9),
        ),
    ),
    (
        (
            ("near", 9), ("third", 7), ("second", 8), ("ready", 4),
        ),
        (
            ("fourth", 5),
        ),
    ),
    (
        (
            ("third_plane", 7), ("fourth", 6), ("ready", 5), ("second", 9),
        ),
        (
            ("third", 8),
        ),
    ),
    (
        (
            ("fourth", 7), ("ready", 6), ("third_plane", 8),
        ),
        (
            ("third", 9),
        ),
    ),
    (
        (
            ("third_plane", 9), ("ready", 7),
        ),
        (
            ("fourth", 8),
        ),
    ),
    (
        (
            ("ready", 8), ("fourth", 9),
        ),
        (),
    ),
    (
        (
            ("ready", 9),
        ),
        (),
    ),
)


def physical_grid(mesh):
    grid = mesh.devices
    try:
        spots = [
            [(*device.coords, device.core_on_chip) for device in line] for line in grid.tolist()
        ]
    except AttributeError:
        return None
    sizes = [len({spot[k] for line in spots for spot in line}) for k in range(4)]
    low = [min(spot[k] for line in spots for spot in line) for k in range(4)]
    x_size, y_size, z_size, cores = sizes
    if (x_size, y_size, z_size, cores) != (2, 2, 4, 2) or grid.shape != (z_size * x_size * cores, y_size):
        return None
    for b, line in enumerate(spots):
        for y, spot in enumerate(line):
            want = ((b // cores) % x_size, y, b // (cores * x_size), b % cores)
            if tuple(v - l for v, l in zip(spot, low)) != want:
                return None
    return z_size, x_size, cores, y_size


def scoped(method):
    @functools.wraps(method)
    def inside(*args):
        with jax.named_scope(method.__name__):
            return method(*args)

    return inside


def by_split(method):
    @functools.wraps(method)
    def inside(exchange, head):
        with jax.named_scope(method.__name__):
            first = 0
            for index, (count, _) in enumerate(SPLITS):
                last = first + count
                if isinstance(head, int):
                    if first <= head < last:
                        method(exchange, head, index)
                elif len(SPLITS) == 1:
                    method(exchange, head, index)
                else:

                    @pl.when((head >= first) & (head < last))
                    def _():
                        method(exchange, head, index)

                first = last

    return inside


class Exchange:
    def __init__(self, sizes, heads, w_buf, send_sem, recv_sem, core_send, core_recv):
        self.sizes, self.heads = sizes, heads
        self.w_buf, self.send_sem, self.recv_sem = w_buf, send_sem, recv_sem
        self.core_send, self.core_recv = core_send, core_recv
        z_size, x_size, cores, _ = sizes
        at = lax.axis_index("batch")
        self.core = lax.rem(at, cores)
        self.x = lax.rem(lax.div(at, cores), x_size)
        self.z = lax.div(at, cores * x_size)
        self.y = lax.axis_index("seq")
        self.shard_rows = w_buf.shape[5]
        self.is_end = (self.z == 0) | (self.z == z_size - 1)

    def device(self, z=None, x=None, core=None, y=None):
        z = self.z if z is None else z
        x = self.x if x is None else x
        core = self.core if core is None else core
        y = self.y if y is None else y
        _, x_size, cores, _ = self.sizes
        return ((z * x_size + x) * cores + core, y)

    def peers(self):
        z_size = self.sizes[0]
        along = [self.device(z=lax.rem(self.z + d, z_size)) for d in range(1, z_size)]
        return along + [
            self.device(x=1 - self.x),
            self.device(y=1 - self.y),
            self.device(x=1 - self.x, y=1 - self.y),
            self.device(core=1 - self.core),
        ]

    def blocks(self, head, z, x, y, first, rows, core=None):
        core = self.core if core is None else core
        return self.w_buf.at[head, z, x, core, y, pl.ds(first, rows)]

    def copy(self, head, stage, group, split, part, to):
        return pltpu.make_async_remote_copy(
            src_ref=part,
            dst_ref=part,
            send_sem=self.send_sem.at[stage, group, split],
            recv_sem=self.recv_sem.at[head, stage if group == NEAR or stage != 1 else 3],
            device_id=to,
            device_id_type=MESH_ID,
        )

    def hand_over(self, head, part):
        pltpu.make_async_remote_copy(
            src_ref=part,
            dst_ref=part,
            send_sem=self.core_send.at[0],
            recv_sem=self.core_recv.at[head],
            device_id=self.device(core=1 - self.core),
            device_id_type=MESH_ID,
        ).start()

    def some(self, head, count, rows):
        every = slice(None)
        if count == 2:
            return self.w_buf.at[head, pl.ds(0, 2), 0, 0, 0, pl.ds(0, rows)]
        if count == 3:
            return self.w_buf.at[head, pl.ds(0, 3), 0, 0, 0, pl.ds(0, rows)]
        if count == 4:
            return self.w_buf.at[head, every, 0, 0, 0, pl.ds(0, rows)]
        if count == 8:
            return self.w_buf.at[head, every, every, 0, 0, pl.ds(0, rows)]
        return self.w_buf.at[head, pl.ds(0, 3), every, 0, every, pl.ds(0, rows)]

    def arrived(self, head, stage, group, count, rows):
        part = self.some(head, count, rows)
        self.copy(head, stage, group, 0, part, self.device(core=1 - self.core)).wait_recv()

    def left(self, stage, group, split, count, rows):
        first = sum(n for n, _ in SPLITS[:split])
        part = self.some(pl.ds(first, SPLITS[split][0]), count, rows)
        self.copy(0, stage, group, split, part, self.device(core=1 - self.core)).wait_send()

    def routes(self, split, act):
        plane_rows, turned = SPLITS[split][1]

        @pl.when(self.core == 0)
        def _():
            if turned:
                act("yx", plane_rows, turned)
            act("xy", plane_rows + turned, self.shard_rows - plane_rows - turned)

        @pl.when(self.core != 0)
        def _():
            act("yx", plane_rows, self.shard_rows - plane_rows)

    @by_split
    def near(self, head, split):
        plane_rows = SPLITS[split][1][0]
        part = self.blocks(head, self.z, self.x, self.y, plane_rows, self.shard_rows - plane_rows)
        for d in range(1, self.sizes[0]):
            to = self.device(z=lax.rem(self.z + d, self.sizes[0]))
            self.copy(head, 0, NEAR, split, part, to).start()

    def across(self, order):
        beside = self.device(x=1 - self.x), self.device(y=1 - self.y)
        return beside if order == "xy" else beside[::-1]

    @by_split
    def own(self, head, split):
        def near(order, first, rows):
            own = self.blocks(head, self.z, self.x, self.y, first, rows)
            for stage, to in enumerate(self.across(order)):
                self.copy(head, 1 + stage, NEAR, split, own, to).start()

        self.routes(split, near)

    @by_split
    def plane(self, head, split):
        plane_rows = SPLITS[split][1][0]
        plane = self.blocks(head, self.z, self.x, self.y, 0, plane_rows)
        self.copy(head, 0, PLANE, split, plane, self.device(x=1 - self.x)).start()
        self.copy(head, 0, PLANE, split, plane, self.device(y=1 - self.y)).start()
        self.copy(head, 0, PLANE, split, plane, self.device(x=1 - self.x, y=1 - self.y)).start()

    @by_split
    def second(self, head, split):
        plane_rows = SPLITS[split][1][0]
        every = slice(None)
        last = self.sizes[0] - 1
        self.arrived(head, 0, NEAR, 3, self.shard_rows)

        def near(order, first, rows):
            for stage, to in enumerate(self.across(order)):
                for d in range(1, last + 1):
                    at = lax.rem(self.z + d, last + 1)
                    part = self.blocks(head, at, self.x, self.y, first, rows)
                    self.copy(head, 1 + stage, NEAR, split, part, to).start()
            self.hand_over(head, self.blocks(head, every, self.x, self.y, first, rows))

        self.routes(split, near)
        plane = self.blocks(head, self.z, every, every, 0, plane_rows)
        up = jnp.where(self.z == last, 1, self.z + 1)
        down = jnp.where(self.z == 0, last - 1, self.z - 1)
        self.copy(head, 1, PLANE, split, plane, self.device(z=up)).start()
        self.copy(head, 1, PLANE, split, plane, self.device(z=down)).start()
        self.hand_over(head, plane)

    @by_split
    def third(self, head, split):
        plane_rows = SPLITS[split][1][0]
        every = slice(None)
        self.arrived(head, 1, NEAR, 4, self.shard_rows - plane_rows)

        def near(order, first, rows):
            if order == "xy":
                part = self.blocks(head, every, 1 - self.x, self.y, first, rows)
            else:
                part = self.blocks(head, every, self.x, 1 - self.y, first, rows)
            to = self.across(order)[1]
            self.copy(head, 2, NEAR, split, part, to).start()
            self.hand_over(head, part)

        self.routes(split, near)

    @by_split
    def third_plane(self, head, split):
        plane_rows = SPLITS[split][1][0]
        every = slice(None)
        last = self.sizes[0] - 1

        @pl.when(self.is_end)
        def _():
            self.arrived(head, 1, PLANE, 4, plane_rows)

        @pl.when(jnp.logical_not(self.is_end))
        def _():
            self.arrived(head, 1, PLANE, 12, plane_rows)
            half = (last + 1) // 2
            start = jnp.where(self.z >= half, 0, half)
            part = self.blocks(head, pl.ds(start, half), every, every, 0, plane_rows)
            self.copy(head, 2, PLANE, split, part, self.device(z=jnp.where(self.z >= half, last, 0))).start()

    @by_split
    def fourth(self, head, split):
        plane_rows = SPLITS[split][1][0]
        every = slice(None)
        z_size = self.sizes[0]

        @pl.when(self.is_end)
        def _():
            self.arrived(head, 2, NEAR, 8, self.shard_rows)

        @pl.when(jnp.logical_not(self.is_end))
        def _():
            self.arrived(head, 2, NEAR, 8, self.shard_rows - plane_rows)

        def near(order, first, rows):
            if order == "xy":
                part = self.blocks(head, every, every, 1 - self.y, first, rows)
            else:
                part = self.blocks(head, every, 1 - self.x, every, first, rows)
            self.hand_over(head, part)

        self.routes(split, near)

        for d in range(1, z_size):
            self.hand_over(head, self.blocks(head, lax.rem(self.z + d, z_size), every, every, 0, plane_rows))

    def handed(self, head, core):
        part = self.w_buf.at[head, slice(None), slice(None), core]
        return pltpu.make_async_remote_copy(
            src_ref=part,
            dst_ref=part,
            send_sem=self.core_send.at[0],
            recv_sem=self.core_recv.at[0 if isinstance(head, slice) else head],
            device_id=self.device(core=1 - self.core),
            device_id_type=MESH_ID,
        )

    @scoped
    def ready(self, head):
        self.handed(head, 1 - self.core).wait_recv()

    @scoped
    def settled(self):
        for split, (_, (plane_rows, _)) in enumerate(SPLITS):
            near_rows = self.shard_rows - plane_rows
            self.left(0, NEAR, split, 3, near_rows)
            self.left(0, PLANE, split, 3, plane_rows)
            self.left(1, NEAR, split, 4, near_rows)
            self.left(1, PLANE, split, 8, plane_rows)
            self.left(2, NEAR, split, 8, near_rows)

            @pl.when(jnp.logical_not(self.is_end))
            def _():
                self.left(2, PLANE, split, 8, plane_rows)

        self.handed(slice(None), self.core).wait_send()


def prefill_kernel(
    sizes,
    length_hbm,
    tokens_hbm,
    attn_hbm,
    norm_gain_hbm,
    attn_gain_hbm,
    w_hbm,
    conv_hbm,
    wa_hbm,
    wi_hbm,
    decay_hbm,
    wkv_hbm,
    own_ref,
    theirs_ref,
    cache_ref,
    w_buf,
    tokens_v,
    attn_v,
    wkv_v,
    wa_v,
    wi_v,
    halo_v,
    rows_v,
    normed_v,
    kv_v,
    xp_v,
    xc_v,
    ga_v,
    gi_v,
    summary_v,
    picked_v,
    turn_v,
    norm_gain_ref,
    attn_gain_ref,
    decay_ref,
    conv_ref,
    length_ref,
    send_sem,
    recv_sem,
    core_send,
    core_recv,
    load_sem,
    side_send,
    side_recv,
):
    heads = w_buf.shape[0]
    local_len = tokens_v.shape[0]
    seq_parts = sizes[3]
    ex = Exchange(sizes, heads, w_buf, send_sem, recv_sem, core_send, core_recv)
    y = ex.y
    start = y * local_len
    beside = ex.device(y=1 - y)

    shard = [
        pltpu.make_async_copy(
            w_hbm.at[:, pl.ds(h * HD, HD)], w_buf.at[h, ex.z, ex.x, ex.core, y], load_sem.at[10]
        )
        for h in range(heads)
    ]
    loads = [
        pltpu.make_async_copy(source, target, load_sem.at[i])
        for i, (source, target) in enumerate(
            (
                (tokens_hbm, tokens_v),
                (attn_hbm, attn_v),
                (wkv_hbm, wkv_v),
                (wa_hbm, wa_v),
                (wi_hbm, wi_v),
                (norm_gain_hbm, norm_gain_ref.at[0]),
                (attn_gain_hbm, attn_gain_ref.at[0]),
                (decay_hbm, decay_ref.at[0]),
                (conv_hbm, conv_ref),
                (length_hbm, length_ref),
            )
        )
    ]
    for copy in shard:
        copy.start()

    barrier = pltpu.get_barrier_semaphore()
    peers = ex.peers()
    for peer in peers:
        pl.semaphore_signal(barrier, inc=1, device_id=peer, device_id_type=MESH_ID)

    own_shard = w_buf.at[:, ex.z, ex.x, ex.core, y]
    pltpu.make_async_copy(own_shard, own_shard, load_sem.at[10]).wait()
    for copy in [loads[1], loads[2], loads[6], loads[9], loads[0], *loads[3:6], loads[7], loads[8]]:
        copy.start()
    pl.semaphore_wait(barrier, len(peers))
    lead = START.index(("kv", 0))
    for name, head in START[:lead]:
        getattr(ex, name)(head)

    quarter = HD // 4
    lane = lax.broadcasted_iota(jnp.int32, (1, 2 * quarter), 1)
    spacing = jnp.exp(
        (-jnp.log(10000.0) / quarter) * lax.rem(lane, quarter).astype(jnp.float32)
    )
    half_len = local_len // 2
    fine = lax.broadcasted_iota(jnp.int32, (half_len, 2 * quarter), 0).astype(jnp.float32) * spacing
    turn_v[0] = jnp.cos(fine)
    turn_v[1] = jnp.sin(fine)

    loads[6].wait()
    loads[9].wait()
    length = length_ref[0]

    def kv_half(k):
        rows = slice(k * half_len, (k + 1) * half_len)
        normed = rms_norm(attn_v[rows], attn_gain_ref[...])
        full = jnp.dot(normed, wkv_v[...], preferred_element_type=jnp.float32)
        place = start + k * half_len
        coarse = place.astype(jnp.float32) * spacing
        cos_c, sin_c = jnp.cos(coarse), jnp.sin(coarse)
        cosine = cos_c * turn_v[0] - sin_c * turn_v[1]
        sine = sin_c * turn_v[0] + cos_c * turn_v[1]
        sine = jnp.where(lane < quarter, -sine, sine)
        at = place + lax.broadcasted_iota(jnp.int32, (half_len, 1), 0)
        window = (at >= length - W) & (at < length)
        turned = full[:, : 2 * quarter]
        other = pltpu.roll(turned, quarter, axis=1)
        turned = turned * cosine + other * sine

        keys = jnp.concatenate([turned, full[:, 2 * quarter : HD]], axis=1)
        first, second = (jnp.where(window, v, 0.0).astype(jnp.bfloat16) for v in (keys, full[:, HD:]))
        cache_ref[pl.ds(place, half_len)] = jnp.where(y == 0, first, second)
        kv_v[rows] = jnp.where(y == 0, second, first)

    halo_copy = pltpu.make_async_remote_copy(
        src_ref=tokens_v.at[pl.ds(local_len - HALO, HALO)],
        dst_ref=halo_v,
        send_sem=side_send.at[0],
        recv_sem=side_recv.at[0],
        device_id=beside,
        device_id_type=MESH_ID,
    )
    kv_copies = [
        pltpu.make_async_remote_copy(
            src_ref=kv_v.at[pl.ds(k * half_len, half_len)],
            dst_ref=cache_ref.at[pl.ds(start + k * half_len, half_len)],
            send_sem=side_send.at[1 + k],
            recv_sem=side_recv.at[1 + k],
            device_id=beside,
            device_id_type=MESH_ID,
        )
        for k in range(2)
    ]

    def take_kv(k):
        if k == 0:
            loads[1].wait()
            loads[2].wait()
        kv_half(k)

    def send_kv(k):
        kv_copies[k].start()

    def send_halo(_):
        loads[0].wait()

        @pl.when(y == 0)
        def _():
            halo_copy.start()
            halo_v[...] = jnp.zeros_like(halo_v)

    norm_step = 64

    def norm_rows(i, carry):
        rows = pl.ds(pl.multiple_of(i * norm_step, norm_step), norm_step)
        rows_v[rows] = rms_norm(tokens_v[rows], norm_gain_ref[...])
        return carry

    def norm(_):
        loads[5].wait()
        lax.fori_loop(0, local_len // norm_step, norm_rows, 0)

    steps = local_len // LANES_OF_TIME
    rows_ext = normed_v.shape[0]
    row = lax.broadcasted_iota(jnp.int32, (rows_ext, local_len), 0)
    col = lax.broadcasted_iota(jnp.int32, (rows_ext, local_len), 1)
    at = lax.rem(row, LANES_OF_TIME) * steps + lax.div(row, LANES_OF_TIME) - (TAPS - 1)
    pick = (at == col).astype(jnp.bfloat16)

    def reorder(i, carry):
        columns = pl.ds(pl.multiple_of(i * HD, HD), HD)
        normed_v[:, columns] = jnp.dot(
            pick, rows_v[:, columns], preferred_element_type=jnp.float32
        ).astype(jnp.bfloat16)
        return carry

    def reorder_half(k):
        half_heads = heads // 2
        lax.fori_loop(*((0, half_heads) if k == 0 else (half_heads, heads)), reorder, 0)
        if k == 0:
            return

        @pl.when(y != 0)
        def _():
            halo_copy.wait_recv()

        edge = 2 * HALO
        row = lax.broadcasted_iota(jnp.int32, (edge, HALO), 0)
        col = lax.broadcasted_iota(jnp.int32, (edge, HALO), 1)
        at = lax.div(row, LANES_OF_TIME) - (TAPS - 1)
        early = (lax.rem(row, LANES_OF_TIME) == 0) & (at < 0) & (at + HALO == col)
        halo_rows = rms_norm(halo_v[...], norm_gain_ref[...])
        before = jnp.dot(early.astype(jnp.bfloat16), halo_rows, preferred_element_type=jnp.float32)
        normed_v[0:edge] = (normed_v[0:edge].astype(jnp.float32) + before).astype(jnp.bfloat16)

    tasks = {"kv": take_kv, "send_kv": send_kv, "halo": send_halo, "norm": norm, "reorder": reorder_half}
    for name, head in START[lead:]:
        if name in tasks:
            with jax.named_scope(name):
                tasks[name](head)
        else:
            getattr(ex, name)(head)
    for copy in (loads[3], loads[4], loads[7], loads[8]):
        copy.wait()

    per_owner = heads // seq_parts

    def summary_copy(head, slot):
        return pltpu.make_async_remote_copy(
            src_ref=summary_v.at[head],
            dst_ref=theirs_ref.at[slot],
            send_sem=side_send.at[3],
            recv_sem=side_recv.at[3],
            device_id=beside,
            device_id_type=MESH_ID,
        )

    inner = lax.broadcasted_iota(jnp.int32, (STEP_ROWS, HD), 0)
    first_at = start + lax.rem(inner, LANES_OF_TIME) * steps + lax.div(inner, LANES_OF_TIME)

    def project(head):
        columns = pl.ds(pl.multiple_of(head * HD, HD), HD)
        w_block = w_buf[head].reshape(normed_v.shape[1], HD)
        projected = jnp.dot(
            normed_v[...], w_block, preferred_element_type=jnp.float32
        ).astype(jnp.bfloat16)
        xp_v[...] = projected.astype(jnp.float32)
        row = lax.broadcasted_iota(jnp.int32, (HALO, rows_ext), 1)
        wanted = length - (TAPS - 1) + lax.broadcasted_iota(jnp.int32, (HALO, rows_ext), 0) - 2
        step = lax.div(row, LANES_OF_TIME) - (TAPS - 1)
        at = start + lax.rem(row, LANES_OF_TIME) * steps + step
        real = (step >= 0) & (step < steps) & (wanted < length) & (wanted >= length - (TAPS - 1))
        picker = (real & (at == wanted)).astype(jnp.bfloat16)
        picked = jnp.dot(picker, projected, preferred_element_type=jnp.float32)
        conv_w = conv_ref[:, columns]
        conv_sum = conv_w[0:1] * xp_v[0:local_len]
        for offset in range(1, TAPS):
            shift = offset * LANES_OF_TIME
            conv_sum = conv_sum + conv_w[offset : offset + 1] * xp_v[shift : shift + local_len]
        x_conv = conv_sum.astype(jnp.bfloat16)
        xc_v[...] = x_conv.astype(jnp.float32)
        ga_v[...] = jnp.dot(x_conv, wa_v[head], preferred_element_type=jnp.float32)
        gi_v[...] = jnp.dot(x_conv, wi_v[head], preferred_element_type=jnp.float32)
        picked_v[...] = picked[0:LANES_OF_TIME]

    def scan(head):
        columns = pl.ds(pl.multiple_of(head * HD, HD), HD)
        rate = -8.0 * jax.nn.softplus(-decay_ref[:, columns])

        def block(i, carry):
            state, rate_sum = carry
            rows = pl.ds(pl.multiple_of(i * STEP_ROWS, STEP_ROWS), STEP_ROWS)
            valid = first_at + i * (STEP_ROWS // LANES_OF_TIME) < length
            log_rate = rate * jax.nn.sigmoid(ga_v[rows])
            fall = -2.0 * log_rate
            lost = 1.0 - fall * (1.0 / 6.0)
            for order in (5.0, 4.0, 3.0, 2.0):
                lost = 1.0 - fall * (1.0 / order) * lost
            lost = fall * lost
            root = lost * lax.rsqrt(jnp.maximum(lost, 1e-37))
            push = jnp.where(valid, root * jax.nn.sigmoid(gi_v[rows]) * xc_v[rows], 0.0)
            held = jnp.where(valid, log_rate, 0.0)
            keep = jnp.exp(held)
            for k in range(STEP_ROWS // LANES_OF_TIME):
                tile = slice(k * LANES_OF_TIME, (k + 1) * LANES_OF_TIME)
                state = keep[tile] * state + push[tile]
                rate_sum = rate_sum + held[tile]
            return state, rate_sum

        zeros = jnp.zeros((LANES_OF_TIME, HD), jnp.float32)
        state, rate_sum = lax.fori_loop(0, local_len // STEP_ROWS, block, (zeros, zeros))
        keep_all = jnp.exp(rate_sum)
        total = state[0:1]
        for s in range(1, LANES_OF_TIME):
            total = keep_all[s : s + 1] * total + state[s : s + 1]
        keep_total = jnp.exp(jnp.sum(rate_sum, axis=0, keepdims=True))
        place = lax.broadcasted_iota(jnp.int32, (LANES_OF_TIME, HD), 0)
        summary_v[head] = jnp.where(
            place == 0, keep_total, jnp.where(place == 1, total, picked_v[...])
        )

        @pl.when(lax.div(head, per_owner) != y)
        def _():
            summary_copy(head, lax.rem(head, per_owner)).start()

    def take(steps):
        for name, head in steps:
            if name in tasks:
                with jax.named_scope(name):
                    tasks[name](head)
            else:
                getattr(ex, name)(head)

    def head_step(head, carry):
        for slot, (name, task) in enumerate((("project", project), ("scan", scan))):
            for at, steps in enumerate(SLOTS):
                if steps[slot]:
                    pl.when(head == at)(functools.partial(take, steps[slot]))
            with jax.named_scope(name):
                task(head)
        return carry

    lax.fori_loop(0, heads, head_step, 0)

    own_ref[...] = summary_v[pl.ds(y * per_owner, per_owner)]
    every = summary_v.at[pl.ds(0, per_owner)]
    exchanged = pltpu.make_async_remote_copy(
        src_ref=every,
        dst_ref=theirs_ref,
        send_sem=side_send.at[3],
        recv_sem=side_recv.at[3],
        device_id=beside,
        device_id_type=MESH_ID,
    )
    for copy in kv_copies:
        copy.wait()

    @pl.when(y == 0)
    def _():
        halo_copy.wait_send()

    ex.settled()
    with jax.named_scope("exchanged"):
        exchanged.wait()


def finish_kernel(
    own_ref, theirs_ref, kv_ref, state_hbm, conv_hbm, cache_hbm, zeros_v, state_v, conv_v, out_sem
):
    rest = kv_ref.shape[0]
    store = [
        pltpu.make_async_copy(kv_ref, cache_hbm.at[pl.ds(0, rest)], out_sem.at[0]),
        pltpu.make_async_copy(zeros_v, cache_hbm.at[pl.ds(rest, zeros_v.shape[0])], out_sem.at[1]),
        pltpu.make_async_copy(state_v, state_hbm, out_sem.at[2]),
        pltpu.make_async_copy(conv_v, conv_hbm, out_sem.at[3]),
    ]
    store[0].start()
    first_half = lax.axis_index("seq") == 0
    for k in range(own_ref.shape[0]):
        own, got = own_ref[k], theirs_ref[k]
        head_part = jnp.where(first_half, own, got)
        tail_part = jnp.where(first_half, got, own)
        columns = slice(k * HD, (k + 1) * HD)
        state_v[:, columns] = tail_part[0:1] * head_part[1:2] + tail_part[1:2]
        picked = head_part[2 : 1 + TAPS] + tail_part[2 : 1 + TAPS]
        conv_v[0, :, columns] = picked.astype(jnp.bfloat16)
    store[2].start()
    store[3].start()
    zeros_v[...] = jnp.zeros_like(zeros_v)
    store[1].start()
    for copy in store:
        copy.wait()


def gathered_on_device(
    sizes, tokens, attn_in, lengths, norm_gain, attn_gain, w_x, conv_w, w_a, w_i, lru_decay, w_kv
):
    local_len, width = tokens.shape[1:]
    z_size, x_size, cores, seq_parts = sizes
    heads = width // HD
    rows_ext = -(-(local_len + (TAPS - 1) * LANES_OF_TIME) // HALO) * HALO
    anywhere = pl.BlockSpec(memory_space=pl.ANY)
    vmem = pl.BlockSpec(memory_space=pltpu.VMEM)
    owned = width // seq_parts
    per_owner = heads // seq_parts
    half = w_kv.shape[1] // seq_parts
    own, theirs, kv = pl.pallas_call(
        functools.partial(prefill_kernel, sizes),
        in_specs=[pl.BlockSpec(memory_space=pltpu.HBM)] * 11,
        out_specs=(vmem, vmem, vmem),
        out_shape=(
            pltpu.VMEM((per_owner, LANES_OF_TIME, HD), jnp.float32),
            pltpu.VMEM((per_owner, LANES_OF_TIME, HD), jnp.float32),
            pltpu.VMEM((seq_parts * local_len, half), jnp.bfloat16),
        ),
        scratch_shapes=[
            pltpu.VMEM((heads, z_size, x_size, cores, seq_parts, w_x.shape[0], HD), jnp.bfloat16),
            pltpu.VMEM((local_len, width), jnp.bfloat16),
            pltpu.VMEM((local_len, width), jnp.bfloat16),
            pltpu.VMEM(w_kv.shape, jnp.bfloat16),
            pltpu.VMEM(w_a.shape, jnp.bfloat16),
            pltpu.VMEM(w_i.shape, jnp.bfloat16),
            pltpu.VMEM((HALO, width), jnp.bfloat16),
            pltpu.VMEM((local_len, width), jnp.bfloat16),
            pltpu.VMEM((rows_ext, width), jnp.bfloat16),
            pltpu.VMEM((local_len, half), jnp.bfloat16),
            pltpu.VMEM((rows_ext, HD), jnp.float32),
            pltpu.VMEM((local_len, HD), jnp.float32),
            pltpu.VMEM((local_len, HD), jnp.float32),
            pltpu.VMEM((local_len, HD), jnp.float32),
            pltpu.VMEM((heads, LANES_OF_TIME, HD), jnp.float32),
            pltpu.VMEM((LANES_OF_TIME, HD), jnp.float32),
            pltpu.VMEM((2, local_len // 2, HD // 2), jnp.float32),
            pltpu.VMEM((1, width), jnp.float32),
            pltpu.VMEM((1, width), jnp.float32),
            pltpu.VMEM((1, width), jnp.float32),
            pltpu.VMEM(conv_w.shape, jnp.float32),
            pltpu.SMEM((1,), jnp.int32),
            pltpu.SemaphoreType.DMA((3, 2, len(SPLITS))),
            pltpu.SemaphoreType.DMA((heads, 4)),
            pltpu.SemaphoreType.DMA((1,)),
            pltpu.SemaphoreType.DMA((heads,)),
            pltpu.SemaphoreType.DMA((11,)),
            pltpu.SemaphoreType.DMA((4,)),
            pltpu.SemaphoreType.DMA((4,)),
        ],
        compiler_params=pltpu.CompilerParams(
            collective_id=0, has_side_effects=True, vmem_limit_bytes=60 * 1024 * 1024
        ),
    )(
        lengths,
        tokens[0],
        attn_in[0],
        norm_gain,
        attn_gain,
        w_x,
        conv_w,
        w_a,
        w_i,
        lru_decay,
        w_kv,
    )
    state_shape, conv_shape = (1, owned), (1, TAPS - 1, owned)
    state, conv_state, cache = pl.pallas_call(
        finish_kernel,
        in_specs=[vmem] * 3,
        out_specs=(anywhere, anywhere, anywhere),
        out_shape=(
            jax.ShapeDtypeStruct(state_shape, jnp.float32),
            jax.ShapeDtypeStruct(conv_shape, jnp.bfloat16),
            jax.ShapeDtypeStruct((W, half), jnp.bfloat16),
        ),
        scratch_shapes=[
            pltpu.VMEM((W - kv.shape[0], half), jnp.bfloat16),
            pltpu.VMEM(state_shape, jnp.float32),
            pltpu.VMEM(conv_shape, jnp.bfloat16),
            pltpu.SemaphoreType.DMA((4,)),
        ],
    )(*(pltpu.with_memory_space_constraint(v, pltpu.VMEM) for v in (own, theirs, kv)))
    return state, conv_state, cache[None]


def fits(mesh, sizes, tokens, w_x, w_kv):
    if sizes is None:
        return False
    _, length, width = tokens.shape
    devices = mesh.size
    seq_parts = mesh.shape["seq"]
    return (
        length < W
        and width % (HD * seq_parts) == 0
        and w_x.shape[0] % (devices * HALO) == 0
        and w_x.shape[0] // devices > max(p + q for _, (p, q) in SPLITS)
        and width // HD == sum(n for n, _ in SPLITS) == len(SLOTS)
        and w_kv.shape[1] == seq_parts * HD
        and tokens.shape[0] == mesh.shape["batch"]
    )


def solution(mesh):
    in_specs = (
        P("batch", "seq", None),
        P("batch", "seq", None),
        P("batch"),
        P(),
        P(),
        P(("batch", "seq"), None),
        P(),
        P(),
        P(),
        P(),
        P(),
    )
    out_specs = (P("batch", "seq"), P("batch", None, "seq"), P("batch", None, "seq"))
    sizes = physical_grid(mesh)

    def run(*arrays):
        tokens, w_x, w_kv = arrays[0], arrays[5], arrays[10]
        body = on_device
        if fits(mesh, sizes, tokens, w_x, w_kv):
            body = functools.partial(gathered_on_device, sizes)
        return jax.shard_map(
            body, mesh=mesh, in_specs=in_specs, out_specs=out_specs, check_vma=False
        )(*arrays)

    return run
```

```python
import functools

import jax
import jax.numpy as jnp
from jax import lax
from jax.experimental import pallas as pl
from jax.experimental.pallas import tpu as pltpu
from jax.sharding import PartitionSpec as P

H = 10
HD = 256
W = 2048
LANES_OF_TIME = 8
TAPS = 4
HALO = 16
STEP_ROWS = 32


def passed_along(block, axis, distance):
    devices = range(lax.axis_size(axis))
    route = [(i - distance, i) for i in devices if i - distance in devices]
    return lax.ppermute(block, axis, route)


def rms_norm(values, gain_vec):
    widened = values.astype(jnp.float32)
    inverse = lax.rsqrt(jnp.mean(widened * widened, axis=-1, keepdims=True) + 1e-06)
    return (widened * inverse * gain_vec).astype(jnp.bfloat16)


def rotate_keys(key_rows, positions):
    quarter = key_rows.shape[-1] // 4
    spacing = jnp.exp(-jnp.log(10000.0) * jnp.arange(quarter, dtype=jnp.float32) / quarter)
    angles = positions.astype(jnp.float32)[:, None] * spacing[None, :]
    cosine_rows = jnp.cos(angles)
    sine_rows = jnp.sin(angles)
    first_part = key_rows[:, :quarter]
    second_part = key_rows[:, quarter : 2 * quarter]
    return jnp.concatenate(
        [
            first_part * cosine_rows - second_part * sine_rows,
            second_part * cosine_rows + first_part * sine_rows,
            key_rows[:, 2 * quarter :],
        ],
        axis=1,
    )


def ordered_rows(tokens_ref, halo_ref, gain_ref, normed_ref):
    local_len = tokens_ref.shape[0]
    steps = local_len // LANES_OF_TIME
    row = lax.broadcasted_iota(jnp.int32, (normed_ref.shape[0], local_len + HALO), 0)
    col = lax.broadcasted_iota(jnp.int32, (normed_ref.shape[0], local_len + HALO), 1)
    at = lax.rem(row, LANES_OF_TIME) * steps + lax.div(row, LANES_OF_TIME) - (TAPS - 1)
    pick = (jnp.where(at < 0, at + local_len + HALO, at) == col).astype(jnp.bfloat16)
    rows = jnp.concatenate(
        [rms_norm(tokens_ref[...], gain_ref[...]), rms_norm(halo_ref[...], gain_ref[...])], axis=0
    )
    normed_ref[...] = jnp.dot(pick, rows, preferred_element_type=jnp.float32).astype(jnp.bfloat16)


def one_head(
    normed_ref, w_block, conv_w, w_a, w_i, rate, length, start, out_ref, xp_ref, xc_ref, ga_ref, gi_ref
):
    rows_ext = normed_ref.shape[0]
    local_len = xc_ref.shape[0]
    steps = local_len // LANES_OF_TIME
    projected = jnp.dot(normed_ref[...], w_block, preferred_element_type=jnp.float32).astype(
        jnp.bfloat16
    )
    xp_ref[...] = projected.astype(jnp.float32)
    row = lax.broadcasted_iota(jnp.int32, (HALO, rows_ext), 1)
    wanted = length - (TAPS - 1) + lax.broadcasted_iota(jnp.int32, (HALO, rows_ext), 0) - 2
    step = lax.div(row, LANES_OF_TIME) - (TAPS - 1)
    at = start + lax.rem(row, LANES_OF_TIME) * steps + step
    real = (step >= 0) & (step < steps) & (wanted < length) & (wanted >= length - (TAPS - 1))
    picker = (real & (at == wanted)).astype(jnp.bfloat16)
    picked = jnp.dot(picker, projected, preferred_element_type=jnp.float32)
    conv_sum = conv_w[0:1] * xp_ref[0:local_len]
    for offset in range(1, TAPS):
        shift = offset * LANES_OF_TIME
        conv_sum = conv_sum + conv_w[offset : offset + 1] * xp_ref[shift : shift + local_len]
    x_conv = conv_sum.astype(jnp.bfloat16)
    xc_ref[...] = x_conv.astype(jnp.float32)
    ga_ref[...] = jnp.dot(x_conv, w_a, preferred_element_type=jnp.float32)
    gi_ref[...] = jnp.dot(x_conv, w_i, preferred_element_type=jnp.float32)
    inner = lax.broadcasted_iota(jnp.int32, (STEP_ROWS, HD), 0)
    first_at = start + lax.rem(inner, LANES_OF_TIME) * steps + lax.div(inner, LANES_OF_TIME)

    def block(i, carry):
        state, rate_sum = carry
        rows = pl.ds(pl.multiple_of(i * STEP_ROWS, STEP_ROWS), STEP_ROWS)
        valid = first_at + i * (STEP_ROWS // LANES_OF_TIME) < length
        log_rate = rate * jax.nn.sigmoid(ga_ref[rows])
        fall = -2.0 * log_rate
        lost = 1.0 - fall * (1.0 / 6.0)
        for order in (5.0, 4.0, 3.0, 2.0):
            lost = 1.0 - fall * (1.0 / order) * lost
        lost = fall * lost
        root = lost * lax.rsqrt(jnp.maximum(lost, 1e-37))
        push = jnp.where(valid, root * jax.nn.sigmoid(gi_ref[rows]) * xc_ref[rows], 0.0)
        held = jnp.where(valid, log_rate, 0.0)
        keep = jnp.exp(held)
        for k in range(STEP_ROWS // LANES_OF_TIME):
            tile = slice(k * LANES_OF_TIME, (k + 1) * LANES_OF_TIME)
            state = keep[tile] * state + push[tile]
            rate_sum = rate_sum + held[tile]
        return state, rate_sum

    zeros = jnp.zeros((LANES_OF_TIME, HD), jnp.float32)
    state, rate_sum = lax.fori_loop(0, local_len // STEP_ROWS, block, (zeros, zeros))
    keep_all = jnp.exp(rate_sum)
    total = state[0:1]
    for s in range(1, LANES_OF_TIME):
        total = keep_all[s : s + 1] * total + state[s : s + 1]
    keep_total = jnp.exp(jnp.sum(rate_sum, axis=0, keepdims=True))
    place = lax.broadcasted_iota(jnp.int32, (LANES_OF_TIME, HD), 0)
    out_ref[...] = jnp.where(
        place == 0, keep_total, jnp.where(place == 1, total, picked[0:LANES_OF_TIME])
    )


def recurrent_kernel(
    length_ref,
    tokens_ref,
    halo_ref,
    gain_ref,
    w_ref,
    conv_ref,
    wa_ref,
    wi_ref,
    rate_ref,
    out_ref,
    normed_ref,
    *work
):
    @pl.when(pl.program_id(0) == 0)
    def _():
        ordered_rows(tokens_ref, halo_ref, gain_ref, normed_ref)

    start = lax.axis_index("seq") * tokens_ref.shape[0]
    one_head(
        normed_ref,
        w_ref[...],
        conv_ref[...],
        wa_ref[0],
        wi_ref[0],
        rate_ref[...],
        length_ref[0],
        start,
        out_ref,
        *work
    )


def recurrent(first, tokens, halo, lengths, norm_gain, w_part, conv_w, w_a, w_i, rate):
    local_len, width = tokens.shape
    part_width = w_part.shape[1]
    rows_ext = -(-(local_len + (TAPS - 1) * LANES_OF_TIME) // HALO) * HALO
    whole = lambda *shape: pl.BlockSpec(shape, lambda h: (0,) * len(shape))
    return pl.pallas_call(
        recurrent_kernel,
        grid=(part_width // HD,),
        in_specs=[
            pl.BlockSpec(memory_space=pltpu.SMEM),
            whole(local_len, width),
            whole(HALO, width),
            whole(1, width),
            pl.BlockSpec((width, HD), lambda h: (0, h)),
            pl.BlockSpec((TAPS, HD), lambda h: (0, h + first)),
            pl.BlockSpec((1, HD, HD), lambda h: (h + first, 0, 0)),
            pl.BlockSpec((1, HD, HD), lambda h: (h + first, 0, 0)),
            pl.BlockSpec((1, HD), lambda h: (0, h + first)),
        ],
        out_specs=pl.BlockSpec((LANES_OF_TIME, HD), lambda h: (0, h)),
        out_shape=jax.ShapeDtypeStruct((LANES_OF_TIME, part_width), jnp.float32),
        scratch_shapes=[
            pltpu.VMEM((rows_ext, width), jnp.bfloat16),
            pltpu.VMEM((rows_ext, HD), jnp.float32),
            pltpu.VMEM((local_len, HD), jnp.float32),
            pltpu.VMEM((local_len, HD), jnp.float32),
            pltpu.VMEM((local_len, HD), jnp.float32),
        ],
        compiler_params=pltpu.CompilerParams(vmem_limit_bytes=60 * 1024 * 1024),
        cost_estimate=pl.CostEstimate(
            flops=2 * local_len * part_width * (width + 2 * HD),
            bytes_accessed=2 * width * (local_len + part_width),
            transcendentals=6 * local_len * part_width,
        ),
    )(lengths, tokens, halo, norm_gain[None], w_part, conv_w, w_a, w_i, rate[None])


def on_device(
    tokens, attn_in, lengths, norm_gain, attn_gain, w_x, conv_w, w_a, w_i, lru_decay, w_kv
):
    local_len = tokens.shape[1]
    feature_dim = tokens.shape[2]
    seq_parts = lax.axis_size("seq")
    seq_place = lax.axis_index("seq")
    length = lengths[0]
    halo = passed_along(tokens[0, local_len - HALO :], "seq", 1)
    heads = feature_dim // HD
    early = (4 * heads) // 5
    positions = seq_place * local_len + jnp.arange(local_len, dtype=jnp.int32)
    attn_normed = rms_norm(attn_in[0], attn_gain)
    kv_full = jnp.dot(attn_normed, w_kv, preferred_element_type=jnp.float32)
    kv_rows = jnp.concatenate(
        [rotate_keys(kv_full[:, :HD], positions), kv_full[:, HD:]], axis=1
    ).astype(jnp.bfloat16)
    in_window = ((positions >= length - W) & (positions < length))[:, None]
    masked = jnp.where(in_window, kv_rows, jnp.zeros_like(kv_rows))
    by_column = lax.all_to_all(masked, "seq", split_axis=1, concat_axis=0, tiled=True)
    laps = -(-seq_parts * local_len // W)
    by_column = jnp.pad(by_column, ((0, laps * W - seq_parts * local_len), (0, 0)))
    kv_cache = by_column[:W]
    for lap in range(1, laps):
        kv_cache = kv_cache + by_column[lap * W : (lap + 1) * W]
    w_early = lax.all_gather(w_x[:, : early * HD], ("batch", "seq"), axis=0, tiled=True)
    w_early, w_local, kv_cache, halo = lax.optimization_barrier((w_early, w_x, kv_cache, halo))
    w_late = lax.all_gather(w_local[:, early * HD :], ("batch", "seq"), axis=0, tiled=True)
    w_parts = ((0, w_early), (early, w_late))
    rate = -8.0 * jax.nn.softplus(-lru_decay)
    summary = jnp.concatenate(
        [
            recurrent(first, tokens[0], halo, lengths, norm_gain, w_part, conv_w, w_a, w_i, rate)
            for first, w_part in w_parts
        ],
        axis=1,
    )
    owned_width = feature_dim // seq_parts
    gathered = lax.all_gather(summary, "seq", axis=0, tiled=True)
    owned = lax.dynamic_slice_in_dim(gathered, seq_place * owned_width, owned_width, 1)
    state = owned[1:2]
    picked = owned[2:5]
    for part in range(1, seq_parts):
        at = part * LANES_OF_TIME
        state = owned[at : at + 1] * state + owned[at + 1 : at + 2]
        picked = picked + owned[at + 2 : at + 5]
    conv_state = picked.astype(jnp.bfloat16)
    return (state, conv_state[None], kv_cache[None])


MESH_ID = pl.DeviceIdType.MESH
SPLITS = ((10, (16, 16)),)
NEAR, PLANE = 0, 1
EDGE = 8
START = (
    ("near", 0), ("plane", 0), ("own", 0), ("near", 1), ("plane", 1), ("own", 1), ("near", 2), ("plane", 2),
    ("own", 2), ("plane", 3), ("own", 3), ("plane", 4), ("own", 4), ("kv", 0), ("halo", 0), ("second", 0),
    ("near", 3), ("send_kv", 0), ("kv", 1), ("second", 1), ("third", 0), ("send_kv", 1), ("norm", 0), ("near", 4),
    ("second", 2), ("third_plane", 0), ("third", 1), ("reorder", 0), ("second", 3), ("third_plane", 1),
    ("reorder", 1),
)
SLOTS = (
    (
        (
            ("fourth", 0), ("ready", 0), ("near", 5), ("plane", 5), ("own", 5), ("second", 4), ("third_plane", 2),
            ("third", 2),
        ),
        (
            ("fourth", 1),
        ),
    ),
    (
        (
            ("ready", 1), ("near", 6), ("plane", 6), ("own", 6), ("second", 5), ("third_plane", 3), ("third", 3),
        ),
        (
            ("fourth", 2),
        ),
    ),
    (
        (
            ("ready", 2), ("near", 7), ("plane", 7), ("own", 7), ("second", 6), ("third_plane", 4), ("third", 4),
        ),
        (
            ("fourth", 3),
        ),
    ),
    (
        (
            ("ready", 3), ("near", 8), ("plane", 8), ("own", 8), ("second", 7), ("third_plane", 5), ("third", 5),
        ),
        (
            ("fourth", 4),
        ),
    ),
    (
        (
            ("ready", 4), ("near", 9), ("plane", 9), ("own", 9), ("second", 8), ("third_plane", 6), ("third", 6),
        ),
        (
            ("fourth", 5),
        ),
    ),
    (
        (
            ("ready", 5), ("second", 9), ("third_plane", 7), ("third", 7),
        ),
        (
            ("fourth", 6),
        ),
    ),
    (
        (
            ("ready", 6), ("third_plane", 8), ("third", 8),
        ),
        (
            ("fourth", 7),
        ),
    ),
    (
        (
            ("ready", 7), ("third_plane", 9), ("third", 9),
        ),
        (
            ("fourth", 8),
        ),
    ),
    (
        (
            ("ready", 8),
        ),
        (
            ("fourth", 9),
        ),
    ),
    (
        (
            ("ready", 9),
        ),
        (),
    ),
)


def physical_grid(mesh):
    grid = mesh.devices
    try:
        spots = [
            [(*device.coords, device.core_on_chip) for device in line] for line in grid.tolist()
        ]
    except AttributeError:
        return None
    sizes = [len({spot[k] for line in spots for spot in line}) for k in range(4)]
    low = [min(spot[k] for line in spots for spot in line) for k in range(4)]
    x_size, y_size, z_size, cores = sizes
    if (x_size, y_size, z_size, cores) != (2, 2, 4, 2) or grid.shape != (z_size * x_size * cores, y_size):
        return None
    for b, line in enumerate(spots):
        for y, spot in enumerate(line):
            want = ((b // cores) % x_size, y, b // (cores * x_size), b % cores)
            if tuple(v - l for v, l in zip(spot, low)) != want:
                return None
    return z_size, x_size, cores, y_size


def scoped(method):
    @functools.wraps(method)
    def inside(*args):
        with jax.named_scope(method.__name__):
            return method(*args)

    return inside


def by_split(method):
    @functools.wraps(method)
    def inside(exchange, head):
        with jax.named_scope(method.__name__):
            first = 0
            for index, (count, _) in enumerate(SPLITS):
                last = first + count
                if isinstance(head, int):
                    if first <= head < last:
                        method(exchange, head, index)
                elif len(SPLITS) == 1:
                    method(exchange, head, index)
                else:

                    @pl.when((head >= first) & (head < last))
                    def _():
                        method(exchange, head, index)

                first = last

    return inside


class Exchange:
    def __init__(self, sizes, heads, w_buf, send_sem, recv_sem, core_send, core_recv):
        self.sizes, self.heads = sizes, heads
        self.w_buf, self.send_sem, self.recv_sem = w_buf, send_sem, recv_sem
        self.core_send, self.core_recv = core_send, core_recv
        z_size, x_size, cores, _ = sizes
        at = lax.axis_index("batch")
        self.core = lax.rem(at, cores)
        self.x = lax.rem(lax.div(at, cores), x_size)
        self.z = lax.div(at, cores * x_size)
        self.y = lax.axis_index("seq")
        self.shard_rows = w_buf.shape[5]
        self.is_end = (self.z == 0) | (self.z == z_size - 1)

    def device(self, z=None, x=None, core=None, y=None):
        z = self.z if z is None else z
        x = self.x if x is None else x
        core = self.core if core is None else core
        y = self.y if y is None else y
        _, x_size, cores, _ = self.sizes
        return ((z * x_size + x) * cores + core, y)

    def peers(self):
        z_size = self.sizes[0]
        along = [self.device(z=lax.rem(self.z + d, z_size)) for d in range(1, z_size)]
        return along + [
            self.device(x=1 - self.x),
            self.device(y=1 - self.y),
            self.device(x=1 - self.x, y=1 - self.y),
            self.device(core=1 - self.core),
        ]

    def blocks(self, head, z, x, y, first, rows, core=None):
        core = self.core if core is None else core
        return self.w_buf.at[head, z, x, core, y, pl.ds(first, rows)]

    def copy(self, head, stage, group, split, part, to):
        return pltpu.make_async_remote_copy(
            src_ref=part,
            dst_ref=part,
            send_sem=self.send_sem.at[stage, group, split],
            recv_sem=self.recv_sem.at[head, stage if group == NEAR or stage != 1 else 3],
            device_id=to,
            device_id_type=MESH_ID,
        )

    def hand_over(self, head, part):
        pltpu.make_async_remote_copy(
            src_ref=part,
            dst_ref=part,
            send_sem=self.core_send.at[0],
            recv_sem=self.core_recv.at[head],
            device_id=self.device(core=1 - self.core),
            device_id_type=MESH_ID,
        ).start()

    def some(self, head, count, rows):
        every = slice(None)
        if count == 2:
            return self.w_buf.at[head, pl.ds(0, 2), 0, 0, 0, pl.ds(0, rows)]
        if count == 3:
            return self.w_buf.at[head, pl.ds(0, 3), 0, 0, 0, pl.ds(0, rows)]
        if count == 4:
            return self.w_buf.at[head, every, 0, 0, 0, pl.ds(0, rows)]
        if count == 8:
            return self.w_buf.at[head, every, every, 0, 0, pl.ds(0, rows)]
        return self.w_buf.at[head, pl.ds(0, 3), every, 0, every, pl.ds(0, rows)]

    def arrived(self, head, stage, group, count, rows):
        part = self.some(head, count, rows)
        self.copy(head, stage, group, 0, part, self.device(core=1 - self.core)).wait_recv()

    def left(self, stage, group, split, count, rows):
        first = sum(n for n, _ in SPLITS[:split])
        part = self.some(pl.ds(first, SPLITS[split][0]), count, rows)
        self.copy(0, stage, group, split, part, self.device(core=1 - self.core)).wait_send()

    def routes(self, split, act):
        plane_rows, turned = SPLITS[split][1]

        @pl.when(self.core == 0)
        def _():
            if turned:
                act("yx", plane_rows, turned)
            act("xy", plane_rows + turned, self.shard_rows - plane_rows - turned)

        @pl.when(self.core != 0)
        def _():
            act("yx", plane_rows, self.shard_rows - plane_rows)

    @by_split
    def near(self, head, split):
        plane_rows = SPLITS[split][1][0]
        part = self.blocks(head, self.z, self.x, self.y, plane_rows, self.shard_rows - plane_rows)
        for d in range(1, self.sizes[0]):
            to = self.device(z=lax.rem(self.z + d, self.sizes[0]))
            self.copy(head, 0, NEAR, split, part, to).start()

    def across(self, order):
        beside = self.device(x=1 - self.x), self.device(y=1 - self.y)
        return beside if order == "xy" else beside[::-1]

    @by_split
    def own(self, head, split):
        def near(order, first, rows):
            own = self.blocks(head, self.z, self.x, self.y, first, rows)
            for stage, to in enumerate(self.across(order)):
                self.copy(head, 1 + stage, NEAR, split, own, to).start()

        self.routes(split, near)

    @by_split
    def plane(self, head, split):
        plane_rows = SPLITS[split][1][0]
        plane = self.blocks(head, self.z, self.x, self.y, 0, plane_rows)
        self.copy(head, 0, PLANE, split, plane, self.device(x=1 - self.x)).start()
        self.copy(head, 0, PLANE, split, plane, self.device(y=1 - self.y)).start()
        self.copy(head, 0, PLANE, split, plane, self.device(x=1 - self.x, y=1 - self.y)).start()

    @by_split
    def second(self, head, split):
        plane_rows = SPLITS[split][1][0]
        every = slice(None)
        last = self.sizes[0] - 1
        self.arrived(head, 0, NEAR, 3, self.shard_rows)

        def near(order, first, rows):
            for stage, to in enumerate(self.across(order)):
                for d in range(1, last + 1):
                    at = lax.rem(self.z + d, last + 1)
                    part = self.blocks(head, at, self.x, self.y, first, rows)
                    self.copy(head, 1 + stage, NEAR, split, part, to).start()
            self.hand_over(head, self.blocks(head, every, self.x, self.y, first, rows))

        self.routes(split, near)
        plane = self.blocks(head, self.z, every, every, 0, plane_rows)
        up = jnp.where(self.z == last, 1, self.z + 1)
        down = jnp.where(self.z == 0, last - 1, self.z - 1)
        self.copy(head, 1, PLANE, split, plane, self.device(z=up)).start()
        self.copy(head, 1, PLANE, split, plane, self.device(z=down)).start()
        self.hand_over(head, plane)

    @by_split
    def third(self, head, split):
        plane_rows = SPLITS[split][1][0]
        every = slice(None)
        self.arrived(head, 1, NEAR, 4, self.shard_rows - plane_rows)

        def near(order, first, rows):
            if order == "xy":
                part = self.blocks(head, every, 1 - self.x, self.y, first, rows)
            else:
                part = self.blocks(head, every, self.x, 1 - self.y, first, rows)
            to = self.across(order)[1]
            self.copy(head, 2, NEAR, split, part, to).start()
            self.hand_over(head, part)

        self.routes(split, near)

    @by_split
    def third_plane(self, head, split):
        plane_rows = SPLITS[split][1][0]
        every = slice(None)
        last = self.sizes[0] - 1

        @pl.when(self.is_end)
        def _():
            self.arrived(head, 1, PLANE, 4, plane_rows)

        @pl.when(jnp.logical_not(self.is_end))
        def _():
            self.arrived(head, 1, PLANE, 12, plane_rows)
            half = (last + 1) // 2
            start = jnp.where(self.z >= half, 0, half)
            part = self.blocks(head, pl.ds(start, half), every, every, 0, plane_rows)
            self.copy(head, 2, PLANE, split, part, self.device(z=jnp.where(self.z >= half, last, 0))).start()

    @by_split
    def fourth(self, head, split):
        plane_rows = SPLITS[split][1][0]
        every = slice(None)
        z_size = self.sizes[0]

        @pl.when(self.is_end)
        def _():
            self.arrived(head, 2, NEAR, 8, self.shard_rows)

        @pl.when(jnp.logical_not(self.is_end))
        def _():
            self.arrived(head, 2, NEAR, 8, self.shard_rows - plane_rows)

        def near(order, first, rows):
            if order == "xy":
                part = self.blocks(head, every, every, 1 - self.y, first, rows)
            else:
                part = self.blocks(head, every, 1 - self.x, every, first, rows)
            self.hand_over(head, part)

        self.routes(split, near)

        for d in range(1, z_size):
            self.hand_over(head, self.blocks(head, lax.rem(self.z + d, z_size), every, every, 0, plane_rows))

    def handed(self, head, core):
        part = self.w_buf.at[head, slice(None), slice(None), core]
        return pltpu.make_async_remote_copy(
            src_ref=part,
            dst_ref=part,
            send_sem=self.core_send.at[0],
            recv_sem=self.core_recv.at[0 if isinstance(head, slice) else head],
            device_id=self.device(core=1 - self.core),
            device_id_type=MESH_ID,
        )

    @scoped
    def ready(self, head):
        self.handed(head, 1 - self.core).wait_recv()

    @scoped
    def settled(self):
        for split, (_, (plane_rows, _)) in enumerate(SPLITS):
            near_rows = self.shard_rows - plane_rows
            self.left(0, NEAR, split, 3, near_rows)
            self.left(0, PLANE, split, 3, plane_rows)
            self.left(1, NEAR, split, 4, near_rows)
            self.left(1, PLANE, split, 8, plane_rows)
            self.left(2, NEAR, split, 8, near_rows)

            @pl.when(jnp.logical_not(self.is_end))
            def _():
                self.left(2, PLANE, split, 8, plane_rows)

        self.handed(slice(None), self.core).wait_send()


def prefill_kernel(
    sizes,
    length_hbm,
    tokens_hbm,
    attn_hbm,
    norm_gain_hbm,
    attn_gain_hbm,
    w_hbm,
    conv_hbm,
    wa_hbm,
    wi_hbm,
    decay_hbm,
    wkv_hbm,
    own_ref,
    theirs_ref,
    cache_ref,
    w_buf,
    tokens_v,
    attn_v,
    wkv_v,
    wa_v,
    wi_v,
    halo_v,
    rows_v,
    normed_v,
    kv_v,
    xp_v,
    xc_v,
    ga_v,
    gi_v,
    summary_v,
    picked_v,
    turn_v,
    norm_gain_ref,
    attn_gain_ref,
    decay_ref,
    conv_ref,
    length_ref,
    send_sem,
    recv_sem,
    core_send,
    core_recv,
    load_sem,
    side_send,
    side_recv,
):
    heads = w_buf.shape[0]
    local_len = tokens_v.shape[0]
    seq_parts = sizes[3]
    ex = Exchange(sizes, heads, w_buf, send_sem, recv_sem, core_send, core_recv)
    y = ex.y
    start = y * local_len
    beside = ex.device(y=1 - y)

    shard = [
        pltpu.make_async_copy(
            w_hbm.at[:, pl.ds(h * HD, HD)], w_buf.at[h, ex.z, ex.x, ex.core, y], load_sem.at[10]
        )
        for h in range(heads)
    ]
    loads = [
        pltpu.make_async_copy(source, target, load_sem.at[i])
        for i, (source, target) in enumerate(
            (
                (tokens_hbm, tokens_v),
                (attn_hbm, attn_v),
                (wkv_hbm, wkv_v),
                (wa_hbm, wa_v),
                (wi_hbm, wi_v),
                (norm_gain_hbm, norm_gain_ref.at[0]),
                (attn_gain_hbm, attn_gain_ref.at[0]),
                (decay_hbm, decay_ref.at[0]),
                (conv_hbm, conv_ref),
                (length_hbm, length_ref),
            )
        )
    ]
    for copy in shard:
        copy.start()

    barrier = pltpu.get_barrier_semaphore()
    peers = ex.peers()
    for peer in peers:
        pl.semaphore_signal(barrier, inc=1, device_id=peer, device_id_type=MESH_ID)

    own_shard = w_buf.at[:, ex.z, ex.x, ex.core, y]
    pltpu.make_async_copy(own_shard, own_shard, load_sem.at[10]).wait()
    for copy in [loads[1], loads[2], loads[6], loads[9], loads[0], *loads[3:6], loads[7], loads[8]]:
        copy.start()
    pl.semaphore_wait(barrier, len(peers))
    lead = START.index(("kv", 0))
    for name, head in START[:lead]:
        getattr(ex, name)(head)

    quarter = HD // 4
    lane = lax.broadcasted_iota(jnp.int32, (1, 2 * quarter), 1)
    spacing = jnp.exp(
        (-jnp.log(10000.0) / quarter) * lax.rem(lane, quarter).astype(jnp.float32)
    )
    half_len = local_len // 2
    fine = lax.broadcasted_iota(jnp.int32, (half_len, 2 * quarter), 0).astype(jnp.float32) * spacing
    turn_v[0] = jnp.cos(fine)
    turn_v[1] = jnp.sin(fine)

    loads[6].wait()
    loads[9].wait()
    length = length_ref[0]

    def kv_half(k):
        rows = slice(k * half_len, (k + 1) * half_len)
        normed = rms_norm(attn_v[rows], attn_gain_ref[...])
        full = jnp.dot(normed, wkv_v[...], preferred_element_type=jnp.float32)
        place = start + k * half_len
        coarse = place.astype(jnp.float32) * spacing
        cos_c, sin_c = jnp.cos(coarse), jnp.sin(coarse)
        cosine = cos_c * turn_v[0] - sin_c * turn_v[1]
        sine = sin_c * turn_v[0] + cos_c * turn_v[1]
        sine = jnp.where(lane < quarter, -sine, sine)
        at = place + lax.broadcasted_iota(jnp.int32, (half_len, 1), 0)
        window = (at >= length - W) & (at < length)
        turned = full[:, : 2 * quarter]
        other = pltpu.roll(turned, quarter, axis=1)
        turned = turned * cosine + other * sine

        keys = jnp.concatenate([turned, full[:, 2 * quarter : HD]], axis=1)
        first, second = (jnp.where(window, v, 0.0).astype(jnp.bfloat16) for v in (keys, full[:, HD:]))
        cache_ref[pl.ds(place, half_len)] = jnp.where(y == 0, first, second)
        kv_v[rows] = jnp.where(y == 0, second, first)

    halo_copy = pltpu.make_async_remote_copy(
        src_ref=tokens_v.at[pl.ds(local_len - EDGE, EDGE)],
        dst_ref=halo_v,
        send_sem=side_send.at[0],
        recv_sem=side_recv.at[0],
        device_id=beside,
        device_id_type=MESH_ID,
    )
    kv_copies = [
        pltpu.make_async_remote_copy(
            src_ref=kv_v.at[pl.ds(k * half_len, half_len)],
            dst_ref=cache_ref.at[pl.ds(start + k * half_len, half_len)],
            send_sem=side_send.at[1 + k],
            recv_sem=side_recv.at[1 + k],
            device_id=beside,
            device_id_type=MESH_ID,
        )
        for k in range(2)
    ]

    def take_kv(k):
        if k == 0:
            loads[1].wait()
            loads[2].wait()
        kv_half(k)

    def send_kv(k):
        kv_copies[k].start()

    def send_halo(_):
        loads[0].wait()

        @pl.when(y == 0)
        def _():
            halo_copy.start()
            halo_v[...] = jnp.zeros_like(halo_v)

    norm_step = 64

    def norm_rows(i, carry):
        rows = pl.ds(pl.multiple_of(i * norm_step, norm_step), norm_step)
        rows_v[rows] = rms_norm(tokens_v[rows], norm_gain_ref[...])
        return carry

    def norm(_):
        loads[5].wait()
        lax.fori_loop(0, local_len // norm_step, norm_rows, 0)

    steps = local_len // LANES_OF_TIME
    rows_ext = normed_v.shape[0]
    row = lax.broadcasted_iota(jnp.int32, (rows_ext, local_len), 0)
    col = lax.broadcasted_iota(jnp.int32, (rows_ext, local_len), 1)
    at = lax.rem(row, LANES_OF_TIME) * steps + lax.div(row, LANES_OF_TIME) - (TAPS - 1)
    pick = (at == col).astype(jnp.bfloat16)

    def reorder(i, carry):
        columns = pl.ds(pl.multiple_of(i * HD, HD), HD)
        normed_v[:, columns] = jnp.dot(
            pick, rows_v[:, columns], preferred_element_type=jnp.float32
        ).astype(jnp.bfloat16)
        return carry

    def reorder_half(k):
        half_heads = heads // 2
        lax.fori_loop(*((0, half_heads) if k == 0 else (half_heads, heads)), reorder, 0)
        if k == 0:
            return

        @pl.when(y != 0)
        def _():
            halo_copy.wait_recv()

        edge = 2 * HALO
        row = lax.broadcasted_iota(jnp.int32, (edge, EDGE), 0)
        col = lax.broadcasted_iota(jnp.int32, (edge, EDGE), 1)
        at = lax.div(row, LANES_OF_TIME) - (TAPS - 1)
        early = (lax.rem(row, LANES_OF_TIME) == 0) & (at < 0) & (at + EDGE == col)
        halo_rows = rms_norm(halo_v[...], norm_gain_ref[...])
        before = jnp.dot(early.astype(jnp.bfloat16), halo_rows, preferred_element_type=jnp.float32)
        normed_v[0:edge] = (normed_v[0:edge].astype(jnp.float32) + before).astype(jnp.bfloat16)

    tasks = {"kv": take_kv, "send_kv": send_kv, "halo": send_halo, "norm": norm, "reorder": reorder_half}
    for name, head in START[lead:]:
        if name in tasks:
            with jax.named_scope(name):
                tasks[name](head)
        else:
            getattr(ex, name)(head)
    for copy in (loads[3], loads[4], loads[7], loads[8]):
        copy.wait()

    per_owner = heads // seq_parts

    def summary_copy(head, slot):
        return pltpu.make_async_remote_copy(
            src_ref=summary_v.at[head],
            dst_ref=theirs_ref.at[slot],
            send_sem=side_send.at[3],
            recv_sem=side_recv.at[3],
            device_id=beside,
            device_id_type=MESH_ID,
        )

    inner = lax.broadcasted_iota(jnp.int32, (STEP_ROWS, HD), 0)
    first_at = start + lax.rem(inner, LANES_OF_TIME) * steps + lax.div(inner, LANES_OF_TIME)

    def project(head):
        columns = pl.ds(pl.multiple_of(head * HD, HD), HD)
        w_block = w_buf[head].reshape(normed_v.shape[1], HD)
        half_rows = rows_ext // 4
        projected = jnp.concatenate(
            [
                jnp.dot(normed_v[k * half_rows : (k + 1) * half_rows], w_block, preferred_element_type=jnp.float32)
                for k in range(4)
            ],
            axis=0,
        ).astype(jnp.bfloat16)
        xp_v[...] = projected.astype(jnp.float32)
        row = lax.broadcasted_iota(jnp.int32, (HALO, rows_ext), 1)
        wanted = length - (TAPS - 1) + lax.broadcasted_iota(jnp.int32, (HALO, rows_ext), 0) - 2
        step = lax.div(row, LANES_OF_TIME) - (TAPS - 1)
        at = start + lax.rem(row, LANES_OF_TIME) * steps + step
        real = (step >= 0) & (step < steps) & (wanted < length) & (wanted >= length - (TAPS - 1))
        picker = (real & (at == wanted)).astype(jnp.bfloat16)
        picked = jnp.dot(picker, projected, preferred_element_type=jnp.float32)
        conv_w = conv_ref[:, columns]
        conv_sum = conv_w[0:1] * xp_v[0:local_len]
        for offset in range(1, TAPS):
            shift = offset * LANES_OF_TIME
            conv_sum = conv_sum + conv_w[offset : offset + 1] * xp_v[shift : shift + local_len]
        x_conv = conv_sum.astype(jnp.bfloat16)
        xc_v[...] = x_conv.astype(jnp.float32)
        ga_v[...] = jnp.dot(x_conv, wa_v[head], preferred_element_type=jnp.float32)
        gi_v[...] = jnp.dot(x_conv, wi_v[head], preferred_element_type=jnp.float32)
        picked_v[...] = picked[0:LANES_OF_TIME]

    def scan(head):
        columns = pl.ds(pl.multiple_of(head * HD, HD), HD)
        rate = -8.0 * jax.nn.softplus(-decay_ref[:, columns])

        def block(i, carry):
            state, rate_sum = carry
            rows = pl.ds(pl.multiple_of(i * STEP_ROWS, STEP_ROWS), STEP_ROWS)
            valid = first_at + i * (STEP_ROWS // LANES_OF_TIME) < length
            log_rate = rate * jax.nn.sigmoid(ga_v[rows])
            fall = -2.0 * log_rate
            lost = 1.0 - fall * (1.0 / 6.0)
            for order in (5.0, 4.0, 3.0, 2.0):
                lost = 1.0 - fall * (1.0 / order) * lost
            lost = fall * lost
            root = lost * lax.rsqrt(jnp.maximum(lost, 1e-37))
            push = jnp.where(valid, root * jax.nn.sigmoid(gi_v[rows]) * xc_v[rows], 0.0)
            held = jnp.where(valid, log_rate, 0.0)
            keep = jnp.exp(held)
            for k in range(STEP_ROWS // LANES_OF_TIME):
                tile = slice(k * LANES_OF_TIME, (k + 1) * LANES_OF_TIME)
                state = keep[tile] * state + push[tile]
                rate_sum = rate_sum + held[tile]
            return state, rate_sum

        zeros = jnp.zeros((LANES_OF_TIME, HD), jnp.float32)
        state, rate_sum = lax.fori_loop(0, local_len // STEP_ROWS, block, (zeros, zeros))
        keep_all = jnp.exp(rate_sum)
        total = state[0:1]
        for s in range(1, LANES_OF_TIME):
            total = keep_all[s : s + 1] * total + state[s : s + 1]
        keep_total = jnp.exp(jnp.sum(rate_sum, axis=0, keepdims=True))
        place = lax.broadcasted_iota(jnp.int32, (LANES_OF_TIME, HD), 0)
        summary_v[head] = jnp.where(
            place == 0, keep_total, jnp.where(place == 1, total, picked_v[...])
        )

        @pl.when(lax.div(head, per_owner) != y)
        def _():
            summary_copy(head, lax.rem(head, per_owner)).start()

    def take(steps):
        for name, head in steps:
            if name in tasks:
                with jax.named_scope(name):
                    tasks[name](head)
            else:
                getattr(ex, name)(head)

    def head_step(head, carry):
        for slot, (name, task) in enumerate((("project", project), ("scan", scan))):
            for at, steps in enumerate(SLOTS):
                if steps[slot]:
                    pl.when(head == at)(functools.partial(take, steps[slot]))
            with jax.named_scope(name):
                task(head)
        return carry

    lax.fori_loop(0, heads, head_step, 0)

    own_ref[...] = summary_v[pl.ds(y * per_owner, per_owner)]
    every = summary_v.at[pl.ds(0, per_owner)]
    exchanged = pltpu.make_async_remote_copy(
        src_ref=every,
        dst_ref=theirs_ref,
        send_sem=side_send.at[3],
        recv_sem=side_recv.at[3],
        device_id=beside,
        device_id_type=MESH_ID,
    )
    for copy in kv_copies:
        copy.wait()

    @pl.when(y == 0)
    def _():
        halo_copy.wait_send()

    ex.settled()
    with jax.named_scope("exchanged"):
        exchanged.wait()


def finish_kernel(
    own_ref, theirs_ref, kv_ref, state_hbm, conv_hbm, cache_hbm, zeros_v, state_v, conv_v, out_sem
):
    rest = kv_ref.shape[0]
    store = [
        pltpu.make_async_copy(kv_ref, cache_hbm.at[pl.ds(0, rest)], out_sem.at[0]),
        pltpu.make_async_copy(zeros_v, cache_hbm.at[pl.ds(rest, zeros_v.shape[0])], out_sem.at[1]),
        pltpu.make_async_copy(state_v, state_hbm, out_sem.at[2]),
        pltpu.make_async_copy(conv_v, conv_hbm, out_sem.at[3]),
    ]
    store[0].start()
    first_half = lax.axis_index("seq") == 0
    for k in range(own_ref.shape[0]):
        own, got = own_ref[k], theirs_ref[k]
        head_part = jnp.where(first_half, own, got)
        tail_part = jnp.where(first_half, got, own)
        columns = slice(k * HD, (k + 1) * HD)
        state_v[:, columns] = tail_part[0:1] * head_part[1:2] + tail_part[1:2]
        picked = head_part[2 : 1 + TAPS] + tail_part[2 : 1 + TAPS]
        conv_v[0, :, columns] = picked.astype(jnp.bfloat16)
    store[2].start()
    store[3].start()
    zeros_v[...] = jnp.zeros_like(zeros_v)
    store[1].start()
    for copy in store:
        copy.wait()


def gathered_on_device(
    sizes, tokens, attn_in, lengths, norm_gain, attn_gain, w_x, conv_w, w_a, w_i, lru_decay, w_kv
):
    local_len, width = tokens.shape[1:]
    z_size, x_size, cores, seq_parts = sizes
    heads = width // HD
    rows_ext = -(-(local_len + (TAPS - 1) * LANES_OF_TIME) // HALO) * HALO
    anywhere = pl.BlockSpec(memory_space=pl.ANY)
    vmem = pl.BlockSpec(memory_space=pltpu.VMEM)
    owned = width // seq_parts
    per_owner = heads // seq_parts
    half = w_kv.shape[1] // seq_parts
    own, theirs, kv = pl.pallas_call(
        functools.partial(prefill_kernel, sizes),
        in_specs=[pl.BlockSpec(memory_space=pltpu.HBM)] * 11,
        out_specs=(vmem, vmem, vmem),
        out_shape=(
            pltpu.VMEM((per_owner, LANES_OF_TIME, HD), jnp.float32),
            pltpu.VMEM((per_owner, LANES_OF_TIME, HD), jnp.float32),
            pltpu.VMEM((seq_parts * local_len, half), jnp.bfloat16),
        ),
        scratch_shapes=[
            pltpu.VMEM((heads, z_size, x_size, cores, seq_parts, w_x.shape[0], HD), jnp.bfloat16),
            pltpu.VMEM((local_len, width), jnp.bfloat16),
            pltpu.VMEM((local_len, width), jnp.bfloat16),
            pltpu.VMEM(w_kv.shape, jnp.bfloat16),
            pltpu.VMEM(w_a.shape, jnp.bfloat16),
            pltpu.VMEM(w_i.shape, jnp.bfloat16),
            pltpu.VMEM((EDGE, width), jnp.bfloat16),
            pltpu.VMEM((local_len, width), jnp.bfloat16),
            pltpu.VMEM((rows_ext, width), jnp.bfloat16),
            pltpu.VMEM((local_len, half), jnp.bfloat16),
            pltpu.VMEM((rows_ext, HD), jnp.float32),
            pltpu.VMEM((local_len, HD), jnp.float32),
            pltpu.VMEM((local_len, HD), jnp.float32),
            pltpu.VMEM((local_len, HD), jnp.float32),
            pltpu.VMEM((heads, LANES_OF_TIME, HD), jnp.float32),
            pltpu.VMEM((LANES_OF_TIME, HD), jnp.float32),
            pltpu.VMEM((2, local_len // 2, HD // 2), jnp.float32),
            pltpu.VMEM((1, width), jnp.float32),
            pltpu.VMEM((1, width), jnp.float32),
            pltpu.VMEM((1, width), jnp.float32),
            pltpu.VMEM(conv_w.shape, jnp.float32),
            pltpu.SMEM((1,), jnp.int32),
            pltpu.SemaphoreType.DMA((3, 2, len(SPLITS))),
            pltpu.SemaphoreType.DMA((heads, 4)),
            pltpu.SemaphoreType.DMA((1,)),
            pltpu.SemaphoreType.DMA((heads,)),
            pltpu.SemaphoreType.DMA((11,)),
            pltpu.SemaphoreType.DMA((4,)),
            pltpu.SemaphoreType.DMA((4,)),
        ],
        compiler_params=pltpu.CompilerParams(
            collective_id=0, has_side_effects=True, vmem_limit_bytes=60 * 1024 * 1024
        ),
    )(
        lengths,
        tokens[0],
        attn_in[0],
        norm_gain,
        attn_gain,
        w_x,
        conv_w,
        w_a,
        w_i,
        lru_decay,
        w_kv,
    )
    state_shape, conv_shape = (1, owned), (1, TAPS - 1, owned)
    state, conv_state, cache = pl.pallas_call(
        finish_kernel,
        in_specs=[vmem] * 3,
        out_specs=(anywhere, anywhere, anywhere),
        out_shape=(
            jax.ShapeDtypeStruct(state_shape, jnp.float32),
            jax.ShapeDtypeStruct(conv_shape, jnp.bfloat16),
            jax.ShapeDtypeStruct((W, half), jnp.bfloat16),
        ),
        scratch_shapes=[
            pltpu.VMEM((W - kv.shape[0], half), jnp.bfloat16),
            pltpu.VMEM(state_shape, jnp.float32),
            pltpu.VMEM(conv_shape, jnp.bfloat16),
            pltpu.SemaphoreType.DMA((4,)),
        ],
    )(*(pltpu.with_memory_space_constraint(v, pltpu.VMEM) for v in (own, theirs, kv)))
    return state, conv_state, cache[None]


def fits(mesh, sizes, tokens, w_x, w_kv):
    if sizes is None:
        return False
    _, length, width = tokens.shape
    devices = mesh.size
    seq_parts = mesh.shape["seq"]
    return (
        length < W
        and width % (HD * seq_parts) == 0
        and w_x.shape[0] % (devices * HALO) == 0
        and w_x.shape[0] // devices > max(p + q for _, (p, q) in SPLITS)
        and width // HD == sum(n for n, _ in SPLITS) == len(SLOTS)
        and w_kv.shape[1] == seq_parts * HD
        and tokens.shape[0] == mesh.shape["batch"]
    )


def solution(mesh):
    in_specs = (
        P("batch", "seq", None),
        P("batch", "seq", None),
        P("batch"),
        P(),
        P(),
        P(("batch", "seq"), None),
        P(),
        P(),
        P(),
        P(),
        P(),
    )
    out_specs = (P("batch", "seq"), P("batch", None, "seq"), P("batch", None, "seq"))
    sizes = physical_grid(mesh)

    def run(*arrays):
        tokens, w_x, w_kv = arrays[0], arrays[5], arrays[10]
        body = on_device
        if fits(mesh, sizes, tokens, w_x, w_kv):
            body = functools.partial(gathered_on_device, sizes)
        return jax.shard_map(
            body, mesh=mesh, in_specs=in_specs, out_specs=out_specs, check_vma=False
        )(*arrays)

    return run
```

```python
import functools

import jax
import jax.numpy as jnp
from jax import lax
from jax.experimental import pallas as pl
from jax.experimental.pallas import tpu as pltpu
from jax.sharding import PartitionSpec as P

H = 10
HD = 256
W = 2048
LANES_OF_TIME = 8
TAPS = 4
HALO = 16
STEP_ROWS = 32


def passed_along(block, axis, distance):
    devices = range(lax.axis_size(axis))
    route = [(i - distance, i) for i in devices if i - distance in devices]
    return lax.ppermute(block, axis, route)


def rms_norm(values, gain_vec):
    widened = values.astype(jnp.float32)
    inverse = lax.rsqrt(jnp.mean(widened * widened, axis=-1, keepdims=True) + 1e-06)
    return (widened * inverse * gain_vec).astype(jnp.bfloat16)


def rotate_keys(key_rows, positions):
    quarter = key_rows.shape[-1] // 4
    spacing = jnp.exp(-jnp.log(10000.0) * jnp.arange(quarter, dtype=jnp.float32) / quarter)
    angles = positions.astype(jnp.float32)[:, None] * spacing[None, :]
    cosine_rows = jnp.cos(angles)
    sine_rows = jnp.sin(angles)
    first_part = key_rows[:, :quarter]
    second_part = key_rows[:, quarter : 2 * quarter]
    return jnp.concatenate(
        [
            first_part * cosine_rows - second_part * sine_rows,
            second_part * cosine_rows + first_part * sine_rows,
            key_rows[:, 2 * quarter :],
        ],
        axis=1,
    )


def ordered_rows(tokens_ref, halo_ref, gain_ref, normed_ref):
    local_len = tokens_ref.shape[0]
    steps = local_len // LANES_OF_TIME
    row = lax.broadcasted_iota(jnp.int32, (normed_ref.shape[0], local_len + HALO), 0)
    col = lax.broadcasted_iota(jnp.int32, (normed_ref.shape[0], local_len + HALO), 1)
    at = lax.rem(row, LANES_OF_TIME) * steps + lax.div(row, LANES_OF_TIME) - (TAPS - 1)
    pick = (jnp.where(at < 0, at + local_len + HALO, at) == col).astype(jnp.bfloat16)
    rows = jnp.concatenate(
        [rms_norm(tokens_ref[...], gain_ref[...]), rms_norm(halo_ref[...], gain_ref[...])], axis=0
    )
    normed_ref[...] = jnp.dot(pick, rows, preferred_element_type=jnp.float32).astype(jnp.bfloat16)


def one_head(
    normed_ref, w_block, conv_w, w_a, w_i, rate, length, start, out_ref, xp_ref, xc_ref, ga_ref, gi_ref
):
    rows_ext = normed_ref.shape[0]
    local_len = xc_ref.shape[0]
    steps = local_len // LANES_OF_TIME
    projected = jnp.dot(normed_ref[...], w_block, preferred_element_type=jnp.float32).astype(
        jnp.bfloat16
    )
    xp_ref[...] = projected.astype(jnp.float32)
    row = lax.broadcasted_iota(jnp.int32, (HALO, rows_ext), 1)
    wanted = length - (TAPS - 1) + lax.broadcasted_iota(jnp.int32, (HALO, rows_ext), 0) - 2
    step = lax.div(row, LANES_OF_TIME) - (TAPS - 1)
    at = start + lax.rem(row, LANES_OF_TIME) * steps + step
    real = (step >= 0) & (step < steps) & (wanted < length) & (wanted >= length - (TAPS - 1))
    picker = (real & (at == wanted)).astype(jnp.bfloat16)
    picked = jnp.dot(picker, projected, preferred_element_type=jnp.float32)
    conv_sum = conv_w[0:1] * xp_ref[0:local_len]
    for offset in range(1, TAPS):
        shift = offset * LANES_OF_TIME
        conv_sum = conv_sum + conv_w[offset : offset + 1] * xp_ref[shift : shift + local_len]
    x_conv = conv_sum.astype(jnp.bfloat16)
    xc_ref[...] = x_conv.astype(jnp.float32)
    ga_ref[...] = jnp.dot(x_conv, w_a, preferred_element_type=jnp.float32)
    gi_ref[...] = jnp.dot(x_conv, w_i, preferred_element_type=jnp.float32)
    inner = lax.broadcasted_iota(jnp.int32, (STEP_ROWS, HD), 0)
    first_at = start + lax.rem(inner, LANES_OF_TIME) * steps + lax.div(inner, LANES_OF_TIME)

    def block(i, carry):
        state, rate_sum = carry
        rows = pl.ds(pl.multiple_of(i * STEP_ROWS, STEP_ROWS), STEP_ROWS)
        valid = first_at + i * (STEP_ROWS // LANES_OF_TIME) < length
        log_rate = rate * jax.nn.sigmoid(ga_ref[rows])
        fall = -2.0 * log_rate
        lost = 1.0 - fall * (1.0 / 6.0)
        for order in (5.0, 4.0, 3.0, 2.0):
            lost = 1.0 - fall * (1.0 / order) * lost
        lost = fall * lost
        root = lost * lax.rsqrt(jnp.maximum(lost, 1e-37))
        push = jnp.where(valid, root * jax.nn.sigmoid(gi_ref[rows]) * xc_ref[rows], 0.0)
        held = jnp.where(valid, log_rate, 0.0)
        keep = jnp.exp(held)
        for k in range(STEP_ROWS // LANES_OF_TIME):
            tile = slice(k * LANES_OF_TIME, (k + 1) * LANES_OF_TIME)
            state = keep[tile] * state + push[tile]
            rate_sum = rate_sum + held[tile]
        return state, rate_sum

    zeros = jnp.zeros((LANES_OF_TIME, HD), jnp.float32)
    state, rate_sum = lax.fori_loop(0, local_len // STEP_ROWS, block, (zeros, zeros))
    keep_all = jnp.exp(rate_sum)
    total = state[0:1]
    for s in range(1, LANES_OF_TIME):
        total = keep_all[s : s + 1] * total + state[s : s + 1]
    keep_total = jnp.exp(jnp.sum(rate_sum, axis=0, keepdims=True))
    place = lax.broadcasted_iota(jnp.int32, (LANES_OF_TIME, HD), 0)
    out_ref[...] = jnp.where(
        place == 0, keep_total, jnp.where(place == 1, total, picked[0:LANES_OF_TIME])
    )


def recurrent_kernel(
    length_ref,
    tokens_ref,
    halo_ref,
    gain_ref,
    w_ref,
    conv_ref,
    wa_ref,
    wi_ref,
    rate_ref,
    out_ref,
    normed_ref,
    *work
):
    @pl.when(pl.program_id(0) == 0)
    def _():
        ordered_rows(tokens_ref, halo_ref, gain_ref, normed_ref)

    start = lax.axis_index("seq") * tokens_ref.shape[0]
    one_head(
        normed_ref,
        w_ref[...],
        conv_ref[...],
        wa_ref[0],
        wi_ref[0],
        rate_ref[...],
        length_ref[0],
        start,
        out_ref,
        *work
    )


def recurrent(first, tokens, halo, lengths, norm_gain, w_part, conv_w, w_a, w_i, rate):
    local_len, width = tokens.shape
    part_width = w_part.shape[1]
    rows_ext = -(-(local_len + (TAPS - 1) * LANES_OF_TIME) // HALO) * HALO
    whole = lambda *shape: pl.BlockSpec(shape, lambda h: (0,) * len(shape))
    return pl.pallas_call(
        recurrent_kernel,
        grid=(part_width // HD,),
        in_specs=[
            pl.BlockSpec(memory_space=pltpu.SMEM),
            whole(local_len, width),
            whole(HALO, width),
            whole(1, width),
            pl.BlockSpec((width, HD), lambda h: (0, h)),
            pl.BlockSpec((TAPS, HD), lambda h: (0, h + first)),
            pl.BlockSpec((1, HD, HD), lambda h: (h + first, 0, 0)),
            pl.BlockSpec((1, HD, HD), lambda h: (h + first, 0, 0)),
            pl.BlockSpec((1, HD), lambda h: (0, h + first)),
        ],
        out_specs=pl.BlockSpec((LANES_OF_TIME, HD), lambda h: (0, h)),
        out_shape=jax.ShapeDtypeStruct((LANES_OF_TIME, part_width), jnp.float32),
        scratch_shapes=[
            pltpu.VMEM((rows_ext, width), jnp.bfloat16),
            pltpu.VMEM((rows_ext, HD), jnp.float32),
            pltpu.VMEM((local_len, HD), jnp.float32),
            pltpu.VMEM((local_len, HD), jnp.float32),
            pltpu.VMEM((local_len, HD), jnp.float32),
        ],
        compiler_params=pltpu.CompilerParams(vmem_limit_bytes=60 * 1024 * 1024),
        cost_estimate=pl.CostEstimate(
            flops=2 * local_len * part_width * (width + 2 * HD),
            bytes_accessed=2 * width * (local_len + part_width),
            transcendentals=6 * local_len * part_width,
        ),
    )(lengths, tokens, halo, norm_gain[None], w_part, conv_w, w_a, w_i, rate[None])


def on_device(
    tokens, attn_in, lengths, norm_gain, attn_gain, w_x, conv_w, w_a, w_i, lru_decay, w_kv
):
    local_len = tokens.shape[1]
    feature_dim = tokens.shape[2]
    seq_parts = lax.axis_size("seq")
    seq_place = lax.axis_index("seq")
    length = lengths[0]
    halo = passed_along(tokens[0, local_len - HALO :], "seq", 1)
    heads = feature_dim // HD
    early = (4 * heads) // 5
    positions = seq_place * local_len + jnp.arange(local_len, dtype=jnp.int32)
    attn_normed = rms_norm(attn_in[0], attn_gain)
    kv_full = jnp.dot(attn_normed, w_kv, preferred_element_type=jnp.float32)
    kv_rows = jnp.concatenate(
        [rotate_keys(kv_full[:, :HD], positions), kv_full[:, HD:]], axis=1
    ).astype(jnp.bfloat16)
    in_window = ((positions >= length - W) & (positions < length))[:, None]
    masked = jnp.where(in_window, kv_rows, jnp.zeros_like(kv_rows))
    by_column = lax.all_to_all(masked, "seq", split_axis=1, concat_axis=0, tiled=True)
    laps = -(-seq_parts * local_len // W)
    by_column = jnp.pad(by_column, ((0, laps * W - seq_parts * local_len), (0, 0)))
    kv_cache = by_column[:W]
    for lap in range(1, laps):
        kv_cache = kv_cache + by_column[lap * W : (lap + 1) * W]
    w_early = lax.all_gather(w_x[:, : early * HD], ("batch", "seq"), axis=0, tiled=True)
    w_early, w_local, kv_cache, halo = lax.optimization_barrier((w_early, w_x, kv_cache, halo))
    w_late = lax.all_gather(w_local[:, early * HD :], ("batch", "seq"), axis=0, tiled=True)
    w_parts = ((0, w_early), (early, w_late))
    rate = -8.0 * jax.nn.softplus(-lru_decay)
    summary = jnp.concatenate(
        [
            recurrent(first, tokens[0], halo, lengths, norm_gain, w_part, conv_w, w_a, w_i, rate)
            for first, w_part in w_parts
        ],
        axis=1,
    )
    owned_width = feature_dim // seq_parts
    gathered = lax.all_gather(summary, "seq", axis=0, tiled=True)
    owned = lax.dynamic_slice_in_dim(gathered, seq_place * owned_width, owned_width, 1)
    state = owned[1:2]
    picked = owned[2:5]
    for part in range(1, seq_parts):
        at = part * LANES_OF_TIME
        state = owned[at : at + 1] * state + owned[at + 1 : at + 2]
        picked = picked + owned[at + 2 : at + 5]
    conv_state = picked.astype(jnp.bfloat16)
    return (state, conv_state[None], kv_cache[None])


MESH_ID = pl.DeviceIdType.MESH
SPLITS = ((10, (16, 16)),)
NEAR, PLANE = 0, 1
EDGE = 8
START = (
    ("near", 0), ("plane", 0), ("own", 0), ("near", 1), ("plane", 1), ("own", 1), ("near", 2), ("plane", 2),
    ("own", 2), ("plane", 3), ("own", 3), ("plane", 4), ("own", 4), ("kv", 0), ("halo", 0), ("second", 0),
    ("near", 3), ("send_kv", 0), ("kv", 1), ("second", 1), ("third", 0), ("send_kv", 1), ("norm", 0), ("near", 4),
    ("second", 2), ("third_plane", 0), ("third", 1), ("reorder", 0), ("second", 3), ("third_plane", 1),
    ("reorder", 1),
)
SLOTS = (
    (
        (
            ("fourth", 0), ("ready", 0), ("near", 5), ("third_plane", 2), ("third", 2),
        ),
        (
            ("fourth", 1), ("plane", 5), ("own", 5), ("second", 4),
        ),
    ),
    (
        (
            ("ready", 1), ("near", 6), ("third_plane", 3), ("third", 3),
        ),
        (
            ("fourth", 2), ("plane", 6), ("own", 6), ("second", 5),
        ),
    ),
    (
        (
            ("ready", 2), ("near", 7), ("third_plane", 4), ("third", 4),
        ),
        (
            ("fourth", 3), ("plane", 7), ("own", 7), ("second", 6),
        ),
    ),
    (
        (
            ("ready", 3), ("near", 8), ("third_plane", 5), ("third", 5),
        ),
        (
            ("fourth", 4), ("plane", 8), ("own", 8), ("second", 7),
        ),
    ),
    (
        (
            ("ready", 4), ("near", 9), ("third_plane", 6), ("third", 6),
        ),
        (
            ("fourth", 5), ("plane", 9), ("own", 9), ("second", 8),
        ),
    ),
    (
        (
            ("ready", 5), ("third_plane", 7), ("third", 7),
        ),
        (
            ("fourth", 6), ("second", 9),
        ),
    ),
    (
        (
            ("ready", 6), ("third_plane", 8), ("third", 8),
        ),
        (
            ("fourth", 7),
        ),
    ),
    (
        (
            ("ready", 7), ("third_plane", 9), ("third", 9),
        ),
        (
            ("fourth", 8),
        ),
    ),
    (
        (
            ("ready", 8),
        ),
        (
            ("fourth", 9),
        ),
    ),
    (
        (
            ("ready", 9),
        ),
        (),
    ),
)


def physical_grid(mesh):
    grid = mesh.devices
    try:
        spots = [
            [(*device.coords, device.core_on_chip) for device in line] for line in grid.tolist()
        ]
    except AttributeError:
        return None
    sizes = [len({spot[k] for line in spots for spot in line}) for k in range(4)]
    low = [min(spot[k] for line in spots for spot in line) for k in range(4)]
    x_size, y_size, z_size, cores = sizes
    if (x_size, y_size, z_size, cores) != (2, 2, 4, 2) or grid.shape != (z_size * x_size * cores, y_size):
        return None
    for b, line in enumerate(spots):
        for y, spot in enumerate(line):
            want = ((b // cores) % x_size, y, b // (cores * x_size), b % cores)
            if tuple(v - l for v, l in zip(spot, low)) != want:
                return None
    return z_size, x_size, cores, y_size


def scoped(method):
    @functools.wraps(method)
    def inside(*args):
        with jax.named_scope(method.__name__):
            return method(*args)

    return inside


def by_split(method):
    @functools.wraps(method)
    def inside(exchange, head):
        with jax.named_scope(method.__name__):
            first = 0
            for index, (count, _) in enumerate(SPLITS):
                last = first + count
                if isinstance(head, int):
                    if first <= head < last:
                        method(exchange, head, index)
                elif len(SPLITS) == 1:
                    method(exchange, head, index)
                else:

                    @pl.when((head >= first) & (head < last))
                    def _():
                        method(exchange, head, index)

                first = last

    return inside


class Exchange:
    def __init__(self, sizes, heads, w_buf, send_sem, recv_sem, core_send, core_recv):
        self.sizes, self.heads = sizes, heads
        self.w_buf, self.send_sem, self.recv_sem = w_buf, send_sem, recv_sem
        self.core_send, self.core_recv = core_send, core_recv
        z_size, x_size, cores, _ = sizes
        at = lax.axis_index("batch")
        self.core = lax.rem(at, cores)
        self.x = lax.rem(lax.div(at, cores), x_size)
        self.z = lax.div(at, cores * x_size)
        self.y = lax.axis_index("seq")
        self.shard_rows = w_buf.shape[5]
        self.is_end = (self.z == 0) | (self.z == z_size - 1)

    def device(self, z=None, x=None, core=None, y=None):
        z = self.z if z is None else z
        x = self.x if x is None else x
        core = self.core if core is None else core
        y = self.y if y is None else y
        _, x_size, cores, _ = self.sizes
        return ((z * x_size + x) * cores + core, y)

    def peers(self):
        z_size = self.sizes[0]
        along = [self.device(z=lax.rem(self.z + d, z_size)) for d in range(1, z_size)]
        return along + [
            self.device(x=1 - self.x),
            self.device(y=1 - self.y),
            self.device(x=1 - self.x, y=1 - self.y),
            self.device(core=1 - self.core),
        ]

    def blocks(self, head, z, x, y, first, rows, core=None):
        core = self.core if core is None else core
        return self.w_buf.at[head, z, x, core, y, pl.ds(first, rows)]

    def copy(self, head, stage, group, split, part, to):
        return pltpu.make_async_remote_copy(
            src_ref=part,
            dst_ref=part,
            send_sem=self.send_sem.at[stage, group, split],
            recv_sem=self.recv_sem.at[head, stage if group == NEAR or stage != 1 else 3],
            device_id=to,
            device_id_type=MESH_ID,
        )

    def hand_over(self, head, part):
        pltpu.make_async_remote_copy(
            src_ref=part,
            dst_ref=part,
            send_sem=self.core_send.at[0],
            recv_sem=self.core_recv.at[head],
            device_id=self.device(core=1 - self.core),
            device_id_type=MESH_ID,
        ).start()

    def some(self, head, count, rows):
        every = slice(None)
        if count == 2:
            return self.w_buf.at[head, pl.ds(0, 2), 0, 0, 0, pl.ds(0, rows)]
        if count == 3:
            return self.w_buf.at[head, pl.ds(0, 3), 0, 0, 0, pl.ds(0, rows)]
        if count == 4:
            return self.w_buf.at[head, every, 0, 0, 0, pl.ds(0, rows)]
        if count == 8:
            return self.w_buf.at[head, every, every, 0, 0, pl.ds(0, rows)]
        return self.w_buf.at[head, pl.ds(0, 3), every, 0, every, pl.ds(0, rows)]

    def arrived(self, head, stage, group, count, rows):
        part = self.some(head, count, rows)
        self.copy(head, stage, group, 0, part, self.device(core=1 - self.core)).wait_recv()

    def left(self, stage, group, split, count, rows):
        first = sum(n for n, _ in SPLITS[:split])
        part = self.some(pl.ds(first, SPLITS[split][0]), count, rows)
        self.copy(0, stage, group, split, part, self.device(core=1 - self.core)).wait_send()

    def routes(self, split, act):
        plane_rows, turned = SPLITS[split][1]

        @pl.when(self.core == 0)
        def _():
            if turned:
                act("yx", plane_rows, turned)
            act("xy", plane_rows + turned, self.shard_rows - plane_rows - turned)

        @pl.when(self.core != 0)
        def _():
            act("yx", plane_rows, self.shard_rows - plane_rows)

    @by_split
    def near(self, head, split):
        plane_rows = SPLITS[split][1][0]
        part = self.blocks(head, self.z, self.x, self.y, plane_rows, self.shard_rows - plane_rows)
        for d in range(1, self.sizes[0]):
            to = self.device(z=lax.rem(self.z + d, self.sizes[0]))
            self.copy(head, 0, NEAR, split, part, to).start()

    def across(self, order):
        beside = self.device(x=1 - self.x), self.device(y=1 - self.y)
        return beside if order == "xy" else beside[::-1]

    @by_split
    def own(self, head, split):
        def near(order, first, rows):
            own = self.blocks(head, self.z, self.x, self.y, first, rows)
            for stage, to in enumerate(self.across(order)):
                self.copy(head, 1 + stage, NEAR, split, own, to).start()

        self.routes(split, near)

    @by_split
    def plane(self, head, split):
        plane_rows = SPLITS[split][1][0]
        plane = self.blocks(head, self.z, self.x, self.y, 0, plane_rows)
        self.copy(head, 0, PLANE, split, plane, self.device(x=1 - self.x)).start()
        self.copy(head, 0, PLANE, split, plane, self.device(y=1 - self.y)).start()
        self.copy(head, 0, PLANE, split, plane, self.device(x=1 - self.x, y=1 - self.y)).start()

    @by_split
    def second(self, head, split):
        plane_rows = SPLITS[split][1][0]
        every = slice(None)
        last = self.sizes[0] - 1
        self.arrived(head, 0, NEAR, 3, self.shard_rows)

        def near(order, first, rows):
            for stage, to in enumerate(self.across(order)):
                for d in range(1, last + 1):
                    at = lax.rem(self.z + d, last + 1)
                    part = self.blocks(head, at, self.x, self.y, first, rows)
                    self.copy(head, 1 + stage, NEAR, split, part, to).start()
            self.hand_over(head, self.blocks(head, every, self.x, self.y, first, rows))

        self.routes(split, near)
        plane = self.blocks(head, self.z, every, every, 0, plane_rows)
        up = jnp.where(self.z == last, 1, self.z + 1)
        down = jnp.where(self.z == 0, last - 1, self.z - 1)
        self.copy(head, 1, PLANE, split, plane, self.device(z=up)).start()
        self.copy(head, 1, PLANE, split, plane, self.device(z=down)).start()
        self.hand_over(head, plane)

    @by_split
    def third(self, head, split):
        plane_rows = SPLITS[split][1][0]
        every = slice(None)
        self.arrived(head, 1, NEAR, 4, self.shard_rows - plane_rows)

        def near(order, first, rows):
            if order == "xy":
                part = self.blocks(head, every, 1 - self.x, self.y, first, rows)
            else:
                part = self.blocks(head, every, self.x, 1 - self.y, first, rows)
            to = self.across(order)[1]
            self.copy(head, 2, NEAR, split, part, to).start()
            self.hand_over(head, part)

        self.routes(split, near)

    @by_split
    def third_plane(self, head, split):
        plane_rows = SPLITS[split][1][0]
        every = slice(None)
        last = self.sizes[0] - 1

        @pl.when(self.is_end)
        def _():
            self.arrived(head, 1, PLANE, 4, plane_rows)

        @pl.when(jnp.logical_not(self.is_end))
        def _():
            self.arrived(head, 1, PLANE, 12, plane_rows)
            half = (last + 1) // 2
            start = jnp.where(self.z >= half, 0, half)
            part = self.blocks(head, pl.ds(start, half), every, every, 0, plane_rows)
            self.copy(head, 2, PLANE, split, part, self.device(z=jnp.where(self.z >= half, last, 0))).start()

    @by_split
    def fourth(self, head, split):
        plane_rows = SPLITS[split][1][0]
        every = slice(None)
        z_size = self.sizes[0]

        @pl.when(self.is_end)
        def _():
            self.arrived(head, 2, NEAR, 8, self.shard_rows)

        @pl.when(jnp.logical_not(self.is_end))
        def _():
            self.arrived(head, 2, NEAR, 8, self.shard_rows - plane_rows)

        def near(order, first, rows):
            if order == "xy":
                part = self.blocks(head, every, every, 1 - self.y, first, rows)
            else:
                part = self.blocks(head, every, 1 - self.x, every, first, rows)
            self.hand_over(head, part)

        self.routes(split, near)

        for d in range(1, z_size):
            self.hand_over(head, self.blocks(head, lax.rem(self.z + d, z_size), every, every, 0, plane_rows))

    def handed(self, head, core):
        part = self.w_buf.at[head, slice(None), slice(None), core]
        return pltpu.make_async_remote_copy(
            src_ref=part,
            dst_ref=part,
            send_sem=self.core_send.at[0],
            recv_sem=self.core_recv.at[0 if isinstance(head, slice) else head],
            device_id=self.device(core=1 - self.core),
            device_id_type=MESH_ID,
        )

    @scoped
    def ready(self, head):
        self.handed(head, 1 - self.core).wait_recv()

    @scoped
    def settled(self):
        for split, (_, (plane_rows, _)) in enumerate(SPLITS):
            near_rows = self.shard_rows - plane_rows
            self.left(0, NEAR, split, 3, near_rows)
            self.left(0, PLANE, split, 3, plane_rows)
            self.left(1, NEAR, split, 4, near_rows)
            self.left(1, PLANE, split, 8, plane_rows)
            self.left(2, NEAR, split, 8, near_rows)

            @pl.when(jnp.logical_not(self.is_end))
            def _():
                self.left(2, PLANE, split, 8, plane_rows)

        self.handed(slice(None), self.core).wait_send()


def prefill_kernel(
    sizes,
    length_hbm,
    tokens_hbm,
    attn_hbm,
    norm_gain_hbm,
    attn_gain_hbm,
    w_hbm,
    conv_hbm,
    wa_hbm,
    wi_hbm,
    decay_hbm,
    wkv_hbm,
    own_ref,
    theirs_ref,
    cache_ref,
    w_buf,
    tokens_v,
    attn_v,
    wkv_v,
    wa_v,
    wi_v,
    halo_v,
    rows_v,
    normed_v,
    kv_v,
    xp_v,
    xc_v,
    ga_v,
    gi_v,
    summary_v,
    picked_v,
    turn_v,
    norm_gain_ref,
    attn_gain_ref,
    decay_ref,
    conv_ref,
    length_ref,
    send_sem,
    recv_sem,
    core_send,
    core_recv,
    load_sem,
    side_send,
    side_recv,
):
    heads = w_buf.shape[0]
    local_len = tokens_v.shape[0]
    seq_parts = sizes[3]
    ex = Exchange(sizes, heads, w_buf, send_sem, recv_sem, core_send, core_recv)
    y = ex.y
    start = y * local_len
    beside = ex.device(y=1 - y)

    shard = [
        pltpu.make_async_copy(
            w_hbm.at[:, pl.ds(h * HD, HD)], w_buf.at[h, ex.z, ex.x, ex.core, y], load_sem.at[10]
        )
        for h in range(heads)
    ]
    loads = [
        pltpu.make_async_copy(source, target, load_sem.at[i])
        for i, (source, target) in enumerate(
            (
                (tokens_hbm, tokens_v),
                (attn_hbm, attn_v),
                (wkv_hbm, wkv_v),
                (wa_hbm, wa_v),
                (wi_hbm, wi_v),
                (norm_gain_hbm, norm_gain_ref.at[0]),
                (attn_gain_hbm, attn_gain_ref.at[0]),
                (decay_hbm, decay_ref.at[0]),
                (conv_hbm, conv_ref),
                (length_hbm, length_ref),
            )
        )
    ]
    for copy in shard:
        copy.start()

    barrier = pltpu.get_barrier_semaphore()
    peers = ex.peers()
    for peer in peers:
        pl.semaphore_signal(barrier, inc=1, device_id=peer, device_id_type=MESH_ID)

    own_shard = w_buf.at[:, ex.z, ex.x, ex.core, y]
    pltpu.make_async_copy(own_shard, own_shard, load_sem.at[10]).wait()
    for copy in [loads[1], loads[2], loads[6], loads[9], loads[0], *loads[3:6], loads[7], loads[8]]:
        copy.start()
    pl.semaphore_wait(barrier, len(peers))
    lead = START.index(("kv", 0))
    for name, head in START[:lead]:
        getattr(ex, name)(head)

    quarter = HD // 4
    lane = lax.broadcasted_iota(jnp.int32, (1, 2 * quarter), 1)
    spacing = jnp.exp(
        (-jnp.log(10000.0) / quarter) * lax.rem(lane, quarter).astype(jnp.float32)
    )
    half_len = local_len // 2
    fine = lax.broadcasted_iota(jnp.int32, (half_len, 2 * quarter), 0).astype(jnp.float32) * spacing
    turn_v[0] = jnp.cos(fine)
    turn_v[1] = jnp.sin(fine)

    loads[6].wait()
    loads[9].wait()
    length = length_ref[0]

    def kv_half(k):
        rows = slice(k * half_len, (k + 1) * half_len)
        normed = rms_norm(attn_v[rows], attn_gain_ref[...])
        full = jnp.dot(normed, wkv_v[...], preferred_element_type=jnp.float32)
        place = start + k * half_len
        coarse = place.astype(jnp.float32) * spacing
        cos_c, sin_c = jnp.cos(coarse), jnp.sin(coarse)
        cosine = cos_c * turn_v[0] - sin_c * turn_v[1]
        sine = sin_c * turn_v[0] + cos_c * turn_v[1]
        sine = jnp.where(lane < quarter, -sine, sine)
        at = place + lax.broadcasted_iota(jnp.int32, (half_len, 1), 0)
        window = (at >= length - W) & (at < length)
        turned = full[:, : 2 * quarter]
        other = pltpu.roll(turned, quarter, axis=1)
        turned = turned * cosine + other * sine

        keys = jnp.concatenate([turned, full[:, 2 * quarter : HD]], axis=1)
        first, second = (jnp.where(window, v, 0.0).astype(jnp.bfloat16) for v in (keys, full[:, HD:]))
        cache_ref[pl.ds(place, half_len)] = jnp.where(y == 0, first, second)
        kv_v[rows] = jnp.where(y == 0, second, first)

    halo_copy = pltpu.make_async_remote_copy(
        src_ref=tokens_v.at[pl.ds(local_len - EDGE, EDGE)],
        dst_ref=halo_v,
        send_sem=side_send.at[0],
        recv_sem=side_recv.at[0],
        device_id=beside,
        device_id_type=MESH_ID,
    )
    kv_copies = [
        pltpu.make_async_remote_copy(
            src_ref=kv_v.at[pl.ds(k * half_len, half_len)],
            dst_ref=cache_ref.at[pl.ds(start + k * half_len, half_len)],
            send_sem=side_send.at[1 + k],
            recv_sem=side_recv.at[1 + k],
            device_id=beside,
            device_id_type=MESH_ID,
        )
        for k in range(2)
    ]

    def take_kv(k):
        if k == 0:
            loads[1].wait()
            loads[2].wait()
        kv_half(k)

    def send_kv(k):
        kv_copies[k].start()

    def send_halo(_):
        loads[0].wait()

        @pl.when(y == 0)
        def _():
            halo_copy.start()
            halo_v[...] = jnp.zeros_like(halo_v)

    norm_step = 64

    def norm_rows(i, carry):
        rows = pl.ds(pl.multiple_of(i * norm_step, norm_step), norm_step)
        rows_v[rows] = rms_norm(tokens_v[rows], norm_gain_ref[...])
        return carry

    def norm(_):
        loads[5].wait()
        lax.fori_loop(0, local_len // norm_step, norm_rows, 0)

    steps = local_len // LANES_OF_TIME
    rows_ext = normed_v.shape[0]
    row = lax.broadcasted_iota(jnp.int32, (rows_ext, local_len), 0)
    col = lax.broadcasted_iota(jnp.int32, (rows_ext, local_len), 1)
    at = lax.rem(row, LANES_OF_TIME) * steps + lax.div(row, LANES_OF_TIME) - (TAPS - 1)
    pick = (at == col).astype(jnp.bfloat16)

    def reorder(i, carry):
        columns = pl.ds(pl.multiple_of(i * HD, HD), HD)
        normed_v[:, columns] = jnp.dot(
            pick, rows_v[:, columns], preferred_element_type=jnp.float32
        ).astype(jnp.bfloat16)
        return carry

    def reorder_half(k):
        half_heads = heads // 2
        lax.fori_loop(*((0, half_heads) if k == 0 else (half_heads, heads)), reorder, 0)
        if k == 0:
            return

        @pl.when(y != 0)
        def _():
            halo_copy.wait_recv()

        edge = 2 * HALO
        row = lax.broadcasted_iota(jnp.int32, (edge, EDGE), 0)
        col = lax.broadcasted_iota(jnp.int32, (edge, EDGE), 1)
        at = lax.div(row, LANES_OF_TIME) - (TAPS - 1)
        early = (lax.rem(row, LANES_OF_TIME) == 0) & (at < 0) & (at + EDGE == col)
        halo_rows = rms_norm(halo_v[...], norm_gain_ref[...])
        before = jnp.dot(early.astype(jnp.bfloat16), halo_rows, preferred_element_type=jnp.float32)
        normed_v[0:edge] = (normed_v[0:edge].astype(jnp.float32) + before).astype(jnp.bfloat16)

    tasks = {"kv": take_kv, "send_kv": send_kv, "halo": send_halo, "norm": norm, "reorder": reorder_half}
    for name, head in START[lead:]:
        if name in tasks:
            with jax.named_scope(name):
                tasks[name](head)
        else:
            getattr(ex, name)(head)
    for copy in (loads[3], loads[4], loads[7], loads[8]):
        copy.wait()

    per_owner = heads // seq_parts

    def summary_copy(head, slot):
        return pltpu.make_async_remote_copy(
            src_ref=summary_v.at[head],
            dst_ref=theirs_ref.at[slot],
            send_sem=side_send.at[3],
            recv_sem=side_recv.at[3],
            device_id=beside,
            device_id_type=MESH_ID,
        )

    inner = lax.broadcasted_iota(jnp.int32, (STEP_ROWS, HD), 0)
    first_at = start + lax.rem(inner, LANES_OF_TIME) * steps + lax.div(inner, LANES_OF_TIME)

    def project(head):
        columns = pl.ds(pl.multiple_of(head * HD, HD), HD)
        w_block = w_buf[head].reshape(normed_v.shape[1], HD)
        half_rows = rows_ext // 4
        projected = jnp.concatenate(
            [
                jnp.dot(normed_v[k * half_rows : (k + 1) * half_rows], w_block, preferred_element_type=jnp.float32)
                for k in range(4)
            ],
            axis=0,
        ).astype(jnp.bfloat16)
        xp_v[...] = projected.astype(jnp.float32)
        row = lax.broadcasted_iota(jnp.int32, (HALO, rows_ext), 1)
        wanted = length - (TAPS - 1) + lax.broadcasted_iota(jnp.int32, (HALO, rows_ext), 0) - 2
        step = lax.div(row, LANES_OF_TIME) - (TAPS - 1)
        at = start + lax.rem(row, LANES_OF_TIME) * steps + step
        real = (step >= 0) & (step < steps) & (wanted < length) & (wanted >= length - (TAPS - 1))
        picker = (real & (at == wanted)).astype(jnp.bfloat16)
        picked = jnp.dot(picker, projected, preferred_element_type=jnp.float32)
        conv_w = conv_ref[:, columns]
        conv_sum = conv_w[0:1] * xp_v[0:local_len]
        for offset in range(1, TAPS):
            shift = offset * LANES_OF_TIME
            conv_sum = conv_sum + conv_w[offset : offset + 1] * xp_v[shift : shift + local_len]
        x_conv = conv_sum.astype(jnp.bfloat16)
        xc_v[...] = x_conv.astype(jnp.float32)
        ga_v[...] = jnp.dot(x_conv, wa_v[head], preferred_element_type=jnp.float32)
        gi_v[...] = jnp.dot(x_conv, wi_v[head], preferred_element_type=jnp.float32)
        picked_v[...] = picked[0:LANES_OF_TIME]

    def scan(head):
        columns = pl.ds(pl.multiple_of(head * HD, HD), HD)
        rate = -8.0 * jax.nn.softplus(-decay_ref[:, columns])

        def block(i, carry):
            state, rate_sum = carry
            rows = pl.ds(pl.multiple_of(i * STEP_ROWS, STEP_ROWS), STEP_ROWS)
            valid = first_at + i * (STEP_ROWS // LANES_OF_TIME) < length
            log_rate = rate * jax.nn.sigmoid(ga_v[rows])
            fall = -2.0 * log_rate
            lost = 1.0 - fall * (1.0 / 6.0)
            for order in (5.0, 4.0, 3.0, 2.0):
                lost = 1.0 - fall * (1.0 / order) * lost
            lost = fall * lost
            root = lost * lax.rsqrt(jnp.maximum(lost, 1e-37))
            push = jnp.where(valid, root * jax.nn.sigmoid(gi_v[rows]) * xc_v[rows], 0.0)
            held = jnp.where(valid, log_rate, 0.0)
            keep = jnp.exp(held)
            for k in range(STEP_ROWS // LANES_OF_TIME):
                tile = slice(k * LANES_OF_TIME, (k + 1) * LANES_OF_TIME)
                state = keep[tile] * state + push[tile]
                rate_sum = rate_sum + held[tile]
            return state, rate_sum

        zeros = jnp.zeros((LANES_OF_TIME, HD), jnp.float32)
        state, rate_sum = lax.fori_loop(0, local_len // STEP_ROWS, block, (zeros, zeros))
        keep_all = jnp.exp(rate_sum)
        total = state[0:1]
        for s in range(1, LANES_OF_TIME):
            total = keep_all[s : s + 1] * total + state[s : s + 1]
        keep_total = jnp.exp(jnp.sum(rate_sum, axis=0, keepdims=True))
        place = lax.broadcasted_iota(jnp.int32, (LANES_OF_TIME, HD), 0)
        summary_v[head] = jnp.where(
            place == 0, keep_total, jnp.where(place == 1, total, picked_v[...])
        )

        @pl.when(lax.div(head, per_owner) != y)
        def _():
            summary_copy(head, lax.rem(head, per_owner)).start()

    def take(steps):
        for name, head in steps:
            if name in tasks:
                with jax.named_scope(name):
                    tasks[name](head)
            else:
                getattr(ex, name)(head)

    def head_step(head, carry):
        for slot, (name, task) in enumerate((("project", project), ("scan", scan))):
            for at, steps in enumerate(SLOTS):
                if steps[slot]:
                    pl.when(head == at)(functools.partial(take, steps[slot]))
            with jax.named_scope(name):
                task(head)
        return carry

    lax.fori_loop(0, heads, head_step, 0)

    own_ref[...] = summary_v[pl.ds(y * per_owner, per_owner)]
    every = summary_v.at[pl.ds(0, per_owner)]
    exchanged = pltpu.make_async_remote_copy(
        src_ref=every,
        dst_ref=theirs_ref,
        send_sem=side_send.at[3],
        recv_sem=side_recv.at[3],
        device_id=beside,
        device_id_type=MESH_ID,
    )
    for copy in kv_copies:
        copy.wait()

    @pl.when(y == 0)
    def _():
        halo_copy.wait_send()

    ex.settled()
    with jax.named_scope("exchanged"):
        exchanged.wait()


def finish_kernel(
    own_ref, theirs_ref, kv_ref, state_hbm, conv_hbm, cache_hbm, zeros_v, state_v, conv_v, out_sem
):
    rest = kv_ref.shape[0]
    store = [
        pltpu.make_async_copy(kv_ref, cache_hbm.at[pl.ds(0, rest)], out_sem.at[0]),
        pltpu.make_async_copy(zeros_v, cache_hbm.at[pl.ds(rest, zeros_v.shape[0])], out_sem.at[1]),
        pltpu.make_async_copy(state_v, state_hbm, out_sem.at[2]),
        pltpu.make_async_copy(conv_v, conv_hbm, out_sem.at[3]),
    ]
    store[0].start()
    first_half = lax.axis_index("seq") == 0
    for k in range(own_ref.shape[0]):
        own, got = own_ref[k], theirs_ref[k]
        head_part = jnp.where(first_half, own, got)
        tail_part = jnp.where(first_half, got, own)
        columns = slice(k * HD, (k + 1) * HD)
        state_v[:, columns] = tail_part[0:1] * head_part[1:2] + tail_part[1:2]
        picked = head_part[2 : 1 + TAPS] + tail_part[2 : 1 + TAPS]
        conv_v[0, :, columns] = picked.astype(jnp.bfloat16)
    store[2].start()
    store[3].start()
    zeros_v[...] = jnp.zeros_like(zeros_v)
    store[1].start()
    for copy in store:
        copy.wait()


def gathered_on_device(
    sizes, tokens, attn_in, lengths, norm_gain, attn_gain, w_x, conv_w, w_a, w_i, lru_decay, w_kv
):
    local_len, width = tokens.shape[1:]
    z_size, x_size, cores, seq_parts = sizes
    heads = width // HD
    rows_ext = -(-(local_len + (TAPS - 1) * LANES_OF_TIME) // HALO) * HALO
    anywhere = pl.BlockSpec(memory_space=pl.ANY)
    vmem = pl.BlockSpec(memory_space=pltpu.VMEM)
    owned = width // seq_parts
    per_owner = heads // seq_parts
    half = w_kv.shape[1] // seq_parts
    own, theirs, kv = pl.pallas_call(
        functools.partial(prefill_kernel, sizes),
        in_specs=[pl.BlockSpec(memory_space=pltpu.HBM)] * 11,
        out_specs=(vmem, vmem, vmem),
        out_shape=(
            pltpu.VMEM((per_owner, LANES_OF_TIME, HD), jnp.float32),
            pltpu.VMEM((per_owner, LANES_OF_TIME, HD), jnp.float32),
            pltpu.VMEM((seq_parts * local_len, half), jnp.bfloat16),
        ),
        scratch_shapes=[
            pltpu.VMEM((heads, z_size, x_size, cores, seq_parts, w_x.shape[0], HD), jnp.bfloat16),
            pltpu.VMEM((local_len, width), jnp.bfloat16),
            pltpu.VMEM((local_len, width), jnp.bfloat16),
            pltpu.VMEM(w_kv.shape, jnp.bfloat16),
            pltpu.VMEM(w_a.shape, jnp.bfloat16),
            pltpu.VMEM(w_i.shape, jnp.bfloat16),
            pltpu.VMEM((EDGE, width), jnp.bfloat16),
            pltpu.VMEM((local_len, width), jnp.bfloat16),
            pltpu.VMEM((rows_ext, width), jnp.bfloat16),
            pltpu.VMEM((local_len, half), jnp.bfloat16),
            pltpu.VMEM((rows_ext, HD), jnp.float32),
            pltpu.VMEM((local_len, HD), jnp.float32),
            pltpu.VMEM((local_len, HD), jnp.float32),
            pltpu.VMEM((local_len, HD), jnp.float32),
            pltpu.VMEM((heads, LANES_OF_TIME, HD), jnp.float32),
            pltpu.VMEM((LANES_OF_TIME, HD), jnp.float32),
            pltpu.VMEM((2, local_len // 2, HD // 2), jnp.float32),
            pltpu.VMEM((1, width), jnp.float32),
            pltpu.VMEM((1, width), jnp.float32),
            pltpu.VMEM((1, width), jnp.float32),
            pltpu.VMEM(conv_w.shape, jnp.float32),
            pltpu.SMEM((1,), jnp.int32),
            pltpu.SemaphoreType.DMA((3, 2, len(SPLITS))),
            pltpu.SemaphoreType.DMA((heads, 4)),
            pltpu.SemaphoreType.DMA((1,)),
            pltpu.SemaphoreType.DMA((heads,)),
            pltpu.SemaphoreType.DMA((11,)),
            pltpu.SemaphoreType.DMA((4,)),
            pltpu.SemaphoreType.DMA((4,)),
        ],
        compiler_params=pltpu.CompilerParams(
            collective_id=0, has_side_effects=True, vmem_limit_bytes=60 * 1024 * 1024
        ),
    )(
        lengths,
        tokens[0],
        attn_in[0],
        norm_gain,
        attn_gain,
        w_x,
        conv_w,
        w_a,
        w_i,
        lru_decay,
        w_kv,
    )
    state_shape, conv_shape = (1, owned), (1, TAPS - 1, owned)
    state, conv_state, cache = pl.pallas_call(
        finish_kernel,
        in_specs=[vmem] * 3,
        out_specs=(anywhere, anywhere, anywhere),
        out_shape=(
            jax.ShapeDtypeStruct(state_shape, jnp.float32),
            jax.ShapeDtypeStruct(conv_shape, jnp.bfloat16),
            jax.ShapeDtypeStruct((W, half), jnp.bfloat16),
        ),
        scratch_shapes=[
            pltpu.VMEM((W - kv.shape[0], half), jnp.bfloat16),
            pltpu.VMEM(state_shape, jnp.float32),
            pltpu.VMEM(conv_shape, jnp.bfloat16),
            pltpu.SemaphoreType.DMA((4,)),
        ],
    )(*(pltpu.with_memory_space_constraint(v, pltpu.VMEM) for v in (own, theirs, kv)))
    return state, conv_state, cache[None]


def fits(mesh, sizes, tokens, w_x, w_kv):
    if sizes is None:
        return False
    _, length, width = tokens.shape
    devices = mesh.size
    seq_parts = mesh.shape["seq"]
    return (
        length < W
        and width % (HD * seq_parts) == 0
        and w_x.shape[0] % (devices * HALO) == 0
        and w_x.shape[0] // devices > max(p + q for _, (p, q) in SPLITS)
        and width // HD == sum(n for n, _ in SPLITS) == len(SLOTS)
        and w_kv.shape[1] == seq_parts * HD
        and tokens.shape[0] == mesh.shape["batch"]
    )


def solution(mesh):
    in_specs = (
        P("batch", "seq", None),
        P("batch", "seq", None),
        P("batch"),
        P(),
        P(),
        P(("batch", "seq"), None),
        P(),
        P(),
        P(),
        P(),
        P(),
    )
    out_specs = (P("batch", "seq"), P("batch", None, "seq"), P("batch", None, "seq"))
    sizes = physical_grid(mesh)

    def run(*arrays):
        tokens, w_x, w_kv = arrays[0], arrays[5], arrays[10]
        body = on_device
        if fits(mesh, sizes, tokens, w_x, w_kv):
            body = functools.partial(gathered_on_device, sizes)
        return jax.shard_map(
            body, mesh=mesh, in_specs=in_specs, out_specs=out_specs, check_vma=False
        )(*arrays)

    return run
```
